32 devices in a mesh: gp: 32 (over z, y, x, core).
Axes of the slice: x: 2, y: 2, z: 4, core: 2. Of those that a mesh axis runs over, the one named last changes fastest.
Arguments:
- grid_in: bfloat16 [65536, 164], P('gp')
- mesh_static: bfloat16 [65536, 3], P('gp')
- edge_static: bfloat16 [98304, 4], P('gp')
- send_rows: int32 [1024, 64], P('gp')
- edge_src: int32 [98304], P('gp')
- edge_dst: int32 [98304], P('gp')
- w_grid_in: bfloat16 [164, 256], replicated
- w_mesh_in: bfloat16 [3, 256], replicated
- w_edge_in: bfloat16 [4, 256], replicated
- w_edge_up: bfloat16 [768, 256], replicated
- w_mesh_up: bfloat16 [512, 256], replicated
- w_grid_up: bfloat16 [256, 256], replicated
- w_second: bfloat16 [6, 256, 256], replicated
- vectors: float32 [6, 4, 256], replicated
- d_mesh_out: bfloat16 [65536, 256], P('gp')
- d_grid_out: bfloat16 [65536, 256], P('gp')
Outputs:
- output 1: bfloat16 [65536, 256], P('gp')
- output 2: bfloat16 [65536, 256], P('gp')
- output 3: float32 [65536, 164], P('gp')
- output 4: float32 [164, 256], replicated
- output 5: float32 [3, 256], replicated
- output 6: float32 [4, 256], replicated
- output 7: float32 [768, 256], replicated
- output 8: float32 [512, 256], replicated
- output 9: float32 [256, 256], replicated
- output 10: float32 [6, 256, 256], replicated
- output 11: float32 [6, 4, 256], replicated
All inputs are finite; a program needn't handle non-finite values.
Results may differ from the reference program's by a relative error of at most 0.0192591.
Values are sent between devices in bfloat16 or wider.
A program may use at most 1 GiB of HBM per device.

```python
import jax
import jax.numpy as jnp
from jax import lax

NUM_PARTS = 32
GRID_DEV = 2048
MESH_DEV = 2048
FEATURES = 164
LATENT = 256
MESH_FEAT = 3
EDGE_FEAT = 4
EDGE_DEV = 3072
SLOT_CAP = 64
GRID_ALL = NUM_PARTS * GRID_DEV
MESH_ALL = NUM_PARTS * MESH_DEV
EDGE_ALL = NUM_PARTS * EDGE_DEV
LN_EPS = 1e-5


def draw_indices(key):
    sub_keys = jax.random.split(key, 5)
    band_ids = jnp.arange(NUM_PARTS)
    polar_band = (band_ids == 0) | (band_ids == NUM_PARTS - 1)
    low_cap = SLOT_CAP // 4
    counts = low_cap + jax.random.randint(sub_keys[0], (NUM_PARTS, NUM_PARTS), 0, SLOT_CAP - low_cap + 1, dtype=jnp.int32)
    counts = jnp.where(polar_band[:, None], SLOT_CAP, counts)
    send_rows = jax.random.randint(sub_keys[1], (NUM_PARTS * NUM_PARTS, SLOT_CAP), 0, GRID_DEV, dtype=jnp.int32)
    slot_valid = jnp.arange(SLOT_CAP)[None, None, :] < counts.T[:, :, None]
    buf_len = NUM_PARTS * SLOT_CAP
    slot_valid = slot_valid.reshape(NUM_PARTS, buf_len)
    order_key = jnp.where(slot_valid, 0, buf_len) + jnp.arange(buf_len)[None, :]
    slot_order = jnp.argsort(order_key, axis=1).astype(jnp.int32)
    n_valid = jnp.sum(slot_valid, axis=1).astype(jnp.int32)
    edge_ids = jnp.arange(EDGE_DEV, dtype=jnp.int32)[None, :]
    slot_pick = jax.random.randint(sub_keys[2], (NUM_PARTS, EDGE_DEV), 0, n_valid[:, None], dtype=jnp.int32)
    slot_pick = jnp.where(edge_ids < n_valid[:, None], edge_ids, slot_pick)
    edge_src = jnp.take_along_axis(slot_order, slot_pick, axis=1)
    dst_draw = jax.random.randint(sub_keys[3], (NUM_PARTS, EDGE_DEV), 0, MESH_DEV, dtype=jnp.int32)
    dst_draw = jnp.where(edge_ids < MESH_DEV, edge_ids, dst_draw)
    edge_dst = jax.random.permutation(sub_keys[4], dst_draw, axis=1, independent=True)
    return send_rows, edge_src.reshape(-1).astype(jnp.int32), edge_dst.reshape(-1).astype(jnp.int32)


def weight_draw(key, shape, fan_in):
    return (jax.random.normal(key, shape, jnp.float32) * fan_in ** -0.5).astype(jnp.bfloat16)


def setup_inputs(seed: int = 0) -> dict:
    key = jax.random.key(seed)
    sub_keys = jax.random.split(key, 16)
    send_rows, edge_src, edge_dst = draw_indices(sub_keys[0])
    grid_in = jax.random.normal(sub_keys[1], (GRID_ALL, FEATURES), jnp.float32)
    lat_draw = jax.random.uniform(sub_keys[2], (MESH_ALL,), jnp.float32, -1.5, 1.5)
    lon_draw = jax.random.uniform(sub_keys[3], (MESH_ALL,), jnp.float32, 0.0, 6.28)
    mesh_static = jnp.stack([jnp.cos(lat_draw), jnp.sin(lon_draw), jnp.cos(lon_draw)], axis=1)
    offsets = 0.5 * jax.random.normal(sub_keys[4], (EDGE_ALL, EDGE_FEAT - 1), jnp.float32)
    lengths = jnp.sqrt(jnp.sum(offsets * offsets, axis=1, keepdims=True))
    edge_static = jnp.concatenate([lengths, offsets], axis=1)
    vec_noise = jax.random.normal(sub_keys[12], (6, 4, LATENT), jnp.float32)
    vec_scale = jnp.array([0.3, 0.3, 0.2, 0.3], jnp.float32)
    vec_shift = jnp.array([0.0, 0.0, 1.0, 0.0], jnp.float32)
    vectors = vec_noise * vec_scale[None, :, None] + vec_shift[None, :, None]
    return {
        'grid_in': grid_in.astype(jnp.bfloat16),
        'mesh_static': mesh_static.astype(jnp.bfloat16),
        'edge_static': edge_static.astype(jnp.bfloat16),
        'send_rows': send_rows,
        'edge_src': edge_src,
        'edge_dst': edge_dst,
        'w_grid_in': weight_draw(sub_keys[5], (FEATURES, LATENT), FEATURES),
        'w_mesh_in': weight_draw(sub_keys[6], (MESH_FEAT, LATENT), MESH_FEAT),
        'w_edge_in': weight_draw(sub_keys[7], (EDGE_FEAT, LATENT), EDGE_FEAT),
        'w_edge_up': weight_draw(sub_keys[8], (3 * LATENT, LATENT), 3 * LATENT),
        'w_mesh_up': weight_draw(sub_keys[9], (2 * LATENT, LATENT), 2 * LATENT),
        'w_grid_up': weight_draw(sub_keys[10], (LATENT, LATENT), LATENT),
        'w_second': weight_draw(sub_keys[11], (6, LATENT, LATENT), LATENT),
        'vectors': vectors,
        'd_mesh_out': jax.random.normal(sub_keys[13], (MESH_ALL, LATENT), jnp.float32).astype(jnp.bfloat16),
        'd_grid_out': jax.random.normal(sub_keys[14], (GRID_ALL, LATENT), jnp.float32).astype(jnp.bfloat16),
    }


def mlp_tail(pre_act, w_two, vec_rows):
    pre_bias = pre_act + vec_rows[0]
    hidden = jax.nn.silu(pre_bias).astype(jnp.bfloat16)
    out_lin = jnp.dot(hidden, w_two, preferred_element_type=jnp.float32) + vec_rows[1]
    centered = out_lin - jnp.mean(out_lin, axis=-1, keepdims=True)
    inv_std = lax.rsqrt(jnp.mean(centered * centered, axis=-1, keepdims=True) + LN_EPS)
    return centered * inv_std * vec_rows[2] + vec_rows[3]


def first_layer(feat_in, w_first):
    return jnp.dot(feat_in, w_first, preferred_element_type=jnp.float32)


def reference(grid_in, mesh_static, edge_static, send_rows, edge_src, edge_dst, w_grid_in, w_mesh_in, w_edge_in, w_edge_up, w_mesh_up, w_grid_up, w_second, vectors, d_mesh_out, d_grid_out):
    edge_part = jnp.arange(EDGE_ALL, dtype=jnp.int32) // EDGE_DEV
    band_ids = edge_src // SLOT_CAP
    sender = band_ids * GRID_DEV + send_rows[band_ids * NUM_PARTS + edge_part, edge_src % SLOT_CAP]
    receiver = edge_part * MESH_DEV + edge_dst

    def forward(grid_x, wg_in, wm_in, we_in, we_up, wm_up, wg_up, w_two_all, vec_all):
        grid_lat = mlp_tail(first_layer(grid_x, wg_in), w_two_all[0], vec_all[0]).astype(jnp.bfloat16)
        mesh_lat = mlp_tail(first_layer(mesh_static, wm_in), w_two_all[1], vec_all[1]).astype(jnp.bfloat16)
        edge_lat = mlp_tail(first_layer(edge_static, we_in), w_two_all[2], vec_all[2]).astype(jnp.bfloat16)
        edge_cat = jnp.concatenate([edge_lat, jnp.take(grid_lat, sender, axis=0), jnp.take(mesh_lat, receiver, axis=0)], axis=1)
        edge_new = (edge_lat.astype(jnp.float32) + mlp_tail(first_layer(edge_cat, we_up), w_two_all[3], vec_all[3])).astype(jnp.bfloat16)
        agg_sum = jax.ops.segment_sum(edge_new.astype(jnp.float32), receiver, num_segments=MESH_ALL)
        mesh_cat = jnp.concatenate([mesh_lat, agg_sum.astype(jnp.bfloat16)], axis=1)
        mesh_out = (mesh_lat.astype(jnp.float32) + mlp_tail(first_layer(mesh_cat, wm_up), w_two_all[4], vec_all[4])).astype(jnp.bfloat16)
        grid_out = (grid_lat.astype(jnp.float32) + mlp_tail(first_layer(grid_lat, wg_up), w_two_all[5], vec_all[5])).astype(jnp.bfloat16)
        return mesh_out, grid_out

    fwd_outs, pull_back = jax.vjp(forward, grid_in, w_grid_in, w_mesh_in, w_edge_in, w_edge_up, w_mesh_up, w_grid_up, w_second, vectors)
    all_grads = pull_back((d_mesh_out, d_grid_out))
    return (fwd_outs[0], fwd_outs[1], all_grads[0].astype(jnp.float32), all_grads[1].astype(jnp.float32), all_grads[2].astype(jnp.float32), all_grads[3].astype(jnp.float32), all_grads[4].astype(jnp.float32), all_grads[5].astype(jnp.float32), all_grads[6].astype(jnp.float32), all_grads[7].astype(jnp.float32), all_grads[8].astype(jnp.float32))
```

```python
import functools

import jax
import jax.numpy as jnp
from jax import lax
from jax.experimental import pallas as pl
from jax.experimental.pallas import tpu as pltpu
from jax.sharding import PartitionSpec as P

LN_EPS = 1e-5
AXIS = 'gp'
BF = jnp.bfloat16
F32 = jnp.float32
MESH = pl.DeviceIdType.MESH
TILE = 256
VMEM_LIMIT = 60 * 1024 * 1024


def nn(lhs, rhs):
    return jnp.dot(lhs, rhs, preferred_element_type=F32)


def tn(lhs, rhs):
    return lax.dot_general(lhs, rhs, (((0,), (0,)), ((), ())), preferred_element_type=F32)


def nt(lhs, rhs):
    return lax.dot_general(lhs, rhs, (((1,), (1,)), ((), ())), preferred_element_type=F32)


def mlp_fwd(pre_act, w_two, vec):
    act = pre_act + vec[0:1]
    sig = 0.5 * jnp.tanh(0.5 * act) + 0.5
    hidden = (act * sig).astype(BF)
    lin = nn(hidden, w_two) + vec[1:2]
    cen = lin - jnp.mean(lin, axis=-1, keepdims=True)
    inv = lax.rsqrt(jnp.mean(cen * cen, axis=-1, keepdims=True) + LN_EPS)
    normed = cen * inv
    return (act, sig, hidden, normed, inv), normed * vec[2:3] + vec[3:4]


def mlp_bwd(saved, w_two, vec, d_out):
    act, sig, hidden, normed, inv = saved
    d_n = d_out * vec[2:3]
    m_one = jnp.mean(d_n, axis=-1, keepdims=True)
    m_two = jnp.mean(d_n * normed, axis=-1, keepdims=True)
    d_lin = inv * (d_n - m_one - normed * m_two)
    d_lin_bf = d_lin.astype(BF)
    d_two = tn(hidden, d_lin_bf)
    d_hid = nt(d_lin_bf, w_two)
    d_pre = d_hid * (sig * (1.0 + act * (1.0 - sig)))
    d_vec = [jnp.sum(d_pre, axis=0, keepdims=True), jnp.sum(d_lin, axis=0, keepdims=True),
             jnp.sum(d_out * normed, axis=0, keepdims=True), jnp.sum(d_out, axis=0, keepdims=True)]
    return d_pre.astype(BF), d_two, d_vec


def add_vec(ref, base, d_vec):
    for j in range(4):
        ref[base + j:base + j + 1, :] += d_vec[j]


def rows_at(i, size=TILE):
    return pl.ds(pl.multiple_of(i * size, size), size)


def hot_cols(col_idx, width):
    ids = lax.broadcasted_iota(jnp.int32, (col_idx.shape[0], width), 1)
    return jnp.where(ids == col_idx, 1.0, 0.0).astype(BF)


def hot_rows(row_idx, base, height):
    ids = lax.broadcasted_iota(jnp.int32, (height, row_idx.shape[1]), 0) + base
    return jnp.where(ids == row_idx, 1.0, 0.0).astype(BF)


def loop(n, body):
    def step(i, carry):
        body(i)
        return carry
    lax.fori_loop(0, n, step, 0)


def grid_fwd_kernel(grid_t, send_col, w_grid_in, w_two, vec, lat_out, send_out):
    def embed(i):
        sl = rows_at(i)
        _, emb = mlp_fwd(tn(grid_t[:, sl], w_grid_in[...]), w_two[0], vec[0])
        lat_out[sl, :] = emb.astype(BF)
    loop(lat_out.shape[0] // TILE, embed)

    def pick(i):
        sl = rows_at(i)
        send_out[sl, :] = nn(hot_cols(send_col[sl, :], lat_out.shape[0]), lat_out[...]).astype(BF)
    loop(send_out.shape[0] // TILE, pick)


def local_kernel(grid_lat, d_grid, mesh_t, edge_t, dst_col, w_mesh_in, w_edge_in, w_edge_up, w_grid_up, w_two, vec,
                 grid_out, d_lat_out, mesh_lat, edge_lat, recv_lat, grad):
    lat = w_grid_up.shape[0]
    grad[...] = jnp.zeros_like(grad)

    def cells(i):
        sl = rows_at(i)
        here = grid_lat[sl, :]
        saved, upd = mlp_fwd(nn(here, w_grid_up[...]), w_two[5], vec[5])
        grid_out[sl, :] = (here.astype(F32) + upd).astype(BF)
        d_top = d_grid[sl, :].astype(F32)
        d_pre, d_two, d_vec = mlp_bwd(saved, w_two[5], vec[5], d_top)
        grad[0:lat, :] += tn(here, d_pre)
        grad[lat:2 * lat, :] += d_two
        add_vec(grad, 2 * lat, d_vec)
        d_lat_out[sl, :] = d_top + nt(d_pre, w_grid_up[...])
    loop(grid_lat.shape[0] // TILE, cells)

    def nodes(i):
        sl = rows_at(i)
        _, emb = mlp_fwd(tn(mesh_t[:, sl], w_mesh_in[...]), w_two[1], vec[1])
        mesh_lat[sl, :] = emb.astype(BF)
    loop(mesh_lat.shape[0] // TILE, nodes)

    def edges(i):
        sl = rows_at(i)
        _, emb = mlp_fwd(tn(edge_t[:, sl], w_edge_in[...]), w_two[2], vec[2])
        edge_lat[sl, :] = emb.astype(BF)
        recv_lat[sl, :] = nn(hot_cols(dst_col[sl, :], mesh_lat.shape[0]), mesh_lat[...]).astype(BF)
    loop(edge_lat.shape[0] // TILE, edges)


def edge_kernel(incoming, mesh_lat, edge_lat, recv_lat, d_mesh, src_col, dst_col, src_row, dst_row, w_edge_up, w_mesh_up, w_two, vec,
                mesh_out, d_mesh_lat, d_edge_lat, d_pre3, d_incoming, grad,
                send_lat, edge_new, act_s, nrm_s, inv_s, d_pre4):
    lat = 256
    n_edge, n_mesh, n_slot = edge_lat.shape[0], mesh_lat.shape[0], incoming.shape[0]
    o_mesh, o_edge, o_four, o_three, o_vec = 0, 2 * lat, 5 * lat, 6 * lat, 7 * lat
    grad[...] = jnp.zeros_like(grad)

    def edges_fwd(i):
        sl = rows_at(i)
        sent = nn(hot_cols(src_col[sl, :], n_slot), incoming[...]).astype(BF)
        send_lat[sl, :] = sent
        here = edge_lat[sl, :]
        pre = nn(here, w_edge_up[0:lat, :]) + nn(sent, w_edge_up[lat:2 * lat, :]) + nn(recv_lat[sl, :], w_edge_up[2 * lat:3 * lat, :])
        (act, _, _, normed, inv), upd = mlp_fwd(pre, w_two[3], vec[3])
        act_s[sl, :] = act
        nrm_s[sl, :] = normed
        inv_s[sl, :] = jnp.broadcast_to(inv, (TILE, 128))
        edge_new[sl, :] = (here.astype(F32) + upd).astype(BF)
    loop(n_edge // TILE, edges_fwd)

    def nodes(i):
        sl = rows_at(i)
        agg = nn(hot_rows(dst_row[...], i * TILE, TILE), edge_new[...]).astype(BF)
        here = mesh_lat[sl, :]
        saved, upd = mlp_fwd(nn(here, w_mesh_up[0:lat, :]) + nn(agg, w_mesh_up[lat:2 * lat, :]), w_two[4], vec[4])
        mesh_out[sl, :] = (here.astype(F32) + upd).astype(BF)
        d_top = d_mesh[sl, :].astype(F32)
        d_pre, d_two, d_vec = mlp_bwd(saved, w_two[4], vec[4], d_top)
        d_pre4[sl, :] = d_pre
        grad[o_mesh:o_mesh + lat, :] += tn(here, d_pre)
        grad[o_mesh + lat:o_mesh + 2 * lat, :] += tn(agg, d_pre)
        grad[o_four:o_four + lat, :] += d_two
        add_vec(grad, o_vec, d_vec)
        d_mesh_lat[sl, :] = d_top + nt(d_pre, w_mesh_up[0:lat, :])
    loop(n_mesh // TILE, nodes)

    def edges_bwd(i):
        sl = rows_at(i)
        picked = nn(hot_cols(dst_col[sl, :], n_mesh), d_pre4[...]).astype(BF)
        d_new = nt(picked, w_mesh_up[lat:2 * lat, :])
        act = act_s[sl, :]
        sig = 0.5 * jnp.tanh(0.5 * act) + 0.5
        hidden = (act * sig).astype(BF)
        d_pre, d_two, d_vec = mlp_bwd((act, sig, hidden, nrm_s[sl, :], inv_s[sl, 0:1]), w_two[3], vec[3], d_new)
        d_pre3[sl, :] = d_pre
        grad[o_three:o_three + lat, :] += d_two
        add_vec(grad, o_vec + 4, d_vec)
        grad[o_edge:o_edge + lat, :] += tn(edge_lat[sl, :], d_pre)
        grad[o_edge + lat:o_edge + 2 * lat, :] += tn(send_lat[sl, :], d_pre)
        grad[o_edge + 2 * lat:o_edge + 3 * lat, :] += tn(recv_lat[sl, :], d_pre)
        d_edge_lat[sl, :] = d_new + nt(d_pre, w_edge_up[0:lat, :])
    loop(n_edge // TILE, edges_bwd)

    def slots(i):
        sl = rows_at(i)
        d_slot = nn(hot_rows(src_row[...], i * TILE, TILE), d_pre3[...]).astype(BF)
        d_incoming[sl, :] = nt(d_slot, w_edge_up[lat:2 * lat, :]).astype(BF)
    loop(n_slot // TILE, slots)


def embed_bwd_kernel(mesh_t, edge_t, dst_row, d_pre3, d_mesh_lat, d_edge_lat, w_mesh_in, w_edge_in, w_edge_up, w_two, vec, grad):
    lat = 256
    grad[...] = jnp.zeros_like(grad)
    o_vec = 2 * lat + 16

    def nodes(i):
        sl = rows_at(i)
        d_node = nn(hot_rows(dst_row[...], i * TILE, TILE), d_pre3[...]).astype(BF)
        d_top = d_mesh_lat[sl, :] + nt(d_node, w_edge_up[2 * lat:3 * lat, :])
        feat = mesh_t[:, sl]
        saved, _ = mlp_fwd(tn(feat, w_mesh_in[...]), w_two[1], vec[1])
        d_pre, d_two, d_vec = mlp_bwd(saved, w_two[1], vec[1], d_top)
        grad[0:lat, :] += d_two
        grad[2 * lat:2 * lat + 3, :] += nn(feat, d_pre)
        add_vec(grad, o_vec, d_vec)
    loop(d_mesh_lat.shape[0] // TILE, nodes)

    def edges(i):
        sl = rows_at(i)
        feat = edge_t[:, sl]
        saved, _ = mlp_fwd(tn(feat, w_edge_in[...]), w_two[2], vec[2])
        d_pre, d_two, d_vec = mlp_bwd(saved, w_two[2], vec[2], d_edge_lat[sl, :])
        grad[lat:2 * lat, :] += d_two
        grad[2 * lat + 8:2 * lat + 12, :] += nn(feat, d_pre)
        add_vec(grad, o_vec + 4, d_vec)
    loop(d_edge_lat.shape[0] // TILE, edges)


def grid_bwd_kernel(grid_t, send_row, d_sent, d_lat, w_grid_in, w_two, vec, d_grid_t, grad):
    feat_n = grid_t.shape[0]
    lat = 256
    grad[...] = jnp.zeros_like(grad)

    def body(i):
        sl = rows_at(i)
        d_top = d_lat[sl, :] + nn(hot_rows(send_row[...], i * TILE, TILE), d_sent[...])
        feat = grid_t[:, sl]
        saved, _ = mlp_fwd(tn(feat, w_grid_in[...]), w_two[0], vec[0])
        d_pre, d_two, d_vec = mlp_bwd(saved, w_two[0], vec[0], d_top)
        grad[0:lat, :] += d_two
        grad[lat:lat + feat_n, :] += nn(feat, d_pre)
        add_vec(grad, lat + 168, d_vec)
        d_grid_t[:, sl] = nt(w_grid_in[...], d_pre)
    loop(d_lat.shape[0] // TILE, body)


def sum_kernel(parts, g_a, g_b, g_c, g_d, out, own, r_one, r_two, r_three, r_four, send_sem, recv_sem, z_send, z_recv):
    me = lax.axis_index(AXIS)
    core = lax.rem(me, 2)
    x_at = lax.rem(me // 2, 2)
    y_at = lax.rem(me // 4, 2)
    z_at = me // 8
    piece = out.shape[0] // 32
    swap_x = me + 2 * (1 - 2 * x_at)
    swap_y = me + 4 * (1 - 2 * y_at)
    swap_c = me + 1 - 2 * core
    first = (1 - core) * swap_x + core * swap_y
    second = (1 - core) * swap_y + core * swap_x
    bit_one = (1 - core) * x_at + core * y_at
    bit_two = (1 - core) * y_at + core * x_at
    plane = me - 8 * z_at

    barrier = pltpu.get_barrier_semaphore()
    pl.semaphore_signal(barrier, inc=1, device_id=(swap_x,), device_id_type=MESH)
    pl.semaphore_signal(barrier, inc=1, device_id=(swap_y,), device_id_type=MESH)
    pl.semaphore_signal(barrier, inc=1, device_id=(swap_c,), device_id_type=MESH)
    for k in range(1, 4):
        pl.semaphore_signal(barrier, inc=1, device_id=(plane + 8 * lax.rem(z_at + k, 4),), device_id_type=MESH)

    base = 0
    for g in (g_a, g_b, g_c, g_d):
        own[base:base + g.shape[0], :] = g[...]
        base += g.shape[0]
    if base < own.shape[0]:
        own[base:, :] = jnp.zeros((own.shape[0] - base, own.shape[1]), F32)
    pl.semaphore_wait(barrier, 6)

    def at(start, size):
        return pl.ds(pl.multiple_of(start, 8), size)

    def exchange(k, src, dst, peer):
        copy = pltpu.make_async_remote_copy(src_ref=src, dst_ref=dst, send_sem=send_sem.at[k], recv_sem=recv_sem.at[k], device_id=(peer,), device_id_type=MESH)
        copy.start()
        copy.wait()

    half, quarter, eighth = 16 * piece, 8 * piece, 4 * piece
    lo_one = core * half
    exchange(0, own.at[at((1 - core) * half, half)], r_one, swap_c)
    own[at(lo_one, half), :] += r_one[...]
    lo_two = lo_one + bit_one * quarter
    exchange(1, own.at[at(lo_one + (1 - bit_one) * quarter, quarter)], r_two, first)
    own[at(lo_two, quarter), :] += r_two[...]
    lo_three = lo_two + bit_two * eighth
    exchange(2, own.at[at(lo_two + (1 - bit_two) * eighth, eighth)], r_three, second)
    own[at(lo_three, eighth), :] += r_three[...]

    copies = []
    for k in range(1, 4):
        z_to = lax.rem(z_at + k, 4)
        copies.append(pltpu.make_async_remote_copy(
            src_ref=own.at[at(lo_three + z_to * piece, piece)], dst_ref=r_four.at[k - 1],
            send_sem=z_send.at[k - 1], recv_sem=z_recv.at[k - 1], device_id=(plane + 8 * z_to,), device_id_type=MESH))
    for copy in copies:
        copy.start()
    for copy in copies:
        copy.wait()
    lo_four = lo_three + z_at * piece
    out[at(lo_four, piece), :] = own[at(lo_four, piece), :] + (r_four[0] + r_four[1] + r_four[2])

    copies = []
    for k in range(1, 4):
        z_to = lax.rem(z_at + k, 4)
        copies.append(pltpu.make_async_remote_copy(
            src_ref=out.at[at(lo_four, piece)], dst_ref=out.at[at(lo_four, piece)],
            send_sem=z_send.at[k + 2], recv_sem=z_recv.at[k + 2], device_id=(plane + 8 * z_to,), device_id_type=MESH))
    for copy in copies:
        copy.start()
    for copy in copies:
        copy.wait()
    exchange(3, out.at[at(lo_three, eighth)], out.at[at(lo_three, eighth)], second)
    exchange(4, out.at[at(lo_two, quarter)], out.at[at(lo_two, quarter)], first)
    exchange(5, out.at[at(lo_one, half)], out.at[at(lo_one, half)], swap_c)


def vmem_call(kernel, outs, name, scratch=(), flops=10**9, collective=None):
    spec = pl.BlockSpec(memory_space=pltpu.VMEM)
    if collective is None:
        params = pltpu.CompilerParams(vmem_limit_bytes=VMEM_LIMIT)
    else:
        params = pltpu.CompilerParams(vmem_limit_bytes=VMEM_LIMIT, collective_id=collective, has_side_effects=True)

    def call(*args):
        return pl.pallas_call(
            kernel,
            out_shape=[jax.ShapeDtypeStruct(s, d) for s, d in outs],
            in_specs=[spec] * len(args),
            out_specs=[spec] * len(outs),
            scratch_shapes=list(scratch),
            compiler_params=params,
            cost_estimate=pl.CostEstimate(flops=flops, bytes_accessed=4 * 10**6, transcendentals=0),
            name=name,
        )(*args)
    return call


def solution(mesh):
    parts = mesh.shape[AXIS]
    row_spec = P(AXIS, None)
    edge_spec = P(AXIS)
    rep_spec = P()
    in_specs = (row_spec, row_spec, row_spec, row_spec, edge_spec, edge_spec) + (rep_spec,) * 8 + (row_spec, row_spec)
    out_specs = (row_spec, row_spec, row_spec) + (rep_spec,) * 8

    def local_step(grid_in, mesh_static, edge_static, send_rows, edge_src, edge_dst, w_grid_in, w_mesh_in, w_edge_in, w_edge_up, w_mesh_up, w_grid_up, w_second, vectors, d_mesh_out, d_grid_out):
        lat = w_grid_up.shape[0]
        n_grid, n_feat = grid_in.shape
        n_mesh = mesh_static.shape[0]
        n_edge = edge_static.shape[0]
        n_slot = send_rows.size
        grid_t, mesh_t, edge_t = grid_in.T, mesh_static.T, edge_static.T
        send_flat = send_rows.reshape(-1)
        send_col, send_row = send_flat[:, None], send_flat[None, :]
        src_col, src_row = edge_src[:, None], edge_src[None, :]
        dst_col, dst_row = edge_dst[:, None], edge_dst[None, :]

        grid_lat, outgoing = vmem_call(grid_fwd_kernel, [((n_grid, lat), BF), ((n_slot, lat), BF)], 'grid_fwd')(
            grid_t, send_col, w_grid_in, w_second, vectors)
        incoming = lax.all_to_all(outgoing, AXIS, 0, 0, tiled=True)
        grid_out, d_lat, mesh_lat, edge_lat, recv_lat, g_a = vmem_call(
            local_kernel, [((n_grid, lat), BF), ((n_grid, lat), F32), ((n_mesh, lat), BF), ((n_edge, lat), BF), ((n_edge, lat), BF), ((2 * lat + 8, lat), F32)],
            'local', flops=4 * 10**9)(
            grid_lat, d_grid_out, mesh_t, edge_t, dst_col, w_mesh_in, w_edge_in, w_edge_up, w_grid_up, w_second, vectors)
        mesh_out, d_mesh_lat, d_edge_lat, d_pre3, d_incoming, g_b = vmem_call(
            edge_kernel,
            [((n_mesh, lat), BF), ((n_mesh, lat), F32), ((n_edge, lat), F32), ((n_edge, lat), BF), ((n_slot, lat), BF), ((7 * lat + 8, lat), F32)],
            'edge',
            scratch=[pltpu.VMEM((n_edge, lat), BF), pltpu.VMEM((n_edge, lat), BF), pltpu.VMEM((n_edge, lat), F32), pltpu.VMEM((n_edge, lat), F32),
                     pltpu.VMEM((n_edge, 128), F32), pltpu.VMEM((n_mesh, lat), BF)], flops=8 * 10**9)(
            incoming, mesh_lat, edge_lat, recv_lat, d_mesh_out, src_col, dst_col, src_row, dst_row, w_edge_up, w_mesh_up, w_second, vectors)
        d_sent = lax.all_to_all(d_incoming, AXIS, 0, 0, tiled=True)
        (g_c,) = vmem_call(embed_bwd_kernel, [((2 * lat + 24, lat), F32)], 'embed_bwd', flops=4 * 10**9)(
            mesh_t, edge_t, dst_row, d_pre3, d_mesh_lat, d_edge_lat, w_mesh_in, w_edge_in, w_edge_up, w_second, vectors)
        d_grid_t, g_d = vmem_call(grid_bwd_kernel, [((n_feat, n_grid), F32), ((lat + 176, lat), F32)], 'grid_bwd')(
            grid_t, send_row, d_sent, d_lat, w_grid_in, w_second, vectors)

        rows = g_a.shape[0] + g_b.shape[0] + g_c.shape[0] + g_d.shape[0]
        piece = -(-rows // (8 * parts)) * 8
        total = piece * parts
        (summed,) = vmem_call(
            functools.partial(sum_kernel, parts), [((total, lat), F32)], 'grad_sum',
            scratch=[pltpu.VMEM((total, lat), F32), pltpu.VMEM((16 * piece, lat), F32), pltpu.VMEM((8 * piece, lat), F32), pltpu.VMEM((4 * piece, lat), F32),
                     pltpu.VMEM((3, piece, lat), F32), pltpu.SemaphoreType.DMA((6,)), pltpu.SemaphoreType.DMA((6,)), pltpu.SemaphoreType.DMA((6,)), pltpu.SemaphoreType.DMA((6,))],
            collective=0)(g_a, g_b, g_c, g_d)
        o_b = g_a.shape[0]
        o_c = o_b + g_b.shape[0]
        o_d = o_c + g_c.shape[0]

        def cut(start, size):
            return summed[start:start + size]
        d_w_grid_up, two5, vec5 = cut(0, lat), cut(lat, lat), cut(2 * lat, 4)
        d_w_mesh_up, d_w_edge_up = cut(o_b, 2 * lat), cut(o_b + 2 * lat, 3 * lat)
        two4, two3, vec4, vec3 = cut(o_b + 5 * lat, lat), cut(o_b + 6 * lat, lat), cut(o_b + 7 * lat, 4), cut(o_b + 7 * lat + 4, 4)
        two1, two2 = cut(o_c, lat), cut(o_c + lat, lat)
        d_w_mesh_in, d_w_edge_in = cut(o_c + 2 * lat, 3), cut(o_c + 2 * lat + 8, 4)
        vec1, vec2 = cut(o_c + 2 * lat + 16, 4), cut(o_c + 2 * lat + 20, 4)
        two0, d_w_grid_in, vec0 = cut(o_d, lat), cut(o_d + lat, n_feat), cut(o_d + lat + 168, 4)
        return (mesh_out, grid_out, d_grid_t.T, d_w_grid_in, d_w_mesh_in, d_w_edge_in, d_w_edge_up, d_w_mesh_up, d_w_grid_up,
                jnp.stack([two0, two1, two2, two3, two4, two5]), jnp.stack([vec0, vec1, vec2, vec3, vec4, vec5]))

    return jax.shard_map(local_step, mesh=mesh, in_specs=in_specs, out_specs=out_specs, check_vma=False)
```

```python
import functools

import jax
import jax.numpy as jnp
from jax import lax
from jax.experimental import pallas as pl
from jax.experimental.pallas import tpu as pltpu
from jax.sharding import PartitionSpec as P

LN_EPS = 1e-5
AXIS = 'gp'
BF = jnp.bfloat16
F32 = jnp.float32
MESH = pl.DeviceIdType.MESH
TILE = 256
VMEM_LIMIT = 60 * 1024 * 1024


def nn(lhs, rhs):
    return jnp.dot(lhs, rhs, preferred_element_type=F32)


def tn(lhs, rhs):
    return lax.dot_general(lhs, rhs, (((0,), (0,)), ((), ())), preferred_element_type=F32)


def nt(lhs, rhs):
    return lax.dot_general(lhs, rhs, (((1,), (1,)), ((), ())), preferred_element_type=F32)


def mlp_fwd(pre_act, w_two, vec):
    act = pre_act + vec[0:1]
    sig = 0.5 * jnp.tanh(0.5 * act) + 0.5
    hidden = (act * sig).astype(BF)
    lin = nn(hidden, w_two) + vec[1:2]
    cen = lin - jnp.mean(lin, axis=-1, keepdims=True)
    inv = lax.rsqrt(jnp.mean(cen * cen, axis=-1, keepdims=True) + LN_EPS)
    normed = cen * inv
    return (act, sig, hidden, normed, inv), normed * vec[2:3] + vec[3:4]


def mlp_bwd(saved, w_two, vec, d_out):
    act, sig, hidden, normed, inv = saved
    d_n = d_out * vec[2:3]
    m_one = jnp.mean(d_n, axis=-1, keepdims=True)
    m_two = jnp.mean(d_n * normed, axis=-1, keepdims=True)
    d_lin = inv * (d_n - m_one - normed * m_two)
    d_lin_bf = d_lin.astype(BF)
    d_two = tn(hidden, d_lin_bf)
    d_hid = nt(d_lin_bf, w_two)
    d_pre = d_hid * (sig * (1.0 + act * (1.0 - sig)))
    d_vec = [jnp.sum(d_pre, axis=0, keepdims=True), jnp.sum(d_lin, axis=0, keepdims=True),
             jnp.sum(d_out * normed, axis=0, keepdims=True), jnp.sum(d_out, axis=0, keepdims=True)]
    return d_pre.astype(BF), d_two, d_vec


def add_vec(ref, base, d_vec):
    for j in range(4):
        ref[base + j:base + j + 1, :] += d_vec[j]


def rows_at(i, size=TILE):
    return pl.ds(pl.multiple_of(i * size, size), size)


def hot_cols(col_idx, width):
    ids = lax.broadcasted_iota(jnp.int32, (col_idx.shape[0], width), 1)
    return jnp.where(ids == col_idx, 1.0, 0.0).astype(BF)


def hot_rows(row_idx, base, height):
    ids = lax.broadcasted_iota(jnp.int32, (height, row_idx.shape[1]), 0) + base
    return jnp.where(ids == row_idx, 1.0, 0.0).astype(BF)


def col_of(idx_ref, i):
    cols = []
    for j in range(TILE // 128):
        row = idx_ref[pl.ds(i * (TILE // 128) + j, 1), :]
        cols.append(jnp.transpose(jnp.broadcast_to(row, (8, 128)))[:, 0:1])
    return jnp.concatenate(cols, axis=0)


def fill_row(idx_ref, row_ref):
    for j in range(idx_ref.shape[0]):
        row_ref[0:1, j * 128:(j + 1) * 128] = idx_ref[j:j + 1, :]


def loop(n, body, events=()):
    def step(i, carry):
        body(i)
        for when, fn in events:
            pl.when(i == when)(fn)
        return carry
    lax.fori_loop(0, n, step, 0)


class Reducer:
    def __init__(self, group, base, rows, place, refs):
        self.own, self.out, r_one, r_two, r_three, r_four, self.send_sem, self.recv_sem = refs
        self.group, self.place = group, place
        self.piece = rows // 32
        self.half, self.quarter, self.eighth = rows // 2, rows // 4, rows // 8
        self.r_one = r_one.at[pl.ds(base // 2, rows // 2)]
        self.r_two = r_two.at[pl.ds(base // 4, rows // 4)]
        self.r_three = r_three.at[pl.ds(base // 8, rows // 8)]
        self.r_four = [r_four.at[k, pl.ds(base // 32, rows // 32)] for k in range(3)]
        self.lo_one = base + place['core'] * self.half
        self.lo_two = self.lo_one + place['bit_one'] * self.quarter
        self.lo_three = self.lo_two + place['bit_two'] * self.eighth
        self.lo_four = self.lo_three + place['z'] * self.piece

    def at(self, start, size):
        return pl.ds(pl.multiple_of(start, 8), size)

    def copies(self, k):
        place, own, out = self.place, self.own, self.out

        def make(slot, src, dst, peer):
            return pltpu.make_async_remote_copy(src_ref=src, dst_ref=dst, send_sem=self.send_sem.at[self.group, slot],
                                                recv_sem=self.recv_sem.at[self.group, slot], device_id=(peer,), device_id_type=MESH)
        if k == 0:
            lo = self.lo_one + (1 - 2 * place['core']) * self.half
            return [make(0, own.at[self.at(lo, self.half)], self.r_one, place['swap_c'])]
        if k == 1:
            lo = self.lo_two + (1 - 2 * place['bit_one']) * self.quarter
            return [make(1, own.at[self.at(lo, self.quarter)], self.r_two, place['first'])]
        if k == 2:
            lo = self.lo_three + (1 - 2 * place['bit_two']) * self.eighth
            return [make(2, own.at[self.at(lo, self.eighth)], self.r_three, place['second'])]
        if k == 3:
            return [make(3 + j, own.at[self.at(self.lo_three + place['z_to'][j] * self.piece, self.piece)], self.r_four[j], place['z_dev'][j]) for j in range(3)]
        if k == 4:
            sl = self.at(self.lo_four, self.piece)
            return [make(6 + j, out.at[sl], out.at[sl], place['z_dev'][j]) for j in range(3)]
        sl = self.at(*((self.lo_three, self.eighth), (self.lo_two, self.quarter), (self.lo_one, self.half))[k - 5])
        return [make(4 + k, out.at[sl], out.at[sl], place[('second', 'first', 'swap_c')[k - 5]])]

    def start(self, k):
        for copy in self.copies(k):
            copy.start()

    def finish(self, k):
        for copy in self.copies(k):
            copy.wait()
        if k == 0:
            sl = self.at(self.lo_one, self.half)
            self.own[sl, :] += self.r_one[...]
        if k == 1:
            sl = self.at(self.lo_two, self.quarter)
            self.own[sl, :] += self.r_two[...]
        if k == 2:
            sl = self.at(self.lo_three, self.eighth)
            self.own[sl, :] += self.r_three[...]
        if k == 3:
            sl = self.at(self.lo_four, self.piece)
            self.out[sl, :] = self.own[sl, :] + (self.r_four[0][...] + self.r_four[1][...] + self.r_four[2][...])

    def step(self, k):
        def fn():
            if k > 0:
                self.finish(k - 1)
            if k < 8:
                self.start(k)
        return fn


def step_kernel(parts, grid_t, mesh_t, edge_t, send_idx, src_idx, dst_idx, w_grid_in, w_mesh_in, w_edge_in, w_two, vec,
                w_edge_up_h, w_mesh_up_h, w_grid_up_h, d_mesh_h, d_grid_h,
                mesh_out_h, grid_out_h, d_grid_t_h, d_wgi, d_wmi, d_wei, d_weu, d_wmu, d_wgu, d_two, d_vec_out,
                w_edge_up, w_mesh_up, w_grid_up, d_mesh, d_grid, mesh_out, grid_out, d_grid_t,
                grid_lat, outgoing, incoming, d_lat, mesh_lat, edge_lat, recv_lat, send_lat, edge_new, act_s, nrm_s, inv_s,
                d_pre4, d_mesh_lat, d_edge_lat, d_pre3, d_incoming, d_sent, send_row, src_row, dst_row,
                own, out, r_one, r_two, r_three, r_four,
                in_sem, out_sem, go_send, go_recv, back_send, back_recv, red_send, red_recv):
    lat = w_two.shape[1]
    n_feat, n_grid = grid_t.shape
    n_mesh, n_edge, n_slot = mesh_lat.shape[0], edge_lat.shape[0], outgoing.shape[0]
    cap = n_slot // parts
    per_tile = TILE // cap
    n_feat_pad = -(-n_feat // 8) * 8
    me = lax.axis_index(AXIS)
    core = lax.rem(me, 2)
    x_at = lax.rem(me // 2, 2)
    y_at = lax.rem(me // 4, 2)
    z_at = me // 8
    plane = me - 8 * z_at
    swap_x = me + 2 * (1 - 2 * x_at)
    swap_y = me + 4 * (1 - 2 * y_at)
    z_to = [lax.rem(z_at + k, 4) for k in range(1, 4)]
    place = dict(core=core, z=z_at, swap_c=me + 1 - 2 * core,
                 first=(1 - core) * swap_x + core * swap_y, second=(1 - core) * swap_y + core * swap_x,
                 bit_one=(1 - core) * x_at + core * y_at, bit_two=(1 - core) * y_at + core * x_at,
                 z_to=z_to, z_dev=[plane + 8 * z for z in z_to])

    barrier = pltpu.get_barrier_semaphore()

    def knock(k, carry):
        pl.semaphore_signal(barrier, inc=1, device_id=(lax.rem(me + k, parts),), device_id_type=MESH)
        return carry
    lax.fori_loop(1, parts, knock, 0)

    loads = [pltpu.make_async_copy(a, b, in_sem.at[k]) for k, (a, b) in enumerate(
        [(d_grid_h, d_grid), (w_grid_up_h, w_grid_up), (w_edge_up_h, w_edge_up), (w_mesh_up_h, w_mesh_up), (d_mesh_h, d_mesh)])]
    for copy in loads:
        copy.start()

    r_wgu, r_two5, r_wmu, r_two4 = 0, lat, 2 * lat, 4 * lat
    r_weu, r_two3 = 5 * lat, 8 * lat
    r_two1, r_two2 = 9 * lat, 10 * lat
    r_two0, r_wgi = 11 * lat, 12 * lat
    r_wmi = r_wgi + n_feat_pad
    r_wei = r_wmi + 8
    r_vec = r_wei + 8
    refs = (own, out, r_one, r_two, r_three, r_four, red_send, red_recv)
    bounds = [0, 5 * lat, 9 * lat, 11 * lat, own.shape[0]]
    red = [Reducer(g, bounds[g], bounds[g + 1] - bounds[g], place, refs) for g in range(4)]

    own[...] = jnp.zeros_like(own)
    fill_row(send_idx, send_row)
    fill_row(src_idx, src_row)
    fill_row(dst_idx, dst_row)

    def embed(i):
        sl = rows_at(i)
        _, emb = mlp_fwd(tn(grid_t[:, sl], w_grid_in[...]), w_two[0], vec[0])
        grid_lat[sl, :] = emb.astype(BF)
    loop(n_grid // TILE, embed)

    pl.semaphore_wait(barrier, parts - 1)

    def part_copy(src, dst, sends, recvs, to, frm):
        return pltpu.make_async_remote_copy(
            src_ref=src.at[pl.ds(pl.multiple_of(to * cap, 8), cap)], dst_ref=dst.at[pl.ds(pl.multiple_of(frm * cap, 8), cap)],
            send_sem=sends.at[to], recv_sem=recvs.at[frm], device_id=(to,), device_id_type=MESH)

    def send_tile(src, dst, sends, recvs, tile):
        for j in range(per_tile):
            to = tile * per_tile + j

            @pl.when(to != me)
            def _():
                part_copy(src, dst, sends, recvs, to, me).start()

            @pl.when(to == me)
            def _():
                own_sl = pl.ds(pl.multiple_of(me * cap, 8), cap)
                dst[own_sl, :] = src[own_sl, :]

    def wait_all(src, dst, sends, recvs):
        def one(k, carry):
            other = lax.rem(me + k, parts)
            part_copy(src, dst, sends, recvs, other, me).wait_send()
            part_copy(src, dst, sends, recvs, me, other).wait_recv()
            return carry
        lax.fori_loop(1, parts, one, 0)

    slot_tiles = n_slot // TILE
    my_tile = me // per_tile

    def turn(i):
        return lax.rem(my_tile + slot_tiles // 2 + i, slot_tiles)

    def pick(i):
        tile = turn(i)
        sl = rows_at(tile)
        outgoing[sl, :] = nn(hot_cols(col_of(send_idx, tile), n_grid), grid_lat[...]).astype(BF)
        send_tile(outgoing, incoming, go_send, go_recv, tile)
    loop(slot_tiles, pick)

    loads[0].wait()
    loads[1].wait()

    def cells(i):
        sl = rows_at(i)
        here = grid_lat[sl, :]
        saved, upd = mlp_fwd(nn(here, w_grid_up[...]), w_two[5], vec[5])
        grid_out[sl, :] = (here.astype(F32) + upd).astype(BF)
        d_top = d_grid[sl, :].astype(F32)
        d_pre, d_two5, d_vec = mlp_bwd(saved, w_two[5], vec[5], d_top)
        own[r_wgu:r_wgu + lat, :] += tn(here, d_pre)
        own[r_two5:r_two5 + lat, :] += d_two5
        add_vec(own, r_vec + 20, d_vec)
        d_lat[sl, :] = d_top + nt(d_pre, w_grid_up[...])
    loop(n_grid // TILE, cells)
    stores = [pltpu.make_async_copy(a, b, out_sem.at[k]) for k, (a, b) in enumerate([(grid_out, grid_out_h), (mesh_out, mesh_out_h), (d_grid_t, d_grid_t_h)])]
    stores[0].start()

    def nodes_in(i):
        sl = rows_at(i)
        _, emb = mlp_fwd(tn(mesh_t[:, sl], w_mesh_in[...]), w_two[1], vec[1])
        mesh_lat[sl, :] = emb.astype(BF)
    loop(n_mesh // TILE, nodes_in)

    def edges_in(i):
        sl = rows_at(i)
        _, emb = mlp_fwd(tn(edge_t[:, sl], w_edge_in[...]), w_two[2], vec[2])
        edge_lat[sl, :] = emb.astype(BF)
        recv_lat[sl, :] = nn(hot_cols(col_of(dst_idx, i), n_mesh), mesh_lat[...]).astype(BF)
    loop(n_edge // TILE, edges_in)

    loads[2].wait()
    loads[3].wait()
    loads[4].wait()
    wait_all(outgoing, incoming, go_send, go_recv)

    def edges_fwd(i):
        sl = rows_at(i)
        sent = nn(hot_cols(col_of(src_idx, i), n_slot), incoming[...]).astype(BF)
        send_lat[sl, :] = sent
        here = edge_lat[sl, :]
        pre = nn(here, w_edge_up[0:lat, :]) + nn(sent, w_edge_up[lat:2 * lat, :]) + nn(recv_lat[sl, :], w_edge_up[2 * lat:3 * lat, :])
        (act, _, _, normed, inv), upd = mlp_fwd(pre, w_two[3], vec[3])
        act_s[sl, :] = act
        nrm_s[sl, :] = normed
        inv_s[sl, :] = jnp.broadcast_to(inv, (TILE, 128))
        edge_new[sl, :] = (here.astype(F32) + upd).astype(BF)
    loop(n_edge // TILE, edges_fwd)

    def nodes(i):
        sl = rows_at(i)
        agg = nn(hot_rows(dst_row[...], i * TILE, TILE), edge_new[...]).astype(BF)
        here = mesh_lat[sl, :]
        saved, upd = mlp_fwd(nn(here, w_mesh_up[0:lat, :]) + nn(agg, w_mesh_up[lat:2 * lat, :]), w_two[4], vec[4])
        mesh_out[sl, :] = (here.astype(F32) + upd).astype(BF)
        d_top = d_mesh[sl, :].astype(F32)
        d_pre, d_two4, d_vec = mlp_bwd(saved, w_two[4], vec[4], d_top)
        d_pre4[sl, :] = d_pre
        own[r_wmu:r_wmu + lat, :] += tn(here, d_pre)
        own[r_wmu + lat:r_wmu + 2 * lat, :] += tn(agg, d_pre)
        own[r_two4:r_two4 + lat, :] += d_two4
        add_vec(own, r_vec + 16, d_vec)
        d_mesh_lat[sl, :] = d_top + nt(d_pre, w_mesh_up[0:lat, :])
    loop(n_mesh // TILE, nodes)
    stores[1].start()

    def edges_bwd(i):
        sl = rows_at(i)
        picked = nn(hot_cols(col_of(dst_idx, i), n_mesh), d_pre4[...]).astype(BF)
        d_new = nt(picked, w_mesh_up[lat:2 * lat, :])
        act = act_s[sl, :]
        sig = 0.5 * jnp.tanh(0.5 * act) + 0.5
        hidden = (act * sig).astype(BF)
        d_pre, d_two3, d_vec = mlp_bwd((act, sig, hidden, nrm_s[sl, :], inv_s[sl, 0:1]), w_two[3], vec[3], d_new)
        d_pre3[sl, :] = d_pre
        own[r_two3:r_two3 + lat, :] += d_two3
        add_vec(own, r_vec + 12, d_vec)
        own[r_weu:r_weu + lat, :] += tn(edge_lat[sl, :], d_pre)
        own[r_weu + lat:r_weu + 2 * lat, :] += tn(send_lat[sl, :], d_pre)
        own[r_weu + 2 * lat:r_weu + 3 * lat, :] += tn(recv_lat[sl, :], d_pre)
        d_edge_lat[sl, :] = d_new + nt(d_pre, w_edge_up[0:lat, :])
    n_et, n_nt, n_gt = n_edge // TILE, n_mesh // TILE, n_grid // TILE
    red[0].start(0)
    loop(n_et, edges_bwd, [(n_et * 2 // 12, red[0].step(1)), (n_et * 7 // 12, red[0].step(2)), (n_et - 1, red[0].step(3))])

    red[1].start(0)

    def slots(i):
        tile = turn(i)
        sl = rows_at(tile)
        d_slot = nn(hot_rows(src_row[...], tile * TILE, TILE), d_pre3[...]).astype(BF)
        d_incoming[sl, :] = nt(d_slot, w_edge_up[lat:2 * lat, :]).astype(BF)
        send_tile(d_incoming, d_sent, back_send, back_recv, tile)
    loop(slot_tiles, slots, [(slot_tiles - 1, red[1].step(1))])

    def nodes_bwd(i):
        sl = rows_at(i)
        d_node = nn(hot_rows(dst_row[...], i * TILE, TILE), d_pre3[...]).astype(BF)
        d_top = d_mesh_lat[sl, :] + nt(d_node, w_edge_up[2 * lat:3 * lat, :])
        feat = mesh_t[:, sl]
        saved, _ = mlp_fwd(tn(feat, w_mesh_in[...]), w_two[1], vec[1])
        d_pre, d_two1, d_vec = mlp_bwd(saved, w_two[1], vec[1], d_top)
        own[r_two1:r_two1 + lat, :] += d_two1
        own[r_wmi:r_wmi + 3, :] += nn(feat, d_pre)
        add_vec(own, r_vec + 4, d_vec)
    loop(n_nt, nodes_bwd, [(n_nt * 2 // 8, red[0].step(4)), (n_nt - 1, red[1].step(2))])

    def edges_in_bwd(i):
        sl = rows_at(i)
        feat = edge_t[:, sl]
        saved, _ = mlp_fwd(tn(feat, w_edge_in[...]), w_two[2], vec[2])
        d_pre, d_two2, d_vec = mlp_bwd(saved, w_two[2], vec[2], d_edge_lat[sl, :])
        own[r_two2:r_two2 + lat, :] += d_two2
        own[r_wei:r_wei + 4, :] += nn(feat, d_pre)
        add_vec(own, r_vec + 8, d_vec)
    loop(n_et, edges_in_bwd, [(n_et * 2 // 12, red[0].step(5)), (n_et * 5 // 12, red[1].step(3)), (n_et * 7 // 12, red[0].step(6)), (n_et - 1, red[0].step(7))])

    red[2].start(0)
    wait_all(d_incoming, d_sent, back_send, back_recv)
    red[1].step(4)()

    def grid_bwd(i):
        sl = rows_at(i)
        d_top = d_lat[sl, :] + nn(hot_rows(send_row[...], i * TILE, TILE), d_sent[...])
        feat = grid_t[:, sl]
        saved, _ = mlp_fwd(tn(feat, w_grid_in[...]), w_two[0], vec[0])
        d_pre, d_two0, d_vec = mlp_bwd(saved, w_two[0], vec[0], d_top)
        own[r_two0:r_two0 + lat, :] += d_two0
        own[r_wgi:r_wgi + n_feat, :] += nn(feat, d_pre)
        add_vec(own, r_vec, d_vec)
        d_grid_t[:, sl] = nt(w_grid_in[...], d_pre)
    loop(n_gt, grid_bwd, [(0, red[2].step(1)), (n_gt * 2 // 8, red[0].step(8)), (n_gt * 3 // 8, red[1].step(5)), (n_gt * 4 // 8, red[2].step(2)), (n_gt * 5 // 8, red[1].step(6)), (n_gt - 1, red[2].step(3))])
    stores[2].start()

    red[3].start(0)
    red[1].step(7)()
    red[3].step(1)()
    red[2].step(4)()
    red[1].step(8)()
    red[3].step(2)()
    red[2].step(5)()
    red[3].step(3)()
    red[2].step(6)()
    red[3].step(4)()
    red[2].step(7)()
    red[2].step(8)()
    puts = [(r_weu, 3 * lat, d_weu), (r_wmu, 2 * lat, d_wmu), (r_wgu, lat, d_wgu), (r_two1, lat, d_two.at[1]),
            (r_two2, lat, d_two.at[2]), (r_two3, lat, d_two.at[3]), (r_two4, lat, d_two.at[4]), (r_two5, lat, d_two.at[5])]
    moves = [pltpu.make_async_copy(out.at[pl.ds(a, n)], ref, out_sem.at[3 + k]) for k, (a, n, ref) in enumerate(puts)]
    for move in moves:
        move.start()
    for k in range(5, 9):
        red[3].step(k)()
    last = pltpu.make_async_copy(out.at[pl.ds(r_two0, lat)], d_two.at[0], out_sem.at[11])
    last.start()
    d_wgi[...] = out[r_wgi:r_wgi + n_feat, :]
    d_wmi[...] = out[r_wmi:r_wmi + 3, :]
    d_wei[...] = out[r_wei:r_wei + 4, :]
    for k in range(6):
        d_vec_out[k] = out[r_vec + 4 * k:r_vec + 4 * k + 4, :]
    for copy in stores + moves + [last]:
        copy.wait()


def solution(mesh):
    parts = mesh.shape[AXIS]
    row_spec = P(AXIS, None)
    edge_spec = P(AXIS)
    rep_spec = P()
    in_specs = (row_spec, row_spec, row_spec, row_spec, edge_spec, edge_spec) + (rep_spec,) * 8 + (row_spec, row_spec)
    out_specs = (row_spec, row_spec, row_spec) + (rep_spec,) * 8

    def local_step(grid_in, mesh_static, edge_static, send_rows, edge_src, edge_dst, w_grid_in, w_mesh_in, w_edge_in, w_edge_up, w_mesh_up, w_grid_up, w_second, vectors, d_mesh_out, d_grid_out):
        lat = w_grid_up.shape[0]
        n_grid, n_feat = grid_in.shape
        n_mesh = mesh_static.shape[0]
        n_edge = edge_static.shape[0]
        n_slot = send_rows.size
        small = -(-n_feat // 8) * 8 + 8 + 8 + 24
        total = 11 * lat + -(-(lat + small) // 256) * 256
        near = pl.BlockSpec(memory_space=pltpu.VMEM)
        far = pl.BlockSpec(memory_space=pl.ANY)

        def sds(shape, dtype):
            return jax.ShapeDtypeStruct(shape, dtype)
        outs = [sds((n_mesh, lat), BF), sds((n_grid, lat), BF), sds((n_feat, n_grid), F32), sds(w_grid_in.shape, F32), sds(w_mesh_in.shape, F32), sds(w_edge_in.shape, F32),
                sds(w_edge_up.shape, F32), sds(w_mesh_up.shape, F32), sds(w_grid_up.shape, F32), sds(w_second.shape, F32), sds(vectors.shape, F32)]
        out_specs = [far, far, far, near, near, near, far, far, far, far, near]
        V = pltpu.VMEM
        D = pltpu.SemaphoreType.DMA
        scratch = [V(w_edge_up.shape, BF), V(w_mesh_up.shape, BF), V(w_grid_up.shape, BF), V((n_mesh, lat), BF), V((n_grid, lat), BF),
                   V((n_mesh, lat), BF), V((n_grid, lat), BF), V((n_feat, n_grid), F32),
                   V((n_grid, lat), BF), V((n_slot, lat), BF), V((n_slot, lat), BF), V((n_grid, lat), F32), V((n_mesh, lat), BF),
                   V((n_edge, lat), BF), V((n_edge, lat), BF), V((n_edge, lat), BF), V((n_edge, lat), BF), V((n_edge, lat), F32), V((n_edge, lat), F32), V((n_edge, 128), F32),
                   V((n_mesh, lat), BF), V((n_mesh, lat), F32), V((n_edge, lat), F32), V((n_edge, lat), BF), V((n_slot, lat), BF), V((n_slot, lat), BF),
                   V((1, n_slot), jnp.int32), V((1, n_edge), jnp.int32), V((1, n_edge), jnp.int32),
                   V((total, lat), F32), V((total, lat), F32), V((total // 2, lat), F32), V((total // 4, lat), F32), V((total // 8, lat), F32), V((3, total // 32, lat), F32),
                   D((5,)), D((12,)), D((parts,)), D((parts,)), D((parts,)), D((parts,)), D((4, 12)), D((4, 12))]
        res = pl.pallas_call(
            functools.partial(step_kernel, parts),
            out_shape=outs,
            in_specs=[near] * 11 + [far] * 5,
            out_specs=out_specs,
            scratch_shapes=scratch,
            compiler_params=pltpu.CompilerParams(vmem_limit_bytes=VMEM_LIMIT, collective_id=0, has_side_effects=True),
            name='step',
        )(grid_in.T, mesh_static.T, edge_static.T, send_rows.reshape(-1, 128), edge_src.reshape(-1, 128), edge_dst.reshape(-1, 128),
          w_grid_in, w_mesh_in, w_edge_in, w_second, vectors, w_edge_up, w_mesh_up, w_grid_up, d_mesh_out, d_grid_out)
        return (res[0], res[1], res[2].T) + tuple(res[3:])

    return jax.shard_map(local_step, mesh=mesh, in_specs=in_specs, out_specs=out_specs, check_vma=False)
```

```python
import functools

import jax
import jax.numpy as jnp
from jax import lax
from jax.experimental import pallas as pl
from jax.experimental.pallas import tpu as pltpu
from jax.sharding import PartitionSpec as P

LN_EPS = 1e-5
AXIS = 'gp'
BF = jnp.bfloat16
F32 = jnp.float32
MESH = pl.DeviceIdType.MESH
TILE = 1024
SEND_TILE = 512
VMEM_LIMIT = 60 * 1024 * 1024


def nn(lhs, rhs):
    return jnp.dot(lhs, rhs, preferred_element_type=F32)


def tn(lhs, rhs):
    return lax.dot_general(lhs, rhs, (((0,), (0,)), ((), ())), preferred_element_type=F32)


def nt(lhs, rhs):
    return lax.dot_general(lhs, rhs, (((1,), (1,)), ((), ())), preferred_element_type=F32)


def mlp_fwd(pre_act, w_two, vec):
    act = pre_act + vec[0:1]
    sig = 0.5 * jnp.tanh(0.5 * act) + 0.5
    hidden = (act * sig).astype(BF)
    lin = nn(hidden, w_two) + vec[1:2]
    cen = lin - jnp.mean(lin, axis=-1, keepdims=True)
    inv = lax.rsqrt(jnp.mean(cen * cen, axis=-1, keepdims=True) + LN_EPS)
    normed = cen * inv
    return (act, sig, hidden, normed, inv), normed * vec[2:3] + vec[3:4]


def mlp_bwd(saved, w_two, vec, d_out):
    act, sig, hidden, normed, inv = saved
    d_n = d_out * vec[2:3]
    m_one = jnp.mean(d_n, axis=-1, keepdims=True)
    m_two = jnp.mean(d_n * normed, axis=-1, keepdims=True)
    d_lin = inv * (d_n - m_one - normed * m_two)
    d_lin_bf = d_lin.astype(BF)
    d_two = tn(hidden, d_lin_bf)
    d_hid = nt(d_lin_bf, w_two)
    d_pre = d_hid * (sig * (1.0 + act * (1.0 - sig)))
    d_vec = [jnp.sum(d_pre, axis=0, keepdims=True), jnp.sum(d_lin, axis=0, keepdims=True),
             jnp.sum(d_out * normed, axis=0, keepdims=True), jnp.sum(d_out, axis=0, keepdims=True)]
    return d_pre.astype(BF), d_two, d_vec


def add_vec(ref, base, d_vec):
    for j in range(4):
        ref[base + j:base + j + 1, :] += d_vec[j]


def rows_at(i, size):
    return pl.ds(pl.multiple_of(i * size, size), size)


def hot_cols(col_idx, width):
    ids = lax.broadcasted_iota(jnp.int32, (col_idx.shape[0], width), 1)
    return jnp.where(ids == col_idx, 1.0, 0.0).astype(BF)


def hot_rows(row_idx, base, height):
    ids = lax.broadcasted_iota(jnp.int32, (height, row_idx.shape[1]), 0) + base
    return jnp.where(ids == row_idx, 1.0, 0.0).astype(BF)


def col_of(row_ref, i, size):
    cols = []
    for j in range(size // 128):
        row = row_ref[0:1, pl.ds(pl.multiple_of(i * size, size) + j * 128, 128)]
        cols.append(jnp.transpose(jnp.broadcast_to(row, (8, 128)))[:, 0:1])
    return jnp.concatenate(cols, axis=0)


def fill_row(idx_ref, row_ref):
    wide = idx_ref.shape[1]
    for j in range(idx_ref.shape[0]):
        row_ref[0:1, j * wide:(j + 1) * wide] = idx_ref[j:j + 1, :]


def loop(n, body, events=()):
    def step(i, carry):
        body(i)
        for when, fn in events:
            pl.when(i == when)(fn)
        return carry
    lax.fori_loop(0, n, step, 0)


class Reducer:
    def __init__(self, group, base, rows, place, refs):
        self.own, self.out, r_one, r_two, r_three, r_four, self.send_sem, self.recv_sem = refs
        self.group, self.place = group, place
        self.piece = rows // 32
        self.half, self.quarter, self.eighth = rows // 2, rows // 4, rows // 8
        self.r_one = r_one.at[pl.ds(base // 2, rows // 2)]
        self.r_two = r_two.at[pl.ds(base // 4, rows // 4)]
        self.r_three = r_three.at[pl.ds(base // 8, rows // 8)]
        self.r_four = [r_four.at[k, pl.ds(base // 32, rows // 32)] for k in range(3)]
        self.lo_one = base + place['core'] * self.half
        self.lo_two = self.lo_one + place['bit_one'] * self.quarter
        self.lo_three = self.lo_two + place['bit_two'] * self.eighth
        self.lo_four = self.lo_three + place['z'] * self.piece

    def at(self, start, size):
        return pl.ds(pl.multiple_of(start, 8), size)

    def copies(self, k):
        place, own, out = self.place, self.own, self.out

        def make(slot, src, dst, peer):
            return pltpu.make_async_remote_copy(src_ref=src, dst_ref=dst, send_sem=self.send_sem.at[self.group, slot],
                                                recv_sem=self.recv_sem.at[self.group, slot], device_id=(peer,), device_id_type=MESH)
        if k == 0:
            lo = self.lo_one + (1 - 2 * place['core']) * self.half
            return [make(0, own.at[self.at(lo, self.half)], self.r_one, place['swap_c'])]
        if k == 1:
            lo = self.lo_two + (1 - 2 * place['bit_one']) * self.quarter
            return [make(1, own.at[self.at(lo, self.quarter)], self.r_two, place['first'])]
        if k == 2:
            lo = self.lo_three + (1 - 2 * place['bit_two']) * self.eighth
            return [make(2, own.at[self.at(lo, self.eighth)], self.r_three, place['second'])]
        if k == 3:
            return [make(3 + j, own.at[self.at(self.lo_three + place['z_to'][j] * self.piece, self.piece)], self.r_four[j], place['z_dev'][j]) for j in range(3)]
        if k == 4:
            sl = self.at(self.lo_four, self.piece)
            return [make(6 + j, out.at[sl], out.at[sl], place['z_dev'][j]) for j in range(3)]
        sl = self.at(*((self.lo_three, self.eighth), (self.lo_two, self.quarter), (self.lo_one, self.half))[k - 5])
        return [make(4 + k, out.at[sl], out.at[sl], place[('second', 'first', 'swap_c')[k - 5]])]

    def start(self, k):
        for copy in self.copies(k):
            copy.start()

    def finish(self, k):
        for copy in self.copies(k):
            copy.wait()
        if k == 0:
            sl = self.at(self.lo_one, self.half)
            self.own[sl, :] += self.r_one[...]
        if k == 1:
            sl = self.at(self.lo_two, self.quarter)
            self.own[sl, :] += self.r_two[...]
        if k == 2:
            sl = self.at(self.lo_three, self.eighth)
            self.own[sl, :] += self.r_three[...]
        if k == 3:
            sl = self.at(self.lo_four, self.piece)
            self.out[sl, :] = self.own[sl, :] + (self.r_four[0][...] + self.r_four[1][...] + self.r_four[2][...])

    def step(self, k):
        def fn():
            if k > 0:
                self.finish(k - 1)
            if k < 8:
                self.start(k)
        return fn


def step_kernel(parts, grid_t, mesh_t, edge_t, send_idx, src_idx, dst_idx, w_grid_in, w_mesh_in, w_edge_in, w_two, vec,
                w_edge_up_h, w_mesh_up_h, w_grid_up_h, d_mesh_h, d_grid_h,
                mesh_out_h, grid_out_h, d_grid_t_h, d_wgi, d_wmi, d_wei, d_weu, d_wmu, d_wgu, d_two, d_vec_out,
                w_edge_up, w_mesh_up, w_grid_up, d_mesh, d_grid, mesh_out, grid_out, d_grid_t,
                grid_lat, outgoing, incoming, d_lat, mesh_lat, edge_lat, recv_lat, send_lat, edge_new, act_s, nrm_s, inv_s,
                d_pre4, d_mesh_lat, d_edge_lat, d_pre3, d_incoming, d_sent, send_row, src_row, dst_row,
                own, out, r_one, r_two, r_three, r_four,
                in_sem, out_sem, go_send, go_recv, back_send, back_recv, red_send, red_recv):
    lat = w_two.shape[1]
    n_feat, n_grid = grid_t.shape
    n_mesh, n_edge, n_slot = mesh_lat.shape[0], edge_lat.shape[0], outgoing.shape[0]
    cap = n_slot // parts
    per_tile = min(SEND_TILE, n_slot) // cap
    n_feat_pad = -(-n_feat // 8) * 8
    t_send, t_slot = min(SEND_TILE, n_slot), min(SEND_TILE, n_slot)
    t_grid, t_mesh, t_edge = min(TILE, n_grid), min(TILE, n_mesh), min(TILE, n_edge)
    n_gt, n_nt, n_et = n_grid // t_grid, n_mesh // t_mesh, n_edge // t_edge
    me = lax.axis_index(AXIS)
    core = lax.rem(me, 2)
    x_at = lax.rem(me // 2, 2)
    y_at = lax.rem(me // 4, 2)
    z_at = me // 8
    plane = me - 8 * z_at
    swap_x = me + 2 * (1 - 2 * x_at)
    swap_y = me + 4 * (1 - 2 * y_at)
    z_to = [lax.rem(z_at + k, 4) for k in range(1, 4)]
    place = dict(core=core, z=z_at, swap_c=me + 1 - 2 * core,
                 first=(1 - core) * swap_x + core * swap_y, second=(1 - core) * swap_y + core * swap_x,
                 bit_one=(1 - core) * x_at + core * y_at, bit_two=(1 - core) * y_at + core * x_at,
                 z_to=z_to, z_dev=[plane + 8 * z for z in z_to])

    barrier = pltpu.get_barrier_semaphore()

    def knock(k, carry):
        pl.semaphore_signal(barrier, inc=1, device_id=(lax.rem(me + k, parts),), device_id_type=MESH)
        return carry
    lax.fori_loop(1, parts, knock, 0)

    loads = [pltpu.make_async_copy(a, b, in_sem.at[k]) for k, (a, b) in enumerate(
        [(d_grid_h, d_grid), (w_grid_up_h, w_grid_up), (w_edge_up_h, w_edge_up), (w_mesh_up_h, w_mesh_up), (d_mesh_h, d_mesh)])]
    for copy in loads:
        copy.start()

    r_wgu, r_two5, r_wmu, r_two4 = 0, lat, 2 * lat, 4 * lat
    r_weu, r_two3 = 5 * lat, 8 * lat
    r_two1, r_two2 = 9 * lat, 10 * lat
    r_two0, r_wgi = 11 * lat, 12 * lat
    r_wmi = r_wgi + n_feat_pad
    r_wei = r_wmi + 8
    r_vec = r_wei + 8
    refs = (own, out, r_one, r_two, r_three, r_four, red_send, red_recv)
    bounds = [0, 2 * lat, 5 * lat, 9 * lat, 11 * lat, own.shape[0]]
    red = [Reducer(g, bounds[g], bounds[g + 1] - bounds[g], place, refs) for g in range(5)]

    own[...] = jnp.zeros_like(own)
    fill_row(send_idx, send_row)
    fill_row(src_idx, src_row)
    fill_row(dst_idx, dst_row)

    def embed(i):
        sl = rows_at(i, t_grid)
        _, emb = mlp_fwd(tn(grid_t[:, sl], w_grid_in[...]), w_two[0], vec[0])
        grid_lat[sl, :] = emb.astype(BF)
    loop(n_gt, embed)

    pl.semaphore_wait(barrier, parts - 1)

    def part_copy(src, dst, sends, recvs, to, frm):
        return pltpu.make_async_remote_copy(
            src_ref=src.at[pl.ds(pl.multiple_of(to * cap, 8), cap)], dst_ref=dst.at[pl.ds(pl.multiple_of(frm * cap, 8), cap)],
            send_sem=sends.at[to], recv_sem=recvs.at[frm], device_id=(to,), device_id_type=MESH)

    def send_tile(src, dst, sends, recvs, tile):
        for j in range(per_tile):
            to = tile * per_tile + j

            @pl.when(to != me)
            def _():
                part_copy(src, dst, sends, recvs, to, me).start()

            @pl.when(to == me)
            def _():
                own_sl = pl.ds(pl.multiple_of(me * cap, 8), cap)
                dst[own_sl, :] = src[own_sl, :]

    def wait_all(src, dst, sends, recvs):
        def one(k, carry):
            other = lax.rem(me + k, parts)
            part_copy(src, dst, sends, recvs, other, me).wait_send()
            part_copy(src, dst, sends, recvs, me, other).wait_recv()
            return carry
        lax.fori_loop(1, parts, one, 0)

    slot_tiles = n_slot // t_send
    my_tile = me // per_tile

    def turn(i):
        return lax.rem(my_tile + slot_tiles // 2 + i, slot_tiles)

    def pick(i):
        tile = turn(i)
        sl = rows_at(tile, t_send)
        outgoing[sl, :] = nn(hot_cols(col_of(send_row, tile, t_send), n_grid), grid_lat[...]).astype(BF)
        send_tile(outgoing, incoming, go_send, go_recv, tile)
    loop(slot_tiles, pick)

    loads[0].wait()
    loads[1].wait()

    def cells(i):
        sl = rows_at(i, t_grid)
        here = grid_lat[sl, :]
        saved, upd = mlp_fwd(nn(here, w_grid_up[...]), w_two[5], vec[5])
        grid_out[sl, :] = (here.astype(F32) + upd).astype(BF)
        d_top = d_grid[sl, :].astype(F32)
        d_pre, d_two5, d_vec = mlp_bwd(saved, w_two[5], vec[5], d_top)
        own[r_wgu:r_wgu + lat, :] += tn(here, d_pre)
        own[r_two5:r_two5 + lat, :] += d_two5
        add_vec(own, r_vec + 20, d_vec)
        d_lat[sl, :] = d_top + nt(d_pre, w_grid_up[...])
    loop(n_gt, cells)
    stores = [pltpu.make_async_copy(a, b, out_sem.at[k]) for k, (a, b) in enumerate([(grid_out, grid_out_h), (mesh_out, mesh_out_h), (d_grid_t, d_grid_t_h)])]
    stores[0].start()
    red[0].start(0)
    loads[2].wait()
    loads[3].wait()
    loads[4].wait()

    def nodes_in(i):
        sl = rows_at(i, t_mesh)
        _, emb = mlp_fwd(tn(mesh_t[:, sl], w_mesh_in[...]), w_two[1], vec[1])
        here = emb.astype(BF)
        mesh_lat[sl, :] = here
        d_mesh_lat[sl, :] = nn(here, w_mesh_up[0:lat, :])
    loop(n_nt, nodes_in)

    def edges_in(i):
        sl = rows_at(i, t_edge)
        _, emb = mlp_fwd(tn(edge_t[:, sl], w_edge_in[...]), w_two[2], vec[2])
        here = emb.astype(BF)
        edge_lat[sl, :] = here
        recv = nn(hot_cols(col_of(dst_row, i, t_edge), n_mesh), mesh_lat[...]).astype(BF)
        recv_lat[sl, :] = recv
        act_s[sl, :] = nn(here, w_edge_up[0:lat, :]) + nn(recv, w_edge_up[2 * lat:3 * lat, :])
    loop(n_et, edges_in)

    wait_all(outgoing, incoming, go_send, go_recv)
    red[0].step(1)()

    def edges_fwd(i):
        sl = rows_at(i, t_edge)
        sent = nn(hot_cols(col_of(src_row, i, t_edge), n_slot), incoming[...]).astype(BF)
        send_lat[sl, :] = sent
        (act, _, _, normed, inv), upd = mlp_fwd(act_s[sl, :] + nn(sent, w_edge_up[lat:2 * lat, :]), w_two[3], vec[3])
        act_s[sl, :] = act
        nrm_s[sl, :] = normed
        inv_s[sl, :] = jnp.broadcast_to(inv, (t_edge, 128))
        edge_new[sl, :] = (edge_lat[sl, :].astype(F32) + upd).astype(BF)
    loop(n_et, edges_fwd, [(0, red[0].step(2)), (n_et // 2, red[0].step(3)), (n_et - 1, red[0].step(4))])

    def nodes(i):
        sl = rows_at(i, t_mesh)
        agg = nn(hot_rows(dst_row[...], i * t_mesh, t_mesh), edge_new[...]).astype(BF)
        here = mesh_lat[sl, :]
        saved, upd = mlp_fwd(d_mesh_lat[sl, :] + nn(agg, w_mesh_up[lat:2 * lat, :]), w_two[4], vec[4])
        mesh_out[sl, :] = (here.astype(F32) + upd).astype(BF)
        d_top = d_mesh[sl, :].astype(F32)
        d_pre, d_two4, d_vec = mlp_bwd(saved, w_two[4], vec[4], d_top)
        d_pre4[sl, :] = d_pre
        own[r_wmu:r_wmu + lat, :] += tn(here, d_pre)
        own[r_wmu + lat:r_wmu + 2 * lat, :] += tn(agg, d_pre)
        own[r_two4:r_two4 + lat, :] += d_two4
        add_vec(own, r_vec + 16, d_vec)
        d_mesh_lat[sl, :] = d_top + nt(d_pre, w_mesh_up[0:lat, :])
    loop(n_nt, nodes, [(0, red[0].step(5)), (n_nt - 1, red[0].step(6))])
    stores[1].start()
    red[1].start(0)

    def edges_bwd(i):
        sl = rows_at(i, t_edge)
        picked = nn(hot_cols(col_of(dst_row, i, t_edge), n_mesh), d_pre4[...]).astype(BF)
        d_new = nt(picked, w_mesh_up[lat:2 * lat, :])
        act = act_s[sl, :]
        sig = 0.5 * jnp.tanh(0.5 * act) + 0.5
        hidden = (act * sig).astype(BF)
        d_pre, d_two3, d_vec = mlp_bwd((act, sig, hidden, nrm_s[sl, :], inv_s[sl, 0:1]), w_two[3], vec[3], d_new)
        d_pre3[sl, :] = d_pre
        own[r_two3:r_two3 + lat, :] += d_two3
        add_vec(own, r_vec + 12, d_vec)
        d_edge_lat[sl, :] = d_new
    loop(n_et, edges_bwd, [(0, red[0].step(7)), (0, red[1].step(1)), (n_et // 2, red[0].step(8)), (n_et // 2, red[1].step(2)), (n_et - 1, red[1].step(3))])

    def slots(i):
        tile = turn(i)
        sl = rows_at(tile, t_send)
        d_slot = nn(hot_rows(src_row[...], tile * t_send, t_send), d_pre3[...]).astype(BF)
        d_incoming[sl, :] = nt(d_slot, w_edge_up[lat:2 * lat, :]).astype(BF)
        send_tile(d_incoming, d_sent, back_send, back_recv, tile)
    loop(slot_tiles, slots)

    def edges_grad(i):
        sl = rows_at(i, t_edge)
        d_pre = d_pre3[sl, :]
        own[r_weu:r_weu + lat, :] += tn(edge_lat[sl, :], d_pre)
        own[r_weu + lat:r_weu + 2 * lat, :] += tn(send_lat[sl, :], d_pre)
        own[r_weu + 2 * lat:r_weu + 3 * lat, :] += tn(recv_lat[sl, :], d_pre)
        d_edge_lat[sl, :] += nt(d_pre, w_edge_up[0:lat, :])
    loop(n_et, edges_grad)
    red[2].start(0)

    def nodes_bwd(i):
        sl = rows_at(i, t_mesh)
        d_node = nn(hot_rows(dst_row[...], i * t_mesh, t_mesh), d_pre3[...]).astype(BF)
        d_top = d_mesh_lat[sl, :] + nt(d_node, w_edge_up[2 * lat:3 * lat, :])
        feat = mesh_t[:, sl]
        saved, _ = mlp_fwd(tn(feat, w_mesh_in[...]), w_two[1], vec[1])
        d_pre, d_two1, d_vec = mlp_bwd(saved, w_two[1], vec[1], d_top)
        own[r_two1:r_two1 + lat, :] += d_two1
        own[r_wmi:r_wmi + 3, :] += nn(feat, d_pre)
        add_vec(own, r_vec + 4, d_vec)
    loop(n_nt, nodes_bwd, [(0, red[2].step(1)), (n_nt - 1, red[2].step(2))])

    def edges_in_bwd(i):
        sl = rows_at(i, t_edge)
        feat = edge_t[:, sl]
        saved, _ = mlp_fwd(tn(feat, w_edge_in[...]), w_two[2], vec[2])
        d_pre, d_two2, d_vec = mlp_bwd(saved, w_two[2], vec[2], d_edge_lat[sl, :])
        own[r_two2:r_two2 + lat, :] += d_two2
        own[r_wei:r_wei + 4, :] += nn(feat, d_pre)
        add_vec(own, r_vec + 8, d_vec)
    loop(n_et, edges_in_bwd)

    red[3].start(0)
    wait_all(d_incoming, d_sent, back_send, back_recv)
    red[1].step(4)()
    red[2].step(3)()
    red[3].step(1)()

    def grid_bwd(i):
        sl = rows_at(i, t_grid)
        d_top = d_lat[sl, :] + nn(hot_rows(send_row[...], i * t_grid, t_grid), d_sent[...])
        feat = grid_t[:, sl]
        saved, _ = mlp_fwd(tn(feat, w_grid_in[...]), w_two[0], vec[0])
        d_pre, d_two0, d_vec = mlp_bwd(saved, w_two[0], vec[0], d_top)
        own[r_two0:r_two0 + lat, :] += d_two0
        own[r_wgi:r_wgi + n_feat, :] += nn(feat, d_pre)
        add_vec(own, r_vec, d_vec)
        d_grid_t[:, sl] = nt(w_grid_in[...], d_pre)
    loop(n_gt, grid_bwd, [(0, red[1].step(5)), (0, red[2].step(4)), (0, red[3].step(2)), (n_gt - 1, red[1].step(6)), (n_gt - 1, red[2].step(5)), (n_gt - 1, red[3].step(3))])

    red[4].start(0)
    stores[2].start()
    for g, k in ((1, 7), (2, 6), (3, 4), (4, 1), (1, 8), (2, 7), (3, 5), (4, 2), (2, 8), (3, 6), (4, 3), (3, 7), (4, 4), (3, 8)):
        red[g].step(k)()
    puts = [(r_weu, 3 * lat, d_weu), (r_wmu, 2 * lat, d_wmu), (r_wgu, lat, d_wgu), (r_two1, lat, d_two.at[1]),
            (r_two2, lat, d_two.at[2]), (r_two3, lat, d_two.at[3]), (r_two4, lat, d_two.at[4]), (r_two5, lat, d_two.at[5])]
    moves = [pltpu.make_async_copy(out.at[pl.ds(a, n)], ref, out_sem.at[3 + k]) for k, (a, n, ref) in enumerate(puts)]
    for move in moves:
        move.start()
    for k in range(5, 9):
        red[4].step(k)()
    last = pltpu.make_async_copy(out.at[pl.ds(r_two0, lat)], d_two.at[0], out_sem.at[11])
    last.start()
    d_wgi[...] = out[r_wgi:r_wgi + n_feat, :]
    d_wmi[...] = out[r_wmi:r_wmi + 3, :]
    d_wei[...] = out[r_wei:r_wei + 4, :]
    for k in range(6):
        d_vec_out[k] = out[r_vec + 4 * k:r_vec + 4 * k + 4, :]
    for copy in stores + moves + [last]:
        copy.wait()


def solution(mesh):
    parts = mesh.shape[AXIS]
    row_spec = P(AXIS, None)
    edge_spec = P(AXIS)
    rep_spec = P()
    in_specs = (row_spec, row_spec, row_spec, row_spec, edge_spec, edge_spec) + (rep_spec,) * 8 + (row_spec, row_spec)
    out_specs = (row_spec, row_spec, row_spec) + (rep_spec,) * 8

    def local_step(grid_in, mesh_static, edge_static, send_rows, edge_src, edge_dst, w_grid_in, w_mesh_in, w_edge_in, w_edge_up, w_mesh_up, w_grid_up, w_second, vectors, d_mesh_out, d_grid_out):
        lat = w_grid_up.shape[0]
        n_grid, n_feat = grid_in.shape
        n_mesh = mesh_static.shape[0]
        n_edge = edge_static.shape[0]
        n_slot = send_rows.size
        small = -(-n_feat // 8) * 8 + 8 + 8 + 24
        total = 11 * lat + -(-(lat + small) // 256) * 256
        near = pl.BlockSpec(memory_space=pltpu.VMEM)
        far = pl.BlockSpec(memory_space=pl.ANY)

        def sds(shape, dtype):
            return jax.ShapeDtypeStruct(shape, dtype)
        outs = [sds((n_mesh, lat), BF), sds((n_grid, lat), BF), sds((n_feat, n_grid), F32), sds(w_grid_in.shape, F32), sds(w_mesh_in.shape, F32), sds(w_edge_in.shape, F32),
                sds(w_edge_up.shape, F32), sds(w_mesh_up.shape, F32), sds(w_grid_up.shape, F32), sds(w_second.shape, F32), sds(vectors.shape, F32)]
        out_specs = [far, far, far, near, near, near, far, far, far, far, near]
        V = pltpu.VMEM
        D = pltpu.SemaphoreType.DMA
        scratch = [V(w_edge_up.shape, BF), V(w_mesh_up.shape, BF), V(w_grid_up.shape, BF), V((n_mesh, lat), BF), V((n_grid, lat), BF),
                   V((n_mesh, lat), BF), V((n_grid, lat), BF), V((n_feat, n_grid), F32),
                   V((n_grid, lat), BF), V((n_slot, lat), BF), V((n_slot, lat), BF), V((n_grid, lat), F32), V((n_mesh, lat), BF),
                   V((n_edge, lat), BF), V((n_edge, lat), BF), V((n_edge, lat), BF), V((n_edge, lat), BF), V((n_edge, lat), F32), V((n_edge, lat), F32), V((n_edge, 128), F32),
                   V((n_mesh, lat), BF), V((n_mesh, lat), F32), V((n_edge, lat), F32), V((n_edge, lat), BF), V((n_slot, lat), BF), V((n_slot, lat), BF),
                   V((1, n_slot), jnp.int32), V((1, n_edge), jnp.int32), V((1, n_edge), jnp.int32),
                   V((total, lat), F32), V((total, lat), F32), V((total // 2, lat), F32), V((total // 4, lat), F32), V((total // 8, lat), F32), V((3, total // 32, lat), F32),
                   D((5,)), D((12,)), D((parts,)), D((parts,)), D((parts,)), D((parts,)), D((5, 12)), D((5, 12))]
        res = pl.pallas_call(
            functools.partial(step_kernel, parts),
            out_shape=outs,
            in_specs=[near] * 11 + [far] * 5,
            out_specs=out_specs,
            scratch_shapes=scratch,
            compiler_params=pltpu.CompilerParams(vmem_limit_bytes=VMEM_LIMIT, collective_id=0, has_side_effects=True),
            name='step',
        )(grid_in.T, mesh_static.T, edge_static.T, send_rows, edge_src.reshape(-1, 128), edge_dst.reshape(-1, 128),
          w_grid_in, w_mesh_in, w_edge_in, w_second, vectors, w_edge_up, w_mesh_up, w_grid_up, d_mesh_out, d_grid_out)
        return (res[0], res[1], res[2].T) + tuple(res[3:])

    return jax.shard_map(local_step, mesh=mesh, in_specs=in_specs, out_specs=out_specs, check_vma=False)
```

```python
import functools

import jax
import jax.numpy as jnp
from jax import lax
from jax.experimental import pallas as pl
from jax.experimental.pallas import tpu as pltpu
from jax.sharding import PartitionSpec as P

LN_EPS = 1e-5
AXIS = 'gp'
BF = jnp.bfloat16
F32 = jnp.float32
MESH = pl.DeviceIdType.MESH
TILE = 1024
VMEM_LIMIT = 60 * 1024 * 1024


def nn(lhs, rhs):
    return jnp.dot(lhs, rhs, preferred_element_type=F32)


def tn(lhs, rhs):
    return lax.dot_general(lhs, rhs, (((0,), (0,)), ((), ())), preferred_element_type=F32)


def nt(lhs, rhs):
    return lax.dot_general(lhs, rhs, (((1,), (1,)), ((), ())), preferred_element_type=F32)


def mlp_fwd(pre_act, w_two, vec):
    act = pre_act + vec[0:1]
    sig = 0.5 * jnp.tanh(0.5 * act) + 0.5
    hidden = (act * sig).astype(BF)
    lin = nn(hidden, w_two) + vec[1:2]
    cen = lin - jnp.mean(lin, axis=-1, keepdims=True)
    inv = lax.rsqrt(jnp.mean(cen * cen, axis=-1, keepdims=True) + LN_EPS)
    normed = cen * inv
    return (act, sig, hidden, normed, inv), normed * vec[2:3] + vec[3:4]


def mlp_bwd(saved, w_two, vec, d_out):
    act, sig, hidden, normed, inv = saved
    d_n = d_out * vec[2:3]
    m_one = jnp.mean(d_n, axis=-1, keepdims=True)
    m_two = jnp.mean(d_n * normed, axis=-1, keepdims=True)
    d_lin = inv * (d_n - m_one - normed * m_two)
    d_lin_bf = d_lin.astype(BF)
    d_two = tn(hidden, d_lin_bf)
    d_hid = nt(d_lin_bf, w_two)
    d_pre = d_hid * (sig * (1.0 + act * (1.0 - sig)))
    d_vec = [jnp.sum(d_pre, axis=0, keepdims=True), jnp.sum(d_lin, axis=0, keepdims=True),
             jnp.sum(d_out * normed, axis=0, keepdims=True), jnp.sum(d_out, axis=0, keepdims=True)]
    return d_pre.astype(BF), d_two, d_vec


def add_vec(ref, base, d_vec):
    for j in range(4):
        ref[base + j:base + j + 1, :] += d_vec[j]


def rows_at(i, size):
    return pl.ds(pl.multiple_of(i * size, size), size)


def one_hot(ids, idx):
    return jnp.where(ids == idx, 1.0, 0.0).astype(BF)


def hot_cols(col_idx, width):
    return one_hot(lax.broadcasted_iota(jnp.int32, (col_idx.shape[0], width), 1), col_idx)


def hot_rows(row_idx, base, height):
    return one_hot(lax.broadcasted_iota(jnp.int32, (height, row_idx.shape[1]), 0) + base, row_idx)


def col_of(row_ref, starts):
    cols = []
    for start in starts:
        row = row_ref[0:1, pl.ds(pl.multiple_of(start, 128), 128)]
        cols.append(jnp.transpose(jnp.broadcast_to(row, (8, 128)))[:, 0:1])
    return jnp.concatenate(cols, axis=0)


def tile_starts(i, size):
    return [i * size + j * 128 for j in range(size // 128)]


def fill_row(idx_ref, row_ref):
    wide = idx_ref.shape[1]
    for j in range(idx_ref.shape[0]):
        row_ref[0:1, j * wide:(j + 1) * wide] = idx_ref[j:j + 1, :]


def loop(n, body, events=()):
    def step(i, carry):
        body(i)
        for when, fn in events:
            pl.when(i == when)(fn)
        return carry
    lax.fori_loop(0, n, step, 0)


class Reducer:
    def __init__(self, group, base, rows, place, refs):
        self.own, self.out, r_one, r_two, r_three, r_four, self.send_sem, self.recv_sem = refs
        self.group, self.place = group, place
        self.piece = rows // 32
        self.half, self.quarter, self.eighth = rows // 2, rows // 4, rows // 8
        self.r_one = r_one.at[pl.ds(base // 2, rows // 2)]
        self.r_two = r_two.at[pl.ds(base // 4, rows // 4)]
        self.r_three = r_three.at[pl.ds(base // 8, rows // 8)]
        self.r_four = [r_four.at[k, pl.ds(base // 32, rows // 32)] for k in range(3)]
        self.lo_one = base + place['core'] * self.half
        self.lo_two = self.lo_one + place['bit_one'] * self.quarter
        self.lo_three = self.lo_two + place['bit_two'] * self.eighth
        self.lo_four = self.lo_three + place['z'] * self.piece

    def at(self, start, size):
        return pl.ds(pl.multiple_of(start, 8), size)

    def copies(self, k):
        place, own, out = self.place, self.own, self.out

        def make(slot, src, dst, peer):
            return pltpu.make_async_remote_copy(src_ref=src, dst_ref=dst, send_sem=self.send_sem.at[self.group, slot],
                                                recv_sem=self.recv_sem.at[self.group, slot], device_id=(peer,), device_id_type=MESH)
        if k == 0:
            lo = self.lo_one + (1 - 2 * place['core']) * self.half
            return [make(0, own.at[self.at(lo, self.half)], self.r_one, place['swap_c'])]
        if k == 1:
            lo = self.lo_two + (1 - 2 * place['bit_one']) * self.quarter
            return [make(1, own.at[self.at(lo, self.quarter)], self.r_two, place['first'])]
        if k == 2:
            lo = self.lo_three + (1 - 2 * place['bit_two']) * self.eighth
            return [make(2, own.at[self.at(lo, self.eighth)], self.r_three, place['second'])]
        if k == 3:
            return [make(3 + j, own.at[self.at(self.lo_three + place['z_to'][j] * self.piece, self.piece)], self.r_four[j], place['z_dev'][j]) for j in range(3)]
        if k == 4:
            sl = self.at(self.lo_four, self.piece)
            return [make(6 + j, out.at[sl], out.at[sl], place['z_dev'][j]) for j in range(3)]
        sl = self.at(*((self.lo_three, self.eighth), (self.lo_two, self.quarter), (self.lo_one, self.half))[k - 5])
        return [make(4 + k, out.at[sl], out.at[sl], place[('second', 'first', 'swap_c')[k - 5]])]

    def start(self, k):
        for copy in self.copies(k):
            copy.start()

    def finish(self, k):
        for copy in self.copies(k):
            copy.wait()
        if k == 0:
            sl = self.at(self.lo_one, self.half)
            self.own[sl, :] += self.r_one[...]
        if k == 1:
            sl = self.at(self.lo_two, self.quarter)
            self.own[sl, :] += self.r_two[...]
        if k == 2:
            sl = self.at(self.lo_three, self.eighth)
            self.own[sl, :] += self.r_three[...]
        if k == 3:
            sl = self.at(self.lo_four, self.piece)
            self.out[sl, :] = self.own[sl, :] + (self.r_four[0][...] + self.r_four[1][...] + self.r_four[2][...])

    def step(self, k):
        def fn():
            if k > 0:
                self.finish(k - 1)
            if k < 8:
                self.start(k)
        return fn


def step_kernel(parts, grid_t, mesh_t, edge_t, send_idx, src_idx, dst_idx, w_grid_in, w_mesh_in, w_edge_in, w_two, vec,
                w_edge_up_h, w_mesh_up_h, w_grid_up_h, d_mesh_h, d_grid_h,
                mesh_out_h, grid_out_h, d_grid_t_h, d_wgi, d_wmi, d_wei, d_weu, d_wmu, d_wgu, d_two, d_vec_out,
                w_edge_up, w_mesh_up, w_grid_up, d_mesh, d_grid, mesh_out, grid_out, d_grid_t,
                grid_lat, outgoing, incoming, d_lat, mesh_lat, edge_lat, recv_lat, send_lat, edge_new, act_s, nrm_s, inv_s,
                d_pre4, d_mesh_lat, d_edge_lat, d_pre3, d_incoming, d_sent, send_row, src_row, dst_row,
                own, out, r_one, r_two, r_three, r_four,
                in_sem, out_sem, go_send, go_recv, back_send, back_recv, red_send, red_recv):
    lat = w_two.shape[1]
    n_feat, n_grid = grid_t.shape
    n_mesh, n_edge, n_slot = mesh_lat.shape[0], edge_lat.shape[0], outgoing.shape[0]
    cap = n_slot // parts
    pair = 2 * cap
    n_feat_pad = -(-n_feat // 8) * 8
    t_grid, t_mesh, t_edge = min(TILE, n_grid), min(TILE, n_mesh), min(TILE, n_edge)
    n_gt, n_nt, n_et = n_grid // t_grid, n_mesh // t_mesh, n_edge // t_edge
    me = lax.axis_index(AXIS)
    core = lax.rem(me, 2)
    x_at = lax.rem(me // 2, 2)
    y_at = lax.rem(me // 4, 2)
    z_at = me // 8
    plane = me - 8 * z_at
    swap_x = me + 2 * (1 - 2 * x_at)
    swap_y = me + 4 * (1 - 2 * y_at)
    z_to = [lax.rem(z_at + k, 4) for k in range(1, 4)]
    place = dict(core=core, z=z_at, swap_c=me + 1 - 2 * core,
                 first=(1 - core) * swap_x + core * swap_y, second=(1 - core) * swap_y + core * swap_x,
                 bit_one=(1 - core) * x_at + core * y_at, bit_two=(1 - core) * y_at + core * x_at,
                 z_to=z_to, z_dev=[plane + 8 * z for z in z_to])

    barrier = pltpu.get_barrier_semaphore()

    def knock(k, carry):
        pl.semaphore_signal(barrier, inc=1, device_id=(lax.rem(me + k, parts),), device_id_type=MESH)
        return carry
    lax.fori_loop(1, parts, knock, 0)

    loads = [pltpu.make_async_copy(a, b, in_sem.at[k]) for k, (a, b) in enumerate(
        [(d_grid_h, d_grid), (w_grid_up_h, w_grid_up), (w_edge_up_h, w_edge_up), (w_mesh_up_h, w_mesh_up), (d_mesh_h, d_mesh)])]
    for copy in loads:
        copy.start()

    r_wgu, r_two5, r_wmu, r_two4 = 0, lat, 2 * lat, 4 * lat
    r_weu, r_two3 = 5 * lat, 8 * lat
    r_two1, r_two2 = 9 * lat, 10 * lat
    r_two0, r_wgi = 11 * lat, 12 * lat
    r_wmi = r_wgi + n_feat_pad
    r_wei = r_wmi + 8
    r_vec = r_wei + 8
    refs = (own, out, r_one, r_two, r_three, r_four, red_send, red_recv)
    bounds = [0, 2 * lat, 5 * lat, 9 * lat, 11 * lat, 12 * lat, own.shape[0]]
    red = [Reducer(g, bounds[g], bounds[g + 1] - bounds[g], place, refs) for g in range(6)]

    own[...] = jnp.zeros_like(own)
    fill_row(send_idx, send_row)
    fill_row(src_idx, src_row)
    fill_row(dst_idx, dst_row)

    def embed(i):
        sl = rows_at(i, t_grid)
        _, emb = mlp_fwd(tn(grid_t[:, sl], w_grid_in[...]), w_two[0], vec[0])
        grid_lat[sl, :] = emb.astype(BF)
    loop(n_gt, embed)

    pl.semaphore_wait(barrier, parts - 1)

    def part_copy(src, dst, sends, recvs, to, frm):
        return pltpu.make_async_remote_copy(
            src_ref=src.at[pl.ds(pl.multiple_of(to * cap, 8), cap)], dst_ref=dst.at[pl.ds(pl.multiple_of(frm * cap, 8), cap)],
            send_sem=sends.at[to], recv_sem=recvs.at[frm], device_id=(to,), device_id_type=MESH)

    z_flip = z_at + 1 - 2 * lax.rem(z_at, 2)
    z_order = [lax.rem(z_at + 2, 4), z_flip, lax.rem(z_flip + 2, 4), z_at]
    planes = parts // 8

    def group_of(i):
        flip_x, flip_y = lax.rem(i + 1, 2), 1 - i // 2
        return x_at + flip_x * (1 - 2 * x_at) + 2 * (y_at + flip_y * (1 - 2 * y_at))

    def starts_of(group):
        return [z * 8 * cap + group * pair for z in range(planes)]

    def pair_at(start):
        return pl.ds(pl.multiple_of(start, 8), pair)

    def send_group(src, dst, sends, recvs, group):
        for z in z_order:
            for c in range(2):
                to = z * 8 + group * 2 + c

                @pl.when(to != me)
                def _():
                    part_copy(src, dst, sends, recvs, to, me).start()

                @pl.when(to == me)
                def _():
                    own_sl = pl.ds(pl.multiple_of(me * cap, 8), cap)
                    dst[own_sl, :] = src[own_sl, :]

    def wait_group(src, dst, sends, recvs, group):
        for z in range(planes):
            for c in range(2):
                other = z * 8 + group * 2 + c

                @pl.when(other != me)
                def _():
                    part_copy(src, dst, sends, recvs, other, me).wait_send()
                    part_copy(src, dst, sends, recvs, me, other).wait_recv()

    def put_group(ref, group, rows):
        for z, start in enumerate(starts_of(group)):
            ref[pair_at(start), :] = rows[z * pair:(z + 1) * pair]

    def get_group(ref, group):
        return jnp.concatenate([ref[pair_at(start), :] for start in starts_of(group)], axis=0)

    def spread(ids, group):
        return ids + (ids // pair) * (8 * cap - pair) + group * pair

    def pick(i):
        group = group_of(i)
        rows = nn(hot_cols(col_of(send_row, starts_of(group)), n_grid), grid_lat[...]).astype(BF)
        put_group(outgoing, group, rows)
        send_group(outgoing, incoming, go_send, go_recv, group)
    loop(4, pick)

    loads[0].wait()
    loads[1].wait()

    def cells(i):
        sl = rows_at(i, t_grid)
        here = grid_lat[sl, :]
        saved, upd = mlp_fwd(nn(here, w_grid_up[...]), w_two[5], vec[5])
        grid_out[sl, :] = (here.astype(F32) + upd).astype(BF)
        d_top = d_grid[sl, :].astype(F32)
        d_pre, d_two5, d_vec = mlp_bwd(saved, w_two[5], vec[5], d_top)
        own[r_wgu:r_wgu + lat, :] += tn(here, d_pre)
        own[r_two5:r_two5 + lat, :] += d_two5
        add_vec(own, r_vec + 20, d_vec)
        d_lat[sl, :] = d_top + nt(d_pre, w_grid_up[...])
    loop(n_gt, cells)
    stores = [pltpu.make_async_copy(a, b, out_sem.at[k]) for k, (a, b) in enumerate([(grid_out, grid_out_h), (mesh_out, mesh_out_h), (d_grid_t, d_grid_t_h)])]
    stores[0].start()
    red[0].start(0)
    loads[2].wait()
    loads[3].wait()
    loads[4].wait()

    def nodes_in(i):
        sl = rows_at(i, t_mesh)
        _, emb = mlp_fwd(tn(mesh_t[:, sl], w_mesh_in[...]), w_two[1], vec[1])
        here = emb.astype(BF)
        mesh_lat[sl, :] = here
        d_mesh_lat[sl, :] = nn(here, w_mesh_up[0:lat, :])
    loop(n_nt, nodes_in)

    def edges_in(i):
        sl = rows_at(i, t_edge)
        _, emb = mlp_fwd(tn(edge_t[:, sl], w_edge_in[...]), w_two[2], vec[2])
        here = emb.astype(BF)
        edge_lat[sl, :] = here
        recv = nn(hot_cols(col_of(dst_row, tile_starts(i, t_edge)), n_mesh), mesh_lat[...]).astype(BF)
        recv_lat[sl, :] = recv
        act_s[sl, :] = nn(here, w_edge_up[0:lat, :]) + nn(recv, w_edge_up[2 * lat:3 * lat, :])
    loop(n_et, edges_in)

    red[0].step(1)()

    def gather(i):
        group = group_of(i // n_et)
        tile = lax.rem(i, n_et)
        sl = rows_at(tile, t_edge)

        @pl.when(tile == 0)
        def _():
            wait_group(outgoing, incoming, go_send, go_recv, group)
        ids = spread(lax.broadcasted_iota(jnp.int32, (t_edge, 4 * pair), 1), group)
        rows = nn(one_hot(ids, col_of(src_row, tile_starts(tile, t_edge))), get_group(incoming, group))

        @pl.when(i < n_et)
        def _():
            nrm_s[sl, :] = rows

        @pl.when(i >= n_et)
        def _():
            nrm_s[sl, :] += rows
    loop(4 * n_et, gather, [(n_et - 1, red[0].step(2)), (2 * n_et - 1, red[0].step(3))])

    def edges_fwd(i):
        sl = rows_at(i, t_edge)
        sent = nrm_s[sl, :].astype(BF)
        send_lat[sl, :] = sent
        (act, _, _, normed, inv), upd = mlp_fwd(act_s[sl, :] + nn(sent, w_edge_up[lat:2 * lat, :]), w_two[3], vec[3])
        act_s[sl, :] = act
        nrm_s[sl, :] = normed
        inv_s[sl, :] = jnp.broadcast_to(inv, (t_edge, 128))
        edge_new[sl, :] = (edge_lat[sl, :].astype(F32) + upd).astype(BF)
    loop(n_et, edges_fwd, [(0, red[0].step(4)), (n_et - 1, red[0].step(5))])

    def nodes(i):
        sl = rows_at(i, t_mesh)
        agg = nn(hot_rows(dst_row[...], i * t_mesh, t_mesh), edge_new[...]).astype(BF)
        here = mesh_lat[sl, :]
        saved, upd = mlp_fwd(d_mesh_lat[sl, :] + nn(agg, w_mesh_up[lat:2 * lat, :]), w_two[4], vec[4])
        mesh_out[sl, :] = (here.astype(F32) + upd).astype(BF)
        d_top = d_mesh[sl, :].astype(F32)
        d_pre, d_two4, d_vec = mlp_bwd(saved, w_two[4], vec[4], d_top)
        d_pre4[sl, :] = d_pre
        own[r_wmu:r_wmu + lat, :] += tn(here, d_pre)
        own[r_wmu + lat:r_wmu + 2 * lat, :] += tn(agg, d_pre)
        own[r_two4:r_two4 + lat, :] += d_two4
        add_vec(own, r_vec + 16, d_vec)
        d_mesh_lat[sl, :] = d_top + nt(d_pre, w_mesh_up[0:lat, :])
    loop(n_nt, nodes, [(0, red[0].step(6)), (n_nt - 1, red[0].step(7))])
    stores[1].start()
    red[1].start(0)

    def edges_bwd(i):
        sl = rows_at(i, t_edge)
        picked = nn(hot_cols(col_of(dst_row, tile_starts(i, t_edge)), n_mesh), d_pre4[...]).astype(BF)
        d_new = nt(picked, w_mesh_up[lat:2 * lat, :])
        act = act_s[sl, :]
        sig = 0.5 * jnp.tanh(0.5 * act) + 0.5
        hidden = (act * sig).astype(BF)
        d_pre, d_two3, d_vec = mlp_bwd((act, sig, hidden, nrm_s[sl, :], inv_s[sl, 0:1]), w_two[3], vec[3], d_new)
        d_pre3[sl, :] = d_pre
        own[r_two3:r_two3 + lat, :] += d_two3
        add_vec(own, r_vec + 12, d_vec)
        d_edge_lat[sl, :] = d_new
    loop(n_et, edges_bwd, [(0, red[0].step(8)), (0, red[1].step(1)), (n_et // 2, red[1].step(2)), (n_et - 1, red[1].step(3))])

    def slots(i):
        group = group_of(i)
        ids = spread(lax.broadcasted_iota(jnp.int32, (4 * pair, n_edge), 0), group)
        d_slot = nn(one_hot(ids, src_row[...]), d_pre3[...]).astype(BF)
        put_group(d_incoming, group, nt(d_slot, w_edge_up[lat:2 * lat, :]).astype(BF))
        send_group(d_incoming, d_sent, back_send, back_recv, group)
    loop(4, slots)

    def edges_grad(i):
        sl = rows_at(i, t_edge)
        d_pre = d_pre3[sl, :]
        own[r_weu:r_weu + lat, :] += tn(edge_lat[sl, :], d_pre)
        own[r_weu + lat:r_weu + 2 * lat, :] += tn(send_lat[sl, :], d_pre)
        own[r_weu + 2 * lat:r_weu + 3 * lat, :] += tn(recv_lat[sl, :], d_pre)
        d_edge_lat[sl, :] += nt(d_pre, w_edge_up[0:lat, :])
    loop(n_et, edges_grad)
    red[2].start(0)

    def nodes_bwd(i):
        sl = rows_at(i, t_mesh)
        d_node = nn(hot_rows(dst_row[...], i * t_mesh, t_mesh), d_pre3[...]).astype(BF)
        d_top = d_mesh_lat[sl, :] + nt(d_node, w_edge_up[2 * lat:3 * lat, :])
        feat = mesh_t[:, sl]
        saved, _ = mlp_fwd(tn(feat, w_mesh_in[...]), w_two[1], vec[1])
        d_pre, d_two1, d_vec = mlp_bwd(saved, w_two[1], vec[1], d_top)
        own[r_two1:r_two1 + lat, :] += d_two1
        own[r_wmi:r_wmi + 3, :] += nn(feat, d_pre)
        add_vec(own, r_vec + 4, d_vec)
    loop(n_nt, nodes_bwd, [(0, red[1].step(4)), (0, red[2].step(1)), (n_nt - 1, red[1].step(5)), (n_nt - 1, red[2].step(2))])

    def edges_in_bwd(i):
        sl = rows_at(i, t_edge)
        feat = edge_t[:, sl]
        saved, _ = mlp_fwd(tn(feat, w_edge_in[...]), w_two[2], vec[2])
        d_pre, d_two2, d_vec = mlp_bwd(saved, w_two[2], vec[2], d_edge_lat[sl, :])
        own[r_two2:r_two2 + lat, :] += d_two2
        own[r_wei:r_wei + 4, :] += nn(feat, d_pre)
        add_vec(own, r_vec + 8, d_vec)
    loop(n_et, edges_in_bwd, [(n_et - 1, red[1].step(6))])

    red[3].start(0)

    def scatter(i):
        group = group_of(i // n_gt)
        tile = lax.rem(i, n_gt)
        sl = rows_at(tile, t_grid)

        @pl.when(tile == 0)
        def _():
            wait_group(d_incoming, d_sent, back_send, back_recv, group)
        picks = jnp.concatenate([send_row[0:1, pl.ds(pl.multiple_of(start, 128), pair)] for start in starts_of(group)], axis=1)
        d_lat[sl, :] += nn(hot_rows(picks, tile * t_grid, t_grid), get_group(d_sent, group))
    loop(4 * n_gt, scatter, [(n_gt - 1, red[3].step(1)), (2 * n_gt - 1, red[1].step(7)), (3 * n_gt - 1, red[2].step(3))])
    red[1].step(8)()
    red[3].step(2)()

    def grid_bwd(i):
        sl = rows_at(i, t_grid)
        d_top = d_lat[sl, :]
        feat = grid_t[:, sl]
        saved, _ = mlp_fwd(tn(feat, w_grid_in[...]), w_two[0], vec[0])
        d_pre, d_two0, d_vec = mlp_bwd(saved, w_two[0], vec[0], d_top)
        own[r_two0:r_two0 + lat, :] += d_two0
        own[r_wgi:r_wgi + n_feat, :] += nn(feat, d_pre)
        add_vec(own, r_vec, d_vec)
        d_grid_t[:, sl] = nt(w_grid_in[...], d_pre)
    loop(n_gt, grid_bwd, [(0, red[2].step(4)), (0, red[3].step(3)), (n_gt - 1, red[2].step(5)), (n_gt - 1, red[3].step(4))])

    red[4].start(0)
    red[5].start(0)
    stores[2].start()
    for g, k in ((4, 1), (5, 1), (2, 6), (3, 5), (4, 2), (5, 2), (2, 7), (3, 6), (4, 3), (5, 3), (2, 8), (3, 7), (4, 4), (5, 4), (3, 8)):
        red[g].step(k)()
    puts = [(r_weu, 3 * lat, d_weu), (r_wmu, 2 * lat, d_wmu), (r_wgu, lat, d_wgu), (r_two1, lat, d_two.at[1]),
            (r_two2, lat, d_two.at[2]), (r_two3, lat, d_two.at[3]), (r_two4, lat, d_two.at[4]), (r_two5, lat, d_two.at[5])]
    moves = [pltpu.make_async_copy(out.at[pl.ds(a, n)], ref, out_sem.at[3 + k]) for k, (a, n, ref) in enumerate(puts)]
    for move in moves:
        move.start()
    for k in range(5, 9):
        red[4].step(k)()
        red[5].step(k)()
    last = pltpu.make_async_copy(out.at[pl.ds(r_two0, lat)], d_two.at[0], out_sem.at[11])
    last.start()
    d_wgi[...] = out[r_wgi:r_wgi + n_feat, :]
    d_wmi[...] = out[r_wmi:r_wmi + 3, :]
    d_wei[...] = out[r_wei:r_wei + 4, :]
    for k in range(6):
        d_vec_out[k] = out[r_vec + 4 * k:r_vec + 4 * k + 4, :]
    for copy in stores + moves + [last]:
        copy.wait()


def finish_kernel(*refs):
    n = (len(refs) - 2) // 3
    srcs, dsts, held, (in_sem, out_sem) = refs[:n], refs[n:2 * n], refs[2 * n:3 * n], refs[3 * n:]
    takes = [pltpu.make_async_copy(srcs[k], held[k], in_sem.at[k]) for k in range(n)]
    gives = [pltpu.make_async_copy(held[k], dsts[k], out_sem.at[k]) for k in range(n)]
    for copy in takes:
        copy.start()
    for take, give in zip(takes, gives):
        take.wait()
        give.start()
    for copy in gives:
        copy.wait()


def solution(mesh):
    parts = mesh.shape[AXIS]
    row_spec = P(AXIS, None)
    edge_spec = P(AXIS)
    rep_spec = P()
    in_specs = (row_spec, row_spec, row_spec, row_spec, edge_spec, edge_spec) + (rep_spec,) * 8 + (row_spec, row_spec)
    out_specs = (row_spec, row_spec, row_spec) + (rep_spec,) * 8

    def local_step(grid_in, mesh_static, edge_static, send_rows, edge_src, edge_dst, w_grid_in, w_mesh_in, w_edge_in, w_edge_up, w_mesh_up, w_grid_up, w_second, vectors, d_mesh_out, d_grid_out):
        lat = w_grid_up.shape[0]
        n_grid, n_feat = grid_in.shape
        n_mesh = mesh_static.shape[0]
        n_edge = edge_static.shape[0]
        n_slot = send_rows.size
        small = -(-n_feat // 8) * 8 + 8 + 8 + 24
        total = 11 * lat + -(-(lat + small) // 256) * 256
        near = pl.BlockSpec(memory_space=pltpu.VMEM)
        far = pl.BlockSpec(memory_space=pl.ANY)

        def sds(shape, dtype):
            return jax.ShapeDtypeStruct(shape, dtype)
        outs = [sds((n_mesh, lat), BF), sds((n_grid, lat), BF), sds((n_feat, n_grid), F32), sds(w_grid_in.shape, F32), sds(w_mesh_in.shape, F32), sds(w_edge_in.shape, F32),
                sds(w_edge_up.shape, F32), sds(w_mesh_up.shape, F32), sds(w_grid_up.shape, F32), sds(w_second.shape, F32), sds(vectors.shape, F32)]
        out_specs = [far, far, far, near, near, near, far, far, far, far, near]
        V = pltpu.VMEM
        D = pltpu.SemaphoreType.DMA
        scratch = [V(w_edge_up.shape, BF), V(w_mesh_up.shape, BF), V(w_grid_up.shape, BF), V((n_mesh, lat), BF), V((n_grid, lat), BF),
                   V((n_mesh, lat), BF), V((n_grid, lat), BF), V((n_feat, n_grid), F32),
                   V((n_grid, lat), BF), V((n_slot, lat), BF), V((n_slot, lat), BF), V((n_grid, lat), F32), V((n_mesh, lat), BF),
                   V((n_edge, lat), BF), V((n_edge, lat), BF), V((n_edge, lat), BF), V((n_edge, lat), BF), V((n_edge, lat), F32), V((n_edge, lat), F32), V((n_edge, 128), F32),
                   V((n_mesh, lat), BF), V((n_mesh, lat), F32), V((n_edge, lat), F32), V((n_edge, lat), BF), V((n_slot, lat), BF), V((n_slot, lat), BF),
                   V((1, n_slot), jnp.int32), V((1, n_edge), jnp.int32), V((1, n_edge), jnp.int32),
                   V((total, lat), F32), V((total, lat), F32), V((total // 2, lat), F32), V((total // 4, lat), F32), V((total // 8, lat), F32), V((3, total // 32, lat), F32),
                   D((5,)), D((12,)), D((parts,)), D((parts,)), D((parts,)), D((parts,)), D((6, 12)), D((6, 12))]
        res = pl.pallas_call(
            functools.partial(step_kernel, parts),
            out_shape=outs,
            in_specs=[near] * 11 + [far] * 5,
            out_specs=out_specs,
            scratch_shapes=scratch,
            compiler_params=pltpu.CompilerParams(vmem_limit_bytes=VMEM_LIMIT, collective_id=0, has_side_effects=True),
            name='step',
        )(grid_in.T, mesh_static.T, edge_static.T, send_rows, edge_src.reshape(-1, 128), edge_dst.reshape(-1, 128),
          w_grid_in, w_mesh_in, w_edge_in, w_second, vectors, w_edge_up, w_mesh_up, w_grid_up, d_mesh_out, d_grid_out)
        res = pl.pallas_call(
            finish_kernel,
            out_shape=outs,
            in_specs=[far] * len(outs),
            out_specs=[far] * len(outs),
            scratch_shapes=[V(o.shape, o.dtype) for o in outs] + [D((len(outs),)), D((len(outs),))],
            compiler_params=pltpu.CompilerParams(vmem_limit_bytes=VMEM_LIMIT),
            name='finish',
        )(*res)
        return (res[0], res[1], res[2].T) + tuple(res[3:])

    return jax.shard_map(local_step, mesh=mesh, in_specs=in_specs, out_specs=out_specs, check_vma=False)
```

```python
import functools

import jax
import jax.numpy as jnp
from jax import lax
from jax.experimental import pallas as pl
from jax.experimental.pallas import tpu as pltpu
from jax.sharding import PartitionSpec as P

LN_EPS = 1e-5
AXIS = 'gp'
BF = jnp.bfloat16
F32 = jnp.float32
MESH = pl.DeviceIdType.MESH
TILE = 1024
VMEM_LIMIT = 60 * 1024 * 1024


def nn(lhs, rhs):
    return jnp.dot(lhs, rhs, preferred_element_type=F32)


def tn(lhs, rhs):
    return lax.dot_general(lhs, rhs, (((0,), (0,)), ((), ())), preferred_element_type=F32)


def nt(lhs, rhs):
    return lax.dot_general(lhs, rhs, (((1,), (1,)), ((), ())), preferred_element_type=F32)


def mlp_fwd(pre_act, w_two, vec):
    act = pre_act + vec[0:1]
    sig = 0.5 * jnp.tanh(0.5 * act) + 0.5
    hidden = (act * sig).astype(BF)
    lin = nn(hidden, w_two) + vec[1:2]
    cen = lin - jnp.mean(lin, axis=-1, keepdims=True)
    inv = lax.rsqrt(jnp.mean(cen * cen, axis=-1, keepdims=True) + LN_EPS)
    normed = cen * inv
    return (act, sig, hidden, normed, inv), normed * vec[2:3] + vec[3:4]


def mlp_bwd(saved, w_two, vec, d_out):
    act, sig, hidden, normed, inv = saved
    d_n = d_out * vec[2:3]
    m_one = jnp.mean(d_n, axis=-1, keepdims=True)
    m_two = jnp.mean(d_n * normed, axis=-1, keepdims=True)
    d_lin = inv * (d_n - m_one - normed * m_two)
    d_lin_bf = d_lin.astype(BF)
    d_two = tn(hidden, d_lin_bf)
    d_hid = nt(d_lin_bf, w_two)
    d_pre = d_hid * (sig * (1.0 + act * (1.0 - sig)))
    d_vec = [jnp.sum(d_pre, axis=0, keepdims=True), jnp.sum(d_lin, axis=0, keepdims=True),
             jnp.sum(d_out * normed, axis=0, keepdims=True), jnp.sum(d_out, axis=0, keepdims=True)]
    return d_pre.astype(BF), d_two, d_vec


def add_vec(ref, base, d_vec):
    for j in range(4):
        ref[base + j:base + j + 1, :] += d_vec[j]


def rows_at(i, size):
    return pl.ds(pl.multiple_of(i * size, size), size)


def one_hot(ids, idx):
    return jnp.where(ids == idx, 1.0, 0.0).astype(BF)


def hot_cols(col_idx, width):
    return one_hot(lax.broadcasted_iota(jnp.int32, (col_idx.shape[0], width), 1), col_idx)


def hot_rows(row_idx, base, height):
    return one_hot(lax.broadcasted_iota(jnp.int32, (height, row_idx.shape[1]), 0) + base, row_idx)


def col_of(row_ref, starts):
    cols = []
    for start in starts:
        row = row_ref[0:1, pl.ds(pl.multiple_of(start, 128), 128)]
        cols.append(jnp.transpose(jnp.broadcast_to(row, (8, 128)))[:, 0:1])
    return jnp.concatenate(cols, axis=0)


def tile_starts(i, size):
    return [i * size + j * 128 for j in range(size // 128)]


def fill_row(idx_ref, row_ref):
    wide = idx_ref.shape[1]
    for j in range(idx_ref.shape[0]):
        row_ref[0:1, j * wide:(j + 1) * wide] = idx_ref[j:j + 1, :]


def loop(n, body, events=()):
    def step(i, carry):
        body(i)
        for when, fn in events:
            pl.when(i == when)(fn)
        return carry
    lax.fori_loop(0, n, step, 0)


class Reducer:
    def __init__(self, group, base, rows, place, refs):
        self.own, self.out, r_one, r_two, r_three, r_four, self.send_sem, self.recv_sem = refs
        self.group, self.place = group, place
        self.piece = rows // 32
        self.half, self.quarter, self.eighth = rows // 2, rows // 4, rows // 8
        self.r_one = r_one.at[pl.ds(base // 2, rows // 2)]
        self.r_two = r_two.at[pl.ds(base // 4, rows // 4)]
        self.r_three = r_three.at[pl.ds(base // 8, rows // 8)]
        self.r_four = [r_four.at[k, pl.ds(base // 32, rows // 32)] for k in range(3)]
        self.lo_one = base + place['core'] * self.half
        self.lo_two = self.lo_one + place['bit_one'] * self.quarter
        self.lo_three = self.lo_two + place['bit_two'] * self.eighth
        self.lo_four = self.lo_three + place['z'] * self.piece

    def at(self, start, size):
        return pl.ds(pl.multiple_of(start, 8), size)

    def copies(self, k):
        place, own, out = self.place, self.own, self.out

        def make(slot, src, dst, peer):
            return pltpu.make_async_remote_copy(src_ref=src, dst_ref=dst, send_sem=self.send_sem.at[self.group, slot],
                                                recv_sem=self.recv_sem.at[self.group, slot], device_id=(peer,), device_id_type=MESH)
        if k == 0:
            lo = self.lo_one + (1 - 2 * place['core']) * self.half
            return [make(0, own.at[self.at(lo, self.half)], self.r_one, place['swap_c'])]
        if k == 1:
            lo = self.lo_two + (1 - 2 * place['bit_one']) * self.quarter
            return [make(1, own.at[self.at(lo, self.quarter)], self.r_two, place['first'])]
        if k == 2:
            lo = self.lo_three + (1 - 2 * place['bit_two']) * self.eighth
            return [make(2, own.at[self.at(lo, self.eighth)], self.r_three, place['second'])]
        if k == 3:
            return [make(3 + j, own.at[self.at(self.lo_three + place['z_to'][j] * self.piece, self.piece)], self.r_four[j], place['z_dev'][j]) for j in range(3)]
        if k == 4:
            sl = self.at(self.lo_four, self.piece)
            return [make(6 + j, out.at[sl], out.at[sl], place['z_dev'][j]) for j in range(3)]
        sl = self.at(*((self.lo_three, self.eighth), (self.lo_two, self.quarter), (self.lo_one, self.half))[k - 5])
        return [make(4 + k, out.at[sl], out.at[sl], place[('second', 'first', 'swap_c')[k - 5]])]

    def start(self, k):
        for copy in self.copies(k):
            copy.start()

    def finish(self, k):
        for copy in self.copies(k):
            copy.wait()
        if k == 0:
            sl = self.at(self.lo_one, self.half)
            self.own[sl, :] += self.r_one[...]
        if k == 1:
            sl = self.at(self.lo_two, self.quarter)
            self.own[sl, :] += self.r_two[...]
        if k == 2:
            sl = self.at(self.lo_three, self.eighth)
            self.own[sl, :] += self.r_three[...]
        if k == 3:
            sl = self.at(self.lo_four, self.piece)
            self.out[sl, :] = self.own[sl, :] + (self.r_four[0][...] + self.r_four[1][...] + self.r_four[2][...])

    def step(self, k):
        def fn():
            if k > 0:
                self.finish(k - 1)
            if k < 8:
                self.start(k)
        return fn


def step_kernel(parts, grid_t, mesh_t, edge_t, send_idx, src_idx, dst_idx, w_grid_in, w_mesh_in, w_edge_in, w_two, vec,
                w_edge_up_h, w_mesh_up_h, w_grid_up_h, d_mesh_h, d_grid_h,
                mesh_out_h, grid_out_h, d_grid_t_h, d_wgi, d_wmi, d_wei, d_weu, d_wmu, d_wgu, d_two, d_vec_out,
                w_edge_up, w_mesh_up, w_grid_up, d_mesh, d_grid, mesh_out, grid_out, d_grid_t,
                grid_lat, outgoing, incoming, d_lat, mesh_lat, edge_lat, recv_lat, send_lat, edge_new, act_s, nrm_s, inv_s,
                d_pre4, d_mesh_lat, d_edge_lat, d_pre3, d_incoming, d_sent, send_row, src_row, dst_row,
                own, out, r_one, r_two, r_three, r_four,
                in_sem, out_sem, go_send, go_recv, back_send, back_recv, red_send, red_recv,
                held_go, held_back, zg_send, zg_recv, zb_send, zb_recv):
    lat = w_two.shape[1]
    n_feat, n_grid = grid_t.shape
    n_mesh, n_edge, n_slot = mesh_lat.shape[0], edge_lat.shape[0], outgoing.shape[0]
    cap = n_slot // parts
    block = n_slot // 4
    n_feat_pad = -(-n_feat // 8) * 8
    t_grid, t_mesh, t_edge = min(TILE, n_grid), min(TILE, n_mesh), min(TILE, n_edge)
    n_gt, n_nt, n_et = n_grid // t_grid, n_mesh // t_mesh, n_edge // t_edge
    me = lax.axis_index(AXIS)
    core = lax.rem(me, 2)
    x_at = lax.rem(me // 2, 2)
    y_at = lax.rem(me // 4, 2)
    z_at = me // 8
    plane = me - 8 * z_at
    swap_x = me + 2 * (1 - 2 * x_at)
    swap_y = me + 4 * (1 - 2 * y_at)
    z_to = [lax.rem(z_at + k, 4) for k in range(1, 4)]
    place = dict(core=core, z=z_at, swap_c=me + 1 - 2 * core,
                 first=(1 - core) * swap_x + core * swap_y, second=(1 - core) * swap_y + core * swap_x,
                 bit_one=(1 - core) * x_at + core * y_at, bit_two=(1 - core) * y_at + core * x_at,
                 z_to=z_to, z_dev=[plane + 8 * z for z in z_to])

    barrier = pltpu.get_barrier_semaphore()

    def knock(k, carry):
        pl.semaphore_signal(barrier, inc=1, device_id=(lax.rem(me + k, parts),), device_id_type=MESH)
        return carry
    lax.fori_loop(1, parts, knock, 0)

    loads = [pltpu.make_async_copy(a, b, in_sem.at[k]) for k, (a, b) in enumerate(
        [(d_grid_h, d_grid), (w_grid_up_h, w_grid_up), (w_edge_up_h, w_edge_up), (w_mesh_up_h, w_mesh_up), (d_mesh_h, d_mesh)])]
    for copy in loads:
        copy.start()

    r_wgu, r_two5, r_wmu, r_two4 = 0, lat, 2 * lat, 4 * lat
    r_weu, r_two3 = 5 * lat, 8 * lat
    r_two1, r_two2 = 9 * lat, 10 * lat
    r_two0, r_wgi = 11 * lat, 12 * lat
    r_wmi = r_wgi + n_feat_pad
    r_wei = r_wmi + 8
    r_vec = r_wei + 8
    refs = (own, out, r_one, r_two, r_three, r_four, red_send, red_recv)
    bounds = [0, 2 * lat, 5 * lat, 9 * lat, 11 * lat, 12 * lat, own.shape[0]]
    red = [Reducer(g, bounds[g], bounds[g + 1] - bounds[g], place, refs) for g in range(6)]

    own[...] = jnp.zeros_like(own)
    fill_row(send_idx, send_row)
    fill_row(src_idx, src_row)
    fill_row(dst_idx, dst_row)

    def embed(i):
        sl = rows_at(i, t_grid)
        _, emb = mlp_fwd(tn(grid_t[:, sl], w_grid_in[...]), w_two[0], vec[0])
        grid_lat[sl, :] = emb.astype(BF)
    loop(n_gt, embed)

    pl.semaphore_wait(barrier, parts - 1)

    spot = me - 8 * z_at
    near = z_at + 1 - 2 * lax.rem(z_at, 2)
    inner = lax.rem(lax.rem(z_at, 2) + z_at // 2, 2)
    mid = inner * (3 - z_at) + (1 - inner) * lax.rem(z_at + 2, 4)
    far = 6 - z_at - near - mid

    def plane_turn(k):
        return lax.rem(z_at + 4 + (1 - 2 * (z_at // 2)) * (1 + k), 4)

    def block_at(z):
        return pl.ds(pl.multiple_of(z * block, block), block)

    def cap_at(k):
        return pl.ds(pl.multiple_of(k * cap, cap), cap)

    class Exchange:
        def __init__(self, src, held, dst, sems):
            self.src, self.held, self.dst = src, held, dst
            self.z_send, self.z_recv, self.p_send, self.p_recv = sems

        def plane_copy(self, to, frm):
            return pltpu.make_async_remote_copy(src_ref=self.src.at[block_at(to)], dst_ref=self.held.at[block_at(frm)],
                                                send_sem=self.z_send.at[to], recv_sem=self.z_recv.at[frm], device_id=(spot + 8 * to,), device_id_type=MESH)

        def list_copy(self, src, z, j_to, j_from):
            return pltpu.make_async_remote_copy(src_ref=src.at[cap_at(z * 8 + j_to)], dst_ref=self.dst.at[cap_at(z * 8 + j_from)],
                                                send_sem=self.p_send.at[z * 8 + j_to], recv_sem=self.p_recv.at[z * 8 + j_from], device_id=(z_at * 8 + j_to,), device_id_type=MESH)

        def send_lists(self, src, z):
            for k in range(1, 8):
                self.list_copy(src, z, lax.rem(spot + k, 8), spot).start()
            self.dst[cap_at(z * 8 + spot), :] = src[cap_at(z * 8 + spot), :]

        def send_plane(self, z):
            @pl.when(z != z_at)
            def _():
                self.plane_copy(z, z_at).start()

            @pl.when(z == z_at)
            def _():
                self.send_lists(self.src, z_at)

        def relay(self, z):
            def fn():
                self.plane_copy(z_at, z).wait_recv()
                self.send_lists(self.held, z)
            return fn

        def wait_lists(self, z):
            for k in range(1, 8):
                j = lax.rem(spot + k, 8)
                self.list_copy(self.held, z, j, spot).wait_send()
                self.list_copy(self.held, z, spot, j).wait_recv()

        def wait_planes(self):
            for z in (near, mid, far):
                self.plane_copy(z, z_at).wait_send()

    go = Exchange(outgoing, held_go, incoming, (zg_send, zg_recv, go_send, go_recv))
    back = Exchange(d_incoming, held_back, d_sent, (zb_send, zb_recv, back_send, back_recv))

    def pick(i):
        z = plane_turn(i)
        outgoing[block_at(z), :] = nn(hot_cols(col_of(send_row, tile_starts(z, block)), n_grid), grid_lat[...]).astype(BF)
        go.send_plane(z)
    loop(4, pick)

    loads[0].wait()
    loads[1].wait()

    def cells(i):
        sl = rows_at(i, t_grid)
        here = grid_lat[sl, :]
        saved, upd = mlp_fwd(nn(here, w_grid_up[...]), w_two[5], vec[5])
        grid_out[sl, :] = (here.astype(F32) + upd).astype(BF)
        d_top = d_grid[sl, :].astype(F32)
        d_pre, d_two5, d_vec = mlp_bwd(saved, w_two[5], vec[5], d_top)
        own[r_wgu:r_wgu + lat, :] += tn(here, d_pre)
        own[r_two5:r_two5 + lat, :] += d_two5
        add_vec(own, r_vec + 20, d_vec)
        d_lat[sl, :] = d_top + nt(d_pre, w_grid_up[...])
    loop(n_gt, cells, [(n_gt - 1, go.relay(near))])
    stores = [pltpu.make_async_copy(a, b, out_sem.at[k]) for k, (a, b) in enumerate([(grid_out, grid_out_h), (mesh_out, mesh_out_h), (d_grid_t, d_grid_t_h)])]
    stores[0].start()
    loads[2].wait()
    loads[3].wait()
    loads[4].wait()

    def nodes_in(i):
        sl = rows_at(i, t_mesh)
        _, emb = mlp_fwd(tn(mesh_t[:, sl], w_mesh_in[...]), w_two[1], vec[1])
        here = emb.astype(BF)
        mesh_lat[sl, :] = here
        d_mesh_lat[sl, :] = nn(here, w_mesh_up[0:lat, :])
    loop(n_nt, nodes_in)

    def edges_in(i):
        sl = rows_at(i, t_edge)
        _, emb = mlp_fwd(tn(edge_t[:, sl], w_edge_in[...]), w_two[2], vec[2])
        here = emb.astype(BF)
        edge_lat[sl, :] = here
        recv = nn(hot_cols(col_of(dst_row, tile_starts(i, t_edge)), n_mesh), mesh_lat[...]).astype(BF)
        recv_lat[sl, :] = recv
        act_s[sl, :] = nn(here, w_edge_up[0:lat, :]) + nn(recv, w_edge_up[2 * lat:3 * lat, :])
    loop(n_et, edges_in, [(n_et - 1, go.relay(mid))])


    def gather(z, first):
        go.wait_lists(z)

        def fn(i):
            sl = rows_at(i, t_edge)
            ids = lax.broadcasted_iota(jnp.int32, (t_edge, block), 1) + z * block
            rows = nn(one_hot(ids, col_of(src_row, tile_starts(i, t_edge))), incoming[block_at(z), :])
            nrm_s[sl, :] = rows if first else nrm_s[sl, :] + rows
        loop(n_et, fn)
    gather(z_at, True)
    gather(near, False)
    go.relay(far)()
    gather(mid, False)
    gather(far, False)
    go.wait_planes()
    red[0].start(0)

    def edges_fwd(i):
        sl = rows_at(i, t_edge)
        sent = nrm_s[sl, :].astype(BF)
        send_lat[sl, :] = sent
        (act, _, _, normed, inv), upd = mlp_fwd(act_s[sl, :] + nn(sent, w_edge_up[lat:2 * lat, :]), w_two[3], vec[3])
        act_s[sl, :] = act
        nrm_s[sl, :] = normed
        inv_s[sl, :] = jnp.broadcast_to(inv, (t_edge, 128))
        edge_new[sl, :] = (edge_lat[sl, :].astype(F32) + upd).astype(BF)
    loop(n_et, edges_fwd, [(n_et // 2, red[0].step(1))])

    def nodes(i):
        sl = rows_at(i, t_mesh)
        agg = nn(hot_rows(dst_row[...], i * t_mesh, t_mesh), edge_new[...]).astype(BF)
        here = mesh_lat[sl, :]
        saved, upd = mlp_fwd(d_mesh_lat[sl, :] + nn(agg, w_mesh_up[lat:2 * lat, :]), w_two[4], vec[4])
        mesh_out[sl, :] = (here.astype(F32) + upd).astype(BF)
        d_top = d_mesh[sl, :].astype(F32)
        d_pre, d_two4, d_vec = mlp_bwd(saved, w_two[4], vec[4], d_top)
        d_pre4[sl, :] = d_pre
        own[r_wmu:r_wmu + lat, :] += tn(here, d_pre)
        own[r_wmu + lat:r_wmu + 2 * lat, :] += tn(agg, d_pre)
        own[r_two4:r_two4 + lat, :] += d_two4
        add_vec(own, r_vec + 16, d_vec)
        d_mesh_lat[sl, :] = d_top + nt(d_pre, w_mesh_up[0:lat, :])
    loop(n_nt, nodes, [(0, red[0].step(2)), (n_nt - 1, red[0].step(3))])
    stores[1].start()
    red[1].start(0)

    def edges_bwd(i):
        sl = rows_at(i, t_edge)
        picked = nn(hot_cols(col_of(dst_row, tile_starts(i, t_edge)), n_mesh), d_pre4[...]).astype(BF)
        d_new = nt(picked, w_mesh_up[lat:2 * lat, :])
        act = act_s[sl, :]
        sig = 0.5 * jnp.tanh(0.5 * act) + 0.5
        hidden = (act * sig).astype(BF)
        d_pre, d_two3, d_vec = mlp_bwd((act, sig, hidden, nrm_s[sl, :], inv_s[sl, 0:1]), w_two[3], vec[3], d_new)
        d_pre3[sl, :] = d_pre
        own[r_two3:r_two3 + lat, :] += d_two3
        add_vec(own, r_vec + 12, d_vec)
        d_edge_lat[sl, :] = d_new
    loop(n_et, edges_bwd, [(0, red[1].step(1)), (0, red[0].step(4)), (n_et // 2, red[1].step(2)), (n_et // 2, red[0].step(5)), (n_et - 1, red[1].step(3)), (n_et - 1, red[0].step(6))])

    def slots(i):
        z = plane_turn(i)
        d_slot = nn(hot_rows(src_row[...], z * block, block), d_pre3[...]).astype(BF)
        d_incoming[block_at(z), :] = nt(d_slot, w_edge_up[lat:2 * lat, :]).astype(BF)
        back.send_plane(z)
    loop(4, slots)
    red[0].step(7)()

    def edges_grad(i):
        sl = rows_at(i, t_edge)
        d_pre = d_pre3[sl, :]
        own[r_weu:r_weu + lat, :] += tn(edge_lat[sl, :], d_pre)
        own[r_weu + lat:r_weu + 2 * lat, :] += tn(send_lat[sl, :], d_pre)
        own[r_weu + 2 * lat:r_weu + 3 * lat, :] += tn(recv_lat[sl, :], d_pre)
        d_edge_lat[sl, :] += nt(d_pre, w_edge_up[0:lat, :])
    loop(n_et, edges_grad)
    red[0].step(8)()
    red[2].start(0)

    def nodes_bwd(i):
        sl = rows_at(i, t_mesh)
        d_node = nn(hot_rows(dst_row[...], i * t_mesh, t_mesh), d_pre3[...]).astype(BF)
        d_top = d_mesh_lat[sl, :] + nt(d_node, w_edge_up[2 * lat:3 * lat, :])
        feat = mesh_t[:, sl]
        saved, _ = mlp_fwd(tn(feat, w_mesh_in[...]), w_two[1], vec[1])
        d_pre, d_two1, d_vec = mlp_bwd(saved, w_two[1], vec[1], d_top)
        own[r_two1:r_two1 + lat, :] += d_two1
        own[r_wmi:r_wmi + 3, :] += nn(feat, d_pre)
        add_vec(own, r_vec + 4, d_vec)
    loop(n_nt, nodes_bwd, [(0, back.relay(near)), (0, red[2].step(1)), (n_nt - 1, red[2].step(2))])

    def edges_in_bwd(i):
        sl = rows_at(i, t_edge)
        feat = edge_t[:, sl]
        saved, _ = mlp_fwd(tn(feat, w_edge_in[...]), w_two[2], vec[2])
        d_pre, d_two2, d_vec = mlp_bwd(saved, w_two[2], vec[2], d_edge_lat[sl, :])
        own[r_two2:r_two2 + lat, :] += d_two2
        own[r_wei:r_wei + 4, :] += nn(feat, d_pre)
        add_vec(own, r_vec + 8, d_vec)
    loop(n_et, edges_in_bwd, [(n_et // 2, back.relay(mid))])
    red[3].start(0)


    def scatter(z):
        back.wait_lists(z)

        def fn(i):
            sl = rows_at(i, t_grid)
            picks = send_row[0:1, block_at(z)]
            d_lat[sl, :] += nn(hot_rows(picks, i * t_grid, t_grid), d_sent[block_at(z), :])
        loop(n_gt, fn)
    scatter(z_at)
    scatter(near)
    red[3].step(1)()
    back.relay(far)()
    red[1].step(4)()
    red[2].step(3)()
    scatter(mid)
    scatter(far)
    back.wait_planes()

    def grid_bwd(i):
        sl = rows_at(i, t_grid)
        d_top = d_lat[sl, :]
        feat = grid_t[:, sl]
        saved, _ = mlp_fwd(tn(feat, w_grid_in[...]), w_two[0], vec[0])
        d_pre, d_two0, d_vec = mlp_bwd(saved, w_two[0], vec[0], d_top)
        own[r_two0:r_two0 + lat, :] += d_two0
        own[r_wgi:r_wgi + n_feat, :] += nn(feat, d_pre)
        add_vec(own, r_vec, d_vec)
        d_grid_t[:, sl] = nt(w_grid_in[...], d_pre)
    loop(n_gt, grid_bwd, [(0, red[1].step(5)), (0, red[2].step(4)), (0, red[3].step(2)), (n_gt - 1, red[1].step(6)), (n_gt - 1, red[3].step(3))])
    red[4].start(0)
    red[5].start(0)

    stores[2].start()
    for g, k in ((4, 1), (5, 1), (1, 7), (2, 5), (4, 2), (5, 2), (3, 4), (1, 8), (2, 6), (4, 3), (5, 3), (3, 5), (2, 7), (4, 4), (5, 4), (3, 6), (2, 8), (3, 7),
                 (4, 5), (5, 5), (3, 8)):
        red[g].step(k)()
    puts = [(r_weu, 3 * lat, d_weu), (r_wmu, 2 * lat, d_wmu), (r_wgu, lat, d_wgu), (r_two1, lat, d_two.at[1]),
            (r_two2, lat, d_two.at[2]), (r_two3, lat, d_two.at[3]), (r_two4, lat, d_two.at[4]), (r_two5, lat, d_two.at[5])]
    moves = [pltpu.make_async_copy(out.at[pl.ds(a, n)], ref, out_sem.at[3 + k]) for k, (a, n, ref) in enumerate(puts)]
    for move in moves:
        move.start()
    for k in range(6, 9):
        red[4].step(k)()
        red[5].step(k)()
    last = pltpu.make_async_copy(out.at[pl.ds(r_two0, lat)], d_two.at[0], out_sem.at[11])
    last.start()
    d_wgi[...] = out[r_wgi:r_wgi + n_feat, :]
    d_wmi[...] = out[r_wmi:r_wmi + 3, :]
    d_wei[...] = out[r_wei:r_wei + 4, :]
    for k in range(6):
        d_vec_out[k] = out[r_vec + 4 * k:r_vec + 4 * k + 4, :]
    for copy in stores + moves + [last]:
        copy.wait()


def finish_kernel(*refs):
    n = (len(refs) - 2) // 3
    srcs, dsts, held, (in_sem, out_sem) = refs[:n], refs[n:2 * n], refs[2 * n:3 * n], refs[3 * n:]
    takes = [pltpu.make_async_copy(srcs[k], held[k], in_sem.at[k]) for k in range(n)]
    gives = [pltpu.make_async_copy(held[k], dsts[k], out_sem.at[k]) for k in range(n)]
    for copy in takes:
        copy.start()
    for take, give in zip(takes, gives):
        take.wait()
        give.start()
    for copy in gives:
        copy.wait()


def solution(mesh):
    parts = mesh.shape[AXIS]
    row_spec = P(AXIS, None)
    edge_spec = P(AXIS)
    rep_spec = P()
    in_specs = (row_spec, row_spec, row_spec, row_spec, edge_spec, edge_spec) + (rep_spec,) * 8 + (row_spec, row_spec)
    out_specs = (row_spec, row_spec, row_spec) + (rep_spec,) * 8

    def local_step(grid_in, mesh_static, edge_static, send_rows, edge_src, edge_dst, w_grid_in, w_mesh_in, w_edge_in, w_edge_up, w_mesh_up, w_grid_up, w_second, vectors, d_mesh_out, d_grid_out):
        lat = w_grid_up.shape[0]
        n_grid, n_feat = grid_in.shape
        n_mesh = mesh_static.shape[0]
        n_edge = edge_static.shape[0]
        n_slot = send_rows.size
        small = -(-n_feat // 8) * 8 + 8 + 8 + 24
        total = 11 * lat + -(-(lat + small) // 256) * 256
        near = pl.BlockSpec(memory_space=pltpu.VMEM)
        far = pl.BlockSpec(memory_space=pl.ANY)

        def sds(shape, dtype):
            return jax.ShapeDtypeStruct(shape, dtype)
        outs = [sds((n_mesh, lat), BF), sds((n_grid, lat), BF), sds((n_feat, n_grid), F32), sds(w_grid_in.shape, F32), sds(w_mesh_in.shape, F32), sds(w_edge_in.shape, F32),
                sds(w_edge_up.shape, F32), sds(w_mesh_up.shape, F32), sds(w_grid_up.shape, F32), sds(w_second.shape, F32), sds(vectors.shape, F32)]
        out_specs = [far, far, far, near, near, near, far, far, far, far, near]
        V = pltpu.VMEM
        D = pltpu.SemaphoreType.DMA
        scratch = [V(w_edge_up.shape, BF), V(w_mesh_up.shape, BF), V(w_grid_up.shape, BF), V((n_mesh, lat), BF), V((n_grid, lat), BF),
                   V((n_mesh, lat), BF), V((n_grid, lat), BF), V((n_feat, n_grid), F32),
                   V((n_grid, lat), BF), V((n_slot, lat), BF), V((n_slot, lat), BF), V((n_grid, lat), F32), V((n_mesh, lat), BF),
                   V((n_edge, lat), BF), V((n_edge, lat), BF), V((n_edge, lat), BF), V((n_edge, lat), BF), V((n_edge, lat), F32), V((n_edge, lat), F32), V((n_edge, 128), F32),
                   V((n_mesh, lat), BF), V((n_mesh, lat), F32), V((n_edge, lat), F32), V((n_edge, lat), BF), V((n_slot, lat), BF), V((n_slot, lat), BF),
                   V((1, n_slot), jnp.int32), V((1, n_edge), jnp.int32), V((1, n_edge), jnp.int32),
                   V((total, lat), F32), V((total, lat), F32), V((total // 2, lat), F32), V((total // 4, lat), F32), V((total // 8, lat), F32), V((3, total // 32, lat), F32),
                   D((5,)), D((12,)), D((parts,)), D((parts,)), D((parts,)), D((parts,)), D((6, 12)), D((6, 12)),
                   V((n_slot, lat), BF), V((n_slot, lat), BF), D((4,)), D((4,)), D((4,)), D((4,))]
        res = pl.pallas_call(
            functools.partial(step_kernel, parts),
            out_shape=outs,
            in_specs=[near] * 11 + [far] * 5,
            out_specs=out_specs,
            scratch_shapes=scratch,
            compiler_params=pltpu.CompilerParams(vmem_limit_bytes=VMEM_LIMIT, collective_id=0, has_side_effects=True),
            name='step',
        )(grid_in.T, mesh_static.T, edge_static.T, send_rows, edge_src.reshape(-1, 128), edge_dst.reshape(-1, 128),
          w_grid_in, w_mesh_in, w_edge_in, w_second, vectors, w_edge_up, w_mesh_up, w_grid_up, d_mesh_out, d_grid_out)
        res = pl.pallas_call(
            finish_kernel,
            out_shape=outs,
            in_specs=[far] * len(outs),
            out_specs=[far] * len(outs),
            scratch_shapes=[V(o.shape, o.dtype) for o in outs] + [D((len(outs),)), D((len(outs),))],
            compiler_params=pltpu.CompilerParams(vmem_limit_bytes=VMEM_LIMIT),
            name='finish',
        )(*res)
        return (res[0], res[1], res[2].T) + tuple(res[3:])

    return jax.shard_map(local_step, mesh=mesh, in_specs=in_specs, out_specs=out_specs, check_vma=False)
```

```python
import functools

import jax
import jax.numpy as jnp
from jax import lax
from jax.experimental import pallas as pl
from jax.experimental.pallas import tpu as pltpu
from jax.sharding import PartitionSpec as P

LN_EPS = 1e-5
AXIS = 'gp'
BF = jnp.bfloat16
F32 = jnp.float32
MESH = pl.DeviceIdType.MESH
TILE = 1024
VMEM_LIMIT = 60 * 1024 * 1024


def nn(lhs, rhs):
    return jnp.dot(lhs, rhs, preferred_element_type=F32)


def tn(lhs, rhs):
    return lax.dot_general(lhs, rhs, (((0,), (0,)), ((), ())), preferred_element_type=F32)


def nt(lhs, rhs):
    return lax.dot_general(lhs, rhs, (((1,), (1,)), ((), ())), preferred_element_type=F32)


def mlp_fwd(pre_act, w_two, vec):
    act = pre_act + vec[0:1]
    sig = 0.5 * jnp.tanh(0.5 * act) + 0.5
    hidden = (act * sig).astype(BF)
    lin = nn(hidden, w_two) + vec[1:2]
    cen = lin - jnp.mean(lin, axis=-1, keepdims=True)
    inv = lax.rsqrt(jnp.mean(cen * cen, axis=-1, keepdims=True) + LN_EPS)
    normed = cen * inv
    return (act, sig, hidden, normed, inv), normed * vec[2:3] + vec[3:4]


def mlp_bwd(saved, w_two, vec, d_out):
    act, sig, hidden, normed, inv = saved
    d_n = d_out * vec[2:3]
    m_one = jnp.mean(d_n, axis=-1, keepdims=True)
    m_two = jnp.mean(d_n * normed, axis=-1, keepdims=True)
    d_lin = inv * (d_n - m_one - normed * m_two)
    d_lin_bf = d_lin.astype(BF)
    d_two = tn(hidden, d_lin_bf)
    d_hid = nt(d_lin_bf, w_two)
    d_pre = d_hid * (sig * (1.0 + act * (1.0 - sig)))
    d_vec = [jnp.sum(d_pre, axis=0, keepdims=True), jnp.sum(d_lin, axis=0, keepdims=True),
             jnp.sum(d_out * normed, axis=0, keepdims=True), jnp.sum(d_out, axis=0, keepdims=True)]
    return d_pre.astype(BF), d_two, d_vec


def add_vec(ref, base, d_vec):
    for j in range(4):
        ref[base + j:base + j + 1, :] += d_vec[j]


def rows_at(i, size):
    return pl.ds(pl.multiple_of(i * size, size), size)


def one_hot(ids, idx):
    return jnp.where(ids == idx, 1.0, 0.0).astype(BF)


def hot_cols(col_idx, width):
    return one_hot(lax.broadcasted_iota(jnp.int32, (col_idx.shape[0], width), 1), col_idx)


def hot_rows(row_idx, base, height):
    return one_hot(lax.broadcasted_iota(jnp.int32, (height, row_idx.shape[1]), 0) + base, row_idx)


def col_of(row_ref, starts):
    cols = []
    for start in starts:
        row = row_ref[0:1, pl.ds(pl.multiple_of(start, 128), 128)]
        cols.append(jnp.transpose(jnp.broadcast_to(row, (8, 128)))[:, 0:1])
    return jnp.concatenate(cols, axis=0)


def tile_starts(i, size):
    return [i * size + j * 128 for j in range(size // 128)]


def fill_row(idx_ref, row_ref):
    wide = idx_ref.shape[1]
    for j in range(idx_ref.shape[0]):
        row_ref[0:1, j * wide:(j + 1) * wide] = idx_ref[j:j + 1, :]


def loop(n, body, events=()):
    def step(i, carry):
        body(i)
        for when, fn in events:
            pl.when(i == when)(fn)
        return carry
    lax.fori_loop(0, n, step, 0)


class Reducer:
    def __init__(self, group, base, rows, place, refs):
        self.own, self.out, r_one, r_two, r_three, r_four, self.send_sem, self.recv_sem = refs
        self.group, self.place = group, place
        self.piece = rows // 32
        self.half, self.quarter, self.eighth = rows // 2, rows // 4, rows // 8
        self.r_one = r_one.at[pl.ds(base // 2, rows // 2)]
        self.r_two = r_two.at[pl.ds(base // 4, rows // 4)]
        self.r_three = r_three.at[pl.ds(base // 8, rows // 8)]
        self.r_four = [r_four.at[k, pl.ds(base // 32, rows // 32)] for k in range(3)]
        self.lo_one = base + place['core'] * self.half
        self.lo_two = self.lo_one + place['bit_one'] * self.quarter
        self.lo_three = self.lo_two + place['bit_two'] * self.eighth
        self.lo_four = self.lo_three + place['z'] * self.piece

    def at(self, start, size):
        return pl.ds(pl.multiple_of(start, 8), size)

    def copies(self, k):
        place, own, out = self.place, self.own, self.out

        def make(slot, src, dst, peer):
            return pltpu.make_async_remote_copy(src_ref=src, dst_ref=dst, send_sem=self.send_sem.at[self.group, slot],
                                                recv_sem=self.recv_sem.at[self.group, slot], device_id=(peer,), device_id_type=MESH)
        if k == 0:
            lo = self.lo_one + (1 - 2 * place['core']) * self.half
            return [make(0, own.at[self.at(lo, self.half)], self.r_one, place['swap_c'])]
        if k == 1:
            lo = self.lo_two + (1 - 2 * place['bit_one']) * self.quarter
            return [make(1, own.at[self.at(lo, self.quarter)], self.r_two, place['first'])]
        if k == 2:
            lo = self.lo_three + (1 - 2 * place['bit_two']) * self.eighth
            return [make(2, own.at[self.at(lo, self.eighth)], self.r_three, place['second'])]
        if k == 3:
            return [make(3 + j, own.at[self.at(self.lo_three + place['z_to'][j] * self.piece, self.piece)], self.r_four[j], place['z_dev'][j]) for j in range(3)]
        if k == 4:
            sl = self.at(self.lo_four, self.piece)
            return [make(6 + j, out.at[sl], out.at[sl], place['z_dev'][j]) for j in range(3)]
        sl = self.at(*((self.lo_three, self.eighth), (self.lo_two, self.quarter), (self.lo_one, self.half))[k - 5])
        return [make(4 + k, out.at[sl], out.at[sl], place[('second', 'first', 'swap_c')[k - 5]])]

    def start(self, k):
        for copy in self.copies(k):
            copy.start()

    def finish(self, k):
        for copy in self.copies(k):
            copy.wait()
        if k == 0:
            sl = self.at(self.lo_one, self.half)
            self.own[sl, :] += self.r_one[...]
        if k == 1:
            sl = self.at(self.lo_two, self.quarter)
            self.own[sl, :] += self.r_two[...]
        if k == 2:
            sl = self.at(self.lo_three, self.eighth)
            self.own[sl, :] += self.r_three[...]
        if k == 3:
            sl = self.at(self.lo_four, self.piece)
            self.out[sl, :] = self.own[sl, :] + (self.r_four[0][...] + self.r_four[1][...] + self.r_four[2][...])

    def step(self, k):
        def fn():
            if k > 0:
                self.finish(k - 1)
            if k < 8:
                self.start(k)
        return fn


def step_kernel(parts, grid_t, mesh_t, edge_t, send_idx, src_idx, dst_idx, w_grid_in, w_mesh_in, w_edge_in, w_two, vec,
                w_edge_up_h, w_mesh_up_h, w_grid_up_h, d_mesh_h, d_grid_h,
                mesh_out_h, grid_out_h, d_grid_t_h, d_wgi, d_wmi, d_wei, d_weu, d_wmu, d_wgu, d_two, d_vec_out,
                w_edge_up, w_mesh_up, w_grid_up, d_mesh, d_grid, mesh_out, grid_out, d_grid_t,
                grid_lat, outgoing, incoming, d_lat, mesh_lat, edge_lat, recv_lat, send_lat, edge_new, act_s, nrm_s, inv_s,
                d_pre4, d_mesh_lat, d_edge_lat, d_pre3, d_incoming, d_sent, send_row, src_row, dst_row,
                own, out, r_one, r_two, r_three, r_four,
                in_sem, out_sem, go_send, go_recv, back_send, back_recv, red_send, red_recv):
    lat = w_two.shape[1]
    n_feat, n_grid = grid_t.shape
    n_mesh, n_edge, n_slot = mesh_lat.shape[0], edge_lat.shape[0], outgoing.shape[0]
    cap = n_slot // parts
    pair = 2 * cap
    n_feat_pad = -(-n_feat // 8) * 8
    t_grid, t_mesh, t_edge = min(TILE, n_grid), min(TILE, n_mesh), min(TILE, n_edge)
    n_gt, n_nt, n_et = n_grid // t_grid, n_mesh // t_mesh, n_edge // t_edge
    me = lax.axis_index(AXIS)
    core = lax.rem(me, 2)
    x_at = lax.rem(me // 2, 2)
    y_at = lax.rem(me // 4, 2)
    z_at = me // 8
    plane = me - 8 * z_at
    swap_x = me + 2 * (1 - 2 * x_at)
    swap_y = me + 4 * (1 - 2 * y_at)
    z_to = [lax.rem(z_at + k, 4) for k in range(1, 4)]
    place = dict(core=core, z=z_at, swap_c=me + 1 - 2 * core,
                 first=(1 - core) * swap_x + core * swap_y, second=(1 - core) * swap_y + core * swap_x,
                 bit_one=(1 - core) * x_at + core * y_at, bit_two=(1 - core) * y_at + core * x_at,
                 z_to=z_to, z_dev=[plane + 8 * z for z in z_to])

    barrier = pltpu.get_barrier_semaphore()

    def knock(k, carry):
        pl.semaphore_signal(barrier, inc=1, device_id=(lax.rem(me + k, parts),), device_id_type=MESH)
        return carry
    lax.fori_loop(1, parts, knock, 0)

    loads = [pltpu.make_async_copy(a, b, in_sem.at[k]) for k, (a, b) in enumerate(
        [(d_grid_h, d_grid), (w_grid_up_h, w_grid_up), (w_edge_up_h, w_edge_up), (w_mesh_up_h, w_mesh_up), (d_mesh_h, d_mesh)])]
    for copy in loads:
        copy.start()

    r_wgu, r_two5, r_wmu, r_two4 = 0, lat, 2 * lat, 4 * lat
    r_weu, r_two3 = 5 * lat, 8 * lat
    r_two1, r_two2 = 9 * lat, 10 * lat
    r_two0, r_wgi = 11 * lat, 12 * lat
    r_wmi = r_wgi + n_feat_pad
    r_wei = r_wmi + 8
    r_vec = r_wei + 8
    refs = (own, out, r_one, r_two, r_three, r_four, red_send, red_recv)
    bounds = [0, 2 * lat, 5 * lat, 9 * lat, 11 * lat, 12 * lat, own.shape[0]]
    red = [Reducer(g, bounds[g], bounds[g + 1] - bounds[g], place, refs) for g in range(6)]

    own[...] = jnp.zeros_like(own)
    fill_row(send_idx, send_row)
    fill_row(src_idx, src_row)
    fill_row(dst_idx, dst_row)

    def embed(i):
        sl = rows_at(i, t_grid)
        _, emb = mlp_fwd(tn(grid_t[:, sl], w_grid_in[...]), w_two[0], vec[0])
        grid_lat[sl, :] = emb.astype(BF)
    loop(n_gt, embed)

    pl.semaphore_wait(barrier, parts - 1)

    def part_copy(src, dst, sends, recvs, to, frm):
        return pltpu.make_async_remote_copy(
            src_ref=src.at[pl.ds(pl.multiple_of(to * cap, 8), cap)], dst_ref=dst.at[pl.ds(pl.multiple_of(frm * cap, 8), cap)],
            send_sem=sends.at[to], recv_sem=recvs.at[frm], device_id=(to,), device_id_type=MESH)

    z_flip = z_at + 1 - 2 * lax.rem(z_at, 2)
    z_order = [lax.rem(z_at + 2, 4), z_flip, lax.rem(z_flip + 2, 4), z_at]
    planes = parts // 8

    def group_of(i):
        flip_x, flip_y = lax.rem(i + 1, 2), 1 - i // 2
        return x_at + flip_x * (1 - 2 * x_at) + 2 * (y_at + flip_y * (1 - 2 * y_at))

    def starts_of(group):
        return [z * 8 * cap + group * pair for z in range(planes)]

    def pair_at(start):
        return pl.ds(pl.multiple_of(start, 8), pair)

    def send_group(src, dst, sends, recvs, group):
        for z in z_order:
            for c in range(2):
                to = z * 8 + group * 2 + c

                @pl.when(to != me)
                def _():
                    part_copy(src, dst, sends, recvs, to, me).start()

                @pl.when(to == me)
                def _():
                    own_sl = pl.ds(pl.multiple_of(me * cap, 8), cap)
                    dst[own_sl, :] = src[own_sl, :]

    def wait_group(src, dst, sends, recvs, group):
        for z in range(planes):
            for c in range(2):
                other = z * 8 + group * 2 + c

                @pl.when(other != me)
                def _():
                    part_copy(src, dst, sends, recvs, other, me).wait_send()
                    part_copy(src, dst, sends, recvs, me, other).wait_recv()

    def put_group(ref, group, rows):
        for z, start in enumerate(starts_of(group)):
            ref[pair_at(start), :] = rows[z * pair:(z + 1) * pair]

    def get_group(ref, group):
        return jnp.concatenate([ref[pair_at(start), :] for start in starts_of(group)], axis=0)

    def spread(ids, group):
        return ids + (ids // pair) * (8 * cap - pair) + group * pair

    def pick(i):
        group = group_of(i)
        rows = nn(hot_cols(col_of(send_row, starts_of(group)), n_grid), grid_lat[...]).astype(BF)
        put_group(outgoing, group, rows)
        send_group(outgoing, incoming, go_send, go_recv, group)
    loop(4, pick)

    loads[0].wait()
    loads[1].wait()

    def cells(i):
        sl = rows_at(i, t_grid)
        here = grid_lat[sl, :]
        saved, upd = mlp_fwd(nn(here, w_grid_up[...]), w_two[5], vec[5])
        grid_out[sl, :] = (here.astype(F32) + upd).astype(BF)
        d_top = d_grid[sl, :].astype(F32)
        d_pre, d_two5, d_vec = mlp_bwd(saved, w_two[5], vec[5], d_top)
        own[r_wgu:r_wgu + lat, :] += tn(here, d_pre)
        own[r_two5:r_two5 + lat, :] += d_two5
        add_vec(own, r_vec + 20, d_vec)
        d_lat[sl, :] = d_top + nt(d_pre, w_grid_up[...])
    loop(n_gt, cells)
    stores = [pltpu.make_async_copy(a, b, out_sem.at[k]) for k, (a, b) in enumerate([(grid_out, grid_out_h), (mesh_out, mesh_out_h), (d_grid_t, d_grid_t_h)])]
    stores[0].start()
    loads[2].wait()
    loads[3].wait()
    loads[4].wait()

    def nodes_in(i):
        sl = rows_at(i, t_mesh)
        _, emb = mlp_fwd(tn(mesh_t[:, sl], w_mesh_in[...]), w_two[1], vec[1])
        here = emb.astype(BF)
        mesh_lat[sl, :] = here
        d_mesh_lat[sl, :] = nn(here, w_mesh_up[0:lat, :])
    loop(n_nt, nodes_in)

    def edges_in(i):
        sl = rows_at(i, t_edge)
        _, emb = mlp_fwd(tn(edge_t[:, sl], w_edge_in[...]), w_two[2], vec[2])
        here = emb.astype(BF)
        edge_lat[sl, :] = here
        recv = nn(hot_cols(col_of(dst_row, tile_starts(i, t_edge)), n_mesh), mesh_lat[...]).astype(BF)
        recv_lat[sl, :] = recv
        act_s[sl, :] = nn(here, w_edge_up[0:lat, :]) + nn(recv, w_edge_up[2 * lat:3 * lat, :])
    loop(n_et, edges_in)


    def gather(i):
        group = group_of(i // n_et)
        tile = lax.rem(i, n_et)
        sl = rows_at(tile, t_edge)

        @pl.when(tile == 0)
        def _():
            wait_group(outgoing, incoming, go_send, go_recv, group)
        ids = spread(lax.broadcasted_iota(jnp.int32, (t_edge, 4 * pair), 1), group)
        rows = nn(one_hot(ids, col_of(src_row, tile_starts(tile, t_edge))), get_group(incoming, group))

        @pl.when(i < n_et)
        def _():
            nrm_s[sl, :] = rows

        @pl.when(i >= n_et)
        def _():
            nrm_s[sl, :] += rows
    loop(4 * n_et, gather)
    red[0].start(0)

    def edges_fwd(i):
        sl = rows_at(i, t_edge)
        sent = nrm_s[sl, :].astype(BF)
        send_lat[sl, :] = sent
        (act, _, _, normed, inv), upd = mlp_fwd(act_s[sl, :] + nn(sent, w_edge_up[lat:2 * lat, :]), w_two[3], vec[3])
        act_s[sl, :] = act
        nrm_s[sl, :] = normed
        inv_s[sl, :] = jnp.broadcast_to(inv, (t_edge, 128))
        edge_new[sl, :] = (edge_lat[sl, :].astype(F32) + upd).astype(BF)
    loop(n_et, edges_fwd, [(n_et // 2, red[0].step(1))])

    def nodes(i):
        sl = rows_at(i, t_mesh)
        agg = nn(hot_rows(dst_row[...], i * t_mesh, t_mesh), edge_new[...]).astype(BF)
        here = mesh_lat[sl, :]
        saved, upd = mlp_fwd(d_mesh_lat[sl, :] + nn(agg, w_mesh_up[lat:2 * lat, :]), w_two[4], vec[4])
        mesh_out[sl, :] = (here.astype(F32) + upd).astype(BF)
        d_top = d_mesh[sl, :].astype(F32)
        d_pre, d_two4, d_vec = mlp_bwd(saved, w_two[4], vec[4], d_top)
        d_pre4[sl, :] = d_pre
        own[r_wmu:r_wmu + lat, :] += tn(here, d_pre)
        own[r_wmu + lat:r_wmu + 2 * lat, :] += tn(agg, d_pre)
        own[r_two4:r_two4 + lat, :] += d_two4
        add_vec(own, r_vec + 16, d_vec)
        d_mesh_lat[sl, :] = d_top + nt(d_pre, w_mesh_up[0:lat, :])
    loop(n_nt, nodes, [(0, red[0].step(2)), (n_nt - 1, red[0].step(3))])
    stores[1].start()
    red[1].start(0)

    def edges_bwd(i):
        sl = rows_at(i, t_edge)
        picked = nn(hot_cols(col_of(dst_row, tile_starts(i, t_edge)), n_mesh), d_pre4[...]).astype(BF)
        d_new = nt(picked, w_mesh_up[lat:2 * lat, :])
        act = act_s[sl, :]
        sig = 0.5 * jnp.tanh(0.5 * act) + 0.5
        hidden = (act * sig).astype(BF)
        d_pre, d_two3, d_vec = mlp_bwd((act, sig, hidden, nrm_s[sl, :], inv_s[sl, 0:1]), w_two[3], vec[3], d_new)
        d_pre3[sl, :] = d_pre
        own[r_two3:r_two3 + lat, :] += d_two3
        add_vec(own, r_vec + 12, d_vec)
        d_edge_lat[sl, :] = d_new
    loop(n_et, edges_bwd, [(0, red[1].step(1)), (0, red[0].step(4)), (n_et // 2, red[1].step(2)), (n_et // 2, red[0].step(5)), (n_et - 1, red[1].step(3)), (n_et - 1, red[0].step(6))])

    def slots(i):
        group = group_of(i)
        ids = spread(lax.broadcasted_iota(jnp.int32, (4 * pair, n_edge), 0), group)
        d_slot = nn(one_hot(ids, src_row[...]), d_pre3[...]).astype(BF)
        put_group(d_incoming, group, nt(d_slot, w_edge_up[lat:2 * lat, :]).astype(BF))
        send_group(d_incoming, d_sent, back_send, back_recv, group)
    loop(4, slots)
    red[0].step(7)()

    def edges_grad(i):
        sl = rows_at(i, t_edge)
        d_pre = d_pre3[sl, :]
        own[r_weu:r_weu + lat, :] += tn(edge_lat[sl, :], d_pre)
        own[r_weu + lat:r_weu + 2 * lat, :] += tn(send_lat[sl, :], d_pre)
        own[r_weu + 2 * lat:r_weu + 3 * lat, :] += tn(recv_lat[sl, :], d_pre)
        d_edge_lat[sl, :] += nt(d_pre, w_edge_up[0:lat, :])
    loop(n_et, edges_grad)
    red[0].step(8)()
    red[2].start(0)

    def nodes_bwd(i):
        sl = rows_at(i, t_mesh)
        d_node = nn(hot_rows(dst_row[...], i * t_mesh, t_mesh), d_pre3[...]).astype(BF)
        d_top = d_mesh_lat[sl, :] + nt(d_node, w_edge_up[2 * lat:3 * lat, :])
        feat = mesh_t[:, sl]
        saved, _ = mlp_fwd(tn(feat, w_mesh_in[...]), w_two[1], vec[1])
        d_pre, d_two1, d_vec = mlp_bwd(saved, w_two[1], vec[1], d_top)
        own[r_two1:r_two1 + lat, :] += d_two1
        own[r_wmi:r_wmi + 3, :] += nn(feat, d_pre)
        add_vec(own, r_vec + 4, d_vec)
    loop(n_nt, nodes_bwd)

    def edges_in_bwd(i):
        sl = rows_at(i, t_edge)
        feat = edge_t[:, sl]
        saved, _ = mlp_fwd(tn(feat, w_edge_in[...]), w_two[2], vec[2])
        d_pre, d_two2, d_vec = mlp_bwd(saved, w_two[2], vec[2], d_edge_lat[sl, :])
        own[r_two2:r_two2 + lat, :] += d_two2
        own[r_wei:r_wei + 4, :] += nn(feat, d_pre)
        add_vec(own, r_vec + 8, d_vec)
    loop(n_et, edges_in_bwd)
    red[3].start(0)


    def scatter(i):
        group = group_of(i // n_gt)
        tile = lax.rem(i, n_gt)
        sl = rows_at(tile, t_grid)

        @pl.when(tile == 0)
        def _():
            wait_group(d_incoming, d_sent, back_send, back_recv, group)
        picks = jnp.concatenate([send_row[0:1, pl.ds(pl.multiple_of(start, 128), pair)] for start in starts_of(group)], axis=1)
        d_lat[sl, :] += nn(hot_rows(picks, tile * t_grid, t_grid), get_group(d_sent, group))
    loop(4 * n_gt, scatter, [(3 * n_gt - 1, red[1].step(4)), (3 * n_gt - 1, red[2].step(1)), (3 * n_gt - 1, red[3].step(1))])

    def grid_bwd(i):
        sl = rows_at(i, t_grid)
        d_top = d_lat[sl, :]
        feat = grid_t[:, sl]
        saved, _ = mlp_fwd(tn(feat, w_grid_in[...]), w_two[0], vec[0])
        d_pre, d_two0, d_vec = mlp_bwd(saved, w_two[0], vec[0], d_top)
        own[r_two0:r_two0 + lat, :] += d_two0
        own[r_wgi:r_wgi + n_feat, :] += nn(feat, d_pre)
        add_vec(own, r_vec, d_vec)
        d_grid_t[:, sl] = nt(w_grid_in[...], d_pre)
    loop(n_gt, grid_bwd, [(0, red[2].step(2)), (0, red[3].step(2)), (0, red[1].step(5)), (n_gt - 1, red[2].step(3)), (n_gt - 1, red[3].step(3)), (n_gt - 1, red[1].step(6))])
    red[4].start(0)
    red[5].start(0)

    stores[2].start()
    for g, k in ((4, 1), (5, 1), (1, 7), (4, 2), (5, 2), (2, 4), (3, 4), (1, 8), (4, 3), (5, 3), (2, 5), (3, 5), (4, 4), (5, 4), (2, 6), (3, 6),
                 (4, 5), (5, 5), (2, 7), (3, 7), (4, 6), (5, 6), (2, 8), (3, 8)):
        red[g].step(k)()
    puts = [(r_weu, 3 * lat, d_weu), (r_wmu, 2 * lat, d_wmu), (r_wgu, lat, d_wgu), (r_two1, lat, d_two.at[1]),
            (r_two2, lat, d_two.at[2]), (r_two3, lat, d_two.at[3]), (r_two4, lat, d_two.at[4]), (r_two5, lat, d_two.at[5])]
    moves = [pltpu.make_async_copy(out.at[pl.ds(a, n)], ref, out_sem.at[3 + k]) for k, (a, n, ref) in enumerate(puts)]
    for move in moves:
        move.start()
    for k in range(7, 9):
        red[4].step(k)()
        red[5].step(k)()
    last = pltpu.make_async_copy(out.at[pl.ds(r_two0, lat)], d_two.at[0], out_sem.at[11])
    last.start()
    d_wgi[...] = out[r_wgi:r_wgi + n_feat, :]
    d_wmi[...] = out[r_wmi:r_wmi + 3, :]
    d_wei[...] = out[r_wei:r_wei + 4, :]
    for k in range(6):
        d_vec_out[k] = out[r_vec + 4 * k:r_vec + 4 * k + 4, :]
    for copy in stores + moves + [last]:
        copy.wait()


def finish_kernel(*refs):
    n = (len(refs) - 2) // 3
    srcs, dsts, held, (in_sem, out_sem) = refs[:n], refs[n:2 * n], refs[2 * n:3 * n], refs[3 * n:]
    takes = [pltpu.make_async_copy(srcs[k], held[k], in_sem.at[k]) for k in range(n)]
    gives = [pltpu.make_async_copy(held[k], dsts[k], out_sem.at[k]) for k in range(n)]
    for copy in takes:
        copy.start()
    for take, give in zip(takes, gives):
        take.wait()
        give.start()
    for copy in gives:
        copy.wait()


def solution(mesh):
    parts = mesh.shape[AXIS]
    row_spec = P(AXIS, None)
    edge_spec = P(AXIS)
    rep_spec = P()
    in_specs = (row_spec, row_spec, row_spec, row_spec, edge_spec, edge_spec) + (rep_spec,) * 8 + (row_spec, row_spec)
    out_specs = (row_spec, row_spec, row_spec) + (rep_spec,) * 8

    def local_step(grid_in, mesh_static, edge_static, send_rows, edge_src, edge_dst, w_grid_in, w_mesh_in, w_edge_in, w_edge_up, w_mesh_up, w_grid_up, w_second, vectors, d_mesh_out, d_grid_out):
        lat = w_grid_up.shape[0]
        n_grid, n_feat = grid_in.shape
        n_mesh = mesh_static.shape[0]
        n_edge = edge_static.shape[0]
        n_slot = send_rows.size
        small = -(-n_feat // 8) * 8 + 8 + 8 + 24
        total = 11 * lat + -(-(lat + small) // 256) * 256
        near = pl.BlockSpec(memory_space=pltpu.VMEM)
        far = pl.BlockSpec(memory_space=pl.ANY)

        def sds(shape, dtype):
            return jax.ShapeDtypeStruct(shape, dtype)
        outs = [sds((n_mesh, lat), BF), sds((n_grid, lat), BF), sds((n_feat, n_grid), F32), sds(w_grid_in.shape, F32), sds(w_mesh_in.shape, F32), sds(w_edge_in.shape, F32),
                sds(w_edge_up.shape, F32), sds(w_mesh_up.shape, F32), sds(w_grid_up.shape, F32), sds(w_second.shape, F32), sds(vectors.shape, F32)]
        out_specs = [far, far, far, near, near, near, far, far, far, far, near]
        V = pltpu.VMEM
        D = pltpu.SemaphoreType.DMA
        scratch = [V(w_edge_up.shape, BF), V(w_mesh_up.shape, BF), V(w_grid_up.shape, BF), V((n_mesh, lat), BF), V((n_grid, lat), BF),
                   V((n_mesh, lat), BF), V((n_grid, lat), BF), V((n_feat, n_grid), F32),
                   V((n_grid, lat), BF), V((n_slot, lat), BF), V((n_slot, lat), BF), V((n_grid, lat), F32), V((n_mesh, lat), BF),
                   V((n_edge, lat), BF), V((n_edge, lat), BF), V((n_edge, lat), BF), V((n_edge, lat), BF), V((n_edge, lat), F32), V((n_edge, lat), F32), V((n_edge, 128), F32),
                   V((n_mesh, lat), BF), V((n_mesh, lat), F32), V((n_edge, lat), F32), V((n_edge, lat), BF), V((n_slot, lat), BF), V((n_slot, lat), BF),
                   V((1, n_slot), jnp.int32), V((1, n_edge), jnp.int32), V((1, n_edge), jnp.int32),
                   V((total, lat), F32), V((total, lat), F32), V((total // 2, lat), F32), V((total // 4, lat), F32), V((total // 8, lat), F32), V((3, total // 32, lat), F32),
                   D((5,)), D((12,)), D((parts,)), D((parts,)), D((parts,)), D((parts,)), D((6, 12)), D((6, 12))]
        res = pl.pallas_call(
            functools.partial(step_kernel, parts),
            out_shape=outs,
            in_specs=[near] * 11 + [far] * 5,
            out_specs=out_specs,
            scratch_shapes=scratch,
            compiler_params=pltpu.CompilerParams(vmem_limit_bytes=VMEM_LIMIT, collective_id=0, has_side_effects=True),
            name='step',
        )(grid_in.T, mesh_static.T, edge_static.T, send_rows, edge_src.reshape(-1, 128), edge_dst.reshape(-1, 128),
          w_grid_in, w_mesh_in, w_edge_in, w_second, vectors, w_edge_up, w_mesh_up, w_grid_up, d_mesh_out, d_grid_out)
        res = pl.pallas_call(
            finish_kernel,
            out_shape=outs,
            in_specs=[far] * len(outs),
            out_specs=[far] * len(outs),
            scratch_shapes=[V(o.shape, o.dtype) for o in outs] + [D((len(outs),)), D((len(outs),))],
            compiler_params=pltpu.CompilerParams(vmem_limit_bytes=VMEM_LIMIT),
            name='finish',
        )(*res)
        return (res[0], res[1], res[2].T) + tuple(res[3:])

    return jax.shard_map(local_step, mesh=mesh, in_specs=in_specs, out_specs=out_specs, check_vma=False)
```

```python
import functools

import jax
import jax.numpy as jnp
from jax import lax
from jax.experimental import pallas as pl
from jax.experimental.pallas import tpu as pltpu
from jax.sharding import PartitionSpec as P

LN_EPS = 1e-5
AXIS = 'gp'
BF = jnp.bfloat16
F32 = jnp.float32
MESH = pl.DeviceIdType.MESH
TILE = 1024
VMEM_LIMIT = 60 * 1024 * 1024
STEP_LIMIT = 56 * 1024 * 1024


def nn(lhs, rhs):
    return jnp.dot(lhs, rhs, preferred_element_type=F32)


def tn(lhs, rhs):
    return lax.dot_general(lhs, rhs, (((0,), (0,)), ((), ())), preferred_element_type=F32)


def nt(lhs, rhs):
    return lax.dot_general(lhs, rhs, (((1,), (1,)), ((), ())), preferred_element_type=F32)


def mlp_fwd(pre_act, w_two, vec):
    act = pre_act + vec[0:1]
    sig = 0.5 * jnp.tanh(0.5 * act) + 0.5
    hidden = (act * sig).astype(BF)
    lin = nn(hidden, w_two) + vec[1:2]
    cen = lin - jnp.mean(lin, axis=-1, keepdims=True)
    inv = lax.rsqrt(jnp.mean(cen * cen, axis=-1, keepdims=True) + LN_EPS)
    normed = cen * inv
    return (act, sig, hidden, normed, inv), normed * vec[2:3] + vec[3:4]


def mlp_bwd(saved, w_two, vec, d_out):
    act, sig, hidden, normed, inv = saved
    d_n = d_out * vec[2:3]
    m_one = jnp.mean(d_n, axis=-1, keepdims=True)
    m_two = jnp.mean(d_n * normed, axis=-1, keepdims=True)
    d_lin = inv * (d_n - m_one - normed * m_two)
    d_lin_bf = d_lin.astype(BF)
    d_two = tn(hidden, d_lin_bf)
    d_hid = nt(d_lin_bf, w_two)
    d_pre = d_hid * (sig * (1.0 + act * (1.0 - sig)))
    d_vec = [jnp.sum(d_pre, axis=0, keepdims=True), jnp.sum(d_lin, axis=0, keepdims=True),
             jnp.sum(d_out * normed, axis=0, keepdims=True), jnp.sum(d_out, axis=0, keepdims=True)]
    return d_pre.astype(BF), d_two, d_vec


def add_vec(ref, base, d_vec):
    for j in range(4):
        ref[base + j:base + j + 1, :] += d_vec[j]


def rows_at(i, size):
    return pl.ds(pl.multiple_of(i * size, size), size)


def one_hot(ids, idx):
    return jnp.where(ids == idx, 1.0, 0.0).astype(BF)


def hot_cols(col_idx, width):
    return one_hot(lax.broadcasted_iota(jnp.int32, (col_idx.shape[0], width), 1), col_idx)


def hot_rows(row_idx, base, height):
    return one_hot(lax.broadcasted_iota(jnp.int32, (height, row_idx.shape[1]), 0) + base, row_idx)


def col_of(row_ref, starts):
    cols = []
    for start in starts:
        row = row_ref[0:1, pl.ds(pl.multiple_of(start, 128), 128)]
        cols.append(jnp.transpose(jnp.broadcast_to(row, (8, 128)))[:, 0:1])
    return jnp.concatenate(cols, axis=0)


def tile_starts(i, size):
    return [i * size + j * 128 for j in range(size // 128)]


def fill_row(idx_ref, row_ref):
    wide = idx_ref.shape[1]
    for j in range(idx_ref.shape[0]):
        row_ref[0:1, j * wide:(j + 1) * wide] = idx_ref[j:j + 1, :]


def loop(n, body, events=()):
    def step(i, carry):
        body(i)
        for when, fn in events:
            pl.when(i == when)(fn)
        return carry
    lax.fori_loop(0, n, step, 0)


class Reducer:
    def __init__(self, group, base, rows, place, refs):
        self.own, self.out, r_one, r_two, r_three, r_four, self.send_sem, self.recv_sem = refs
        self.group, self.place = group, place
        self.piece = rows // 32
        self.half, self.quarter, self.eighth = rows // 2, rows // 4, rows // 8
        self.r_one = r_one.at[pl.ds(base // 2, rows // 2)]
        self.r_two = r_two.at[pl.ds(base // 4, rows // 4)]
        self.r_three = r_three.at[pl.ds(base // 8, rows // 8)]
        self.r_four = [r_four.at[k, pl.ds(base // 32, rows // 32)] for k in range(3)]
        self.lo_one = base + place['core'] * self.half
        self.lo_two = self.lo_one + place['bit_one'] * self.quarter
        self.lo_three = self.lo_two + place['bit_two'] * self.eighth
        self.lo_four = self.lo_three + place['z'] * self.piece

    def at(self, start, size):
        return pl.ds(pl.multiple_of(start, 8), size)

    def copies(self, k):
        place, own, out = self.place, self.own, self.out

        def make(slot, src, dst, peer):
            return pltpu.make_async_remote_copy(src_ref=src, dst_ref=dst, send_sem=self.send_sem.at[self.group, slot],
                                                recv_sem=self.recv_sem.at[self.group, slot], device_id=(peer,), device_id_type=MESH)
        if k == 0:
            lo = self.lo_one + (1 - 2 * place['core']) * self.half
            return [make(0, own.at[self.at(lo, self.half)], self.r_one, place['swap_c'])]
        if k == 1:
            lo = self.lo_two + (1 - 2 * place['bit_one']) * self.quarter
            return [make(1, own.at[self.at(lo, self.quarter)], self.r_two, place['first'])]
        if k == 2:
            lo = self.lo_three + (1 - 2 * place['bit_two']) * self.eighth
            return [make(2, own.at[self.at(lo, self.eighth)], self.r_three, place['second'])]
        if k == 3:
            return [make(3 + j, own.at[self.at(self.lo_three + place['z_to'][j] * self.piece, self.piece)], self.r_four[j], place['z_dev'][j]) for j in range(3)]
        if k == 4:
            sl = self.at(self.lo_four, self.piece)
            return [make(6 + j, out.at[sl], out.at[sl], place['z_dev'][j]) for j in range(3)]
        sl = self.at(*((self.lo_three, self.eighth), (self.lo_two, self.quarter), (self.lo_one, self.half))[k - 5])
        return [make(4 + k, out.at[sl], out.at[sl], place[('second', 'first', 'swap_c')[k - 5]])]

    def start(self, k):
        for copy in self.copies(k):
            copy.start()

    def finish(self, k):
        for copy in self.copies(k):
            copy.wait()
        if k == 0:
            sl = self.at(self.lo_one, self.half)
            self.own[sl, :] += self.r_one[...]
        if k == 1:
            sl = self.at(self.lo_two, self.quarter)
            self.own[sl, :] += self.r_two[...]
        if k == 2:
            sl = self.at(self.lo_three, self.eighth)
            self.own[sl, :] += self.r_three[...]
        if k == 3:
            sl = self.at(self.lo_four, self.piece)
            self.out[sl, :] = self.own[sl, :] + (self.r_four[0][...] + self.r_four[1][...] + self.r_four[2][...])

    def step(self, k):
        def fn():
            if k > 0:
                self.finish(k - 1)
            if k < 8:
                self.start(k)
        return fn


def step_kernel(parts, grid_t, mesh_t, edge_t, send_idx, src_idx, dst_idx, w_grid_in, w_mesh_in, w_edge_in, w_two, vec,
                w_edge_up_h, w_mesh_up_h, w_grid_up_h, d_mesh_h, d_grid_h,
                mesh_out_h, grid_out_h, d_grid_t_h, d_wgi, d_wmi, d_wei, d_weu, d_wmu, d_wgu, d_two, d_vec_out,
                w_edge_up, w_mesh_up, w_grid_up, d_mesh, d_grid, mesh_out, grid_out, d_grid_t,
                grid_lat, outgoing, incoming, d_lat, mesh_lat, edge_lat, recv_lat, send_lat, edge_new, act_s, nrm_s, inv_s,
                d_pre4, d_mesh_lat, d_edge_lat, d_pre3, d_incoming, d_sent, send_row, src_row, dst_row,
                own, out, r_one, r_two, r_three, r_four,
                in_sem, out_sem, go_send, go_recv, back_send, back_recv, red_send, red_recv):
    lat = w_two.shape[1]
    n_feat, n_grid = grid_t.shape
    n_mesh, n_edge, n_slot = mesh_lat.shape[0], edge_lat.shape[0], outgoing.shape[0]
    cap = n_slot // parts
    pair = 2 * cap
    n_feat_pad = -(-n_feat // 8) * 8
    t_grid, t_mesh, t_edge = min(TILE, n_grid), min(TILE, n_mesh), min(TILE, n_edge)
    n_gt, n_nt, n_et = n_grid // t_grid, n_mesh // t_mesh, n_edge // t_edge
    me = lax.axis_index(AXIS)
    core = lax.rem(me, 2)
    x_at = lax.rem(me // 2, 2)
    y_at = lax.rem(me // 4, 2)
    z_at = me // 8
    plane = me - 8 * z_at
    swap_x = me + 2 * (1 - 2 * x_at)
    swap_y = me + 4 * (1 - 2 * y_at)
    z_to = [lax.rem(z_at + k, 4) for k in range(1, 4)]
    place = dict(core=core, z=z_at, swap_c=me + 1 - 2 * core,
                 first=(1 - core) * swap_x + core * swap_y, second=(1 - core) * swap_y + core * swap_x,
                 bit_one=(1 - core) * x_at + core * y_at, bit_two=(1 - core) * y_at + core * x_at,
                 z_to=z_to, z_dev=[plane + 8 * z for z in z_to])

    barrier = pltpu.get_barrier_semaphore()

    def knock(k, carry):
        pl.semaphore_signal(barrier, inc=1, device_id=(lax.rem(me + k, parts),), device_id_type=MESH)
        return carry
    lax.fori_loop(1, parts, knock, 0)

    loads = [pltpu.make_async_copy(a, b, in_sem.at[k]) for k, (a, b) in enumerate(
        [(d_grid_h, d_grid), (w_grid_up_h, w_grid_up), (w_edge_up_h, w_edge_up), (w_mesh_up_h, w_mesh_up), (d_mesh_h, d_mesh)])]
    for copy in loads:
        copy.start()

    r_wgu, r_two5, r_wmu, r_two4 = 0, lat, 2 * lat, 4 * lat
    r_weu, r_two3 = 5 * lat, 8 * lat
    r_two1, r_two2 = 9 * lat, 10 * lat
    r_two0, r_wgi = 11 * lat, 12 * lat
    r_wmi = r_wgi + n_feat_pad
    r_wei = r_wmi + 8
    r_vec = r_wei + 8
    refs = (own, out, r_one, r_two, r_three, r_four, red_send, red_recv)
    bounds = [0, 2 * lat, 5 * lat, 9 * lat, 11 * lat, 12 * lat, own.shape[0]]
    red = [Reducer(g, bounds[g], bounds[g + 1] - bounds[g], place, refs) for g in range(6)]

    own[...] = jnp.zeros_like(own)
    fill_row(send_idx, send_row)
    fill_row(src_idx, src_row)
    fill_row(dst_idx, dst_row)

    def embed(i):
        sl = rows_at(i, t_grid)
        _, emb = mlp_fwd(tn(grid_t[:, sl], w_grid_in[...]), w_two[0], vec[0])
        grid_lat[sl, :] = emb.astype(BF)
    loop(n_gt, embed)

    pl.semaphore_wait(barrier, parts - 1)

    def part_copy(src, dst, sends, recvs, to, frm):
        return pltpu.make_async_remote_copy(
            src_ref=src.at[pl.ds(pl.multiple_of(to * cap, 8), cap)], dst_ref=dst.at[pl.ds(pl.multiple_of(frm * cap, 8), cap)],
            send_sem=sends.at[to], recv_sem=recvs.at[frm], device_id=(to,), device_id_type=MESH)

    z_flip = z_at + 1 - 2 * lax.rem(z_at, 2)
    z_order = [lax.rem(z_at + 2, 4), z_flip, lax.rem(z_flip + 2, 4), z_at]
    planes = parts // 8

    def group_of(i):
        flip_x, flip_y = lax.rem(i + 1, 2), 1 - i // 2
        return x_at + flip_x * (1 - 2 * x_at) + 2 * (y_at + flip_y * (1 - 2 * y_at))

    def starts_of(group):
        return [z * 8 * cap + group * pair for z in range(planes)]

    def pair_at(start):
        return pl.ds(pl.multiple_of(start, 8), pair)

    def send_group(src, dst, sends, recvs, group):
        for z in z_order:
            for c in range(2):
                to = z * 8 + group * 2 + c

                @pl.when(to != me)
                def _():
                    part_copy(src, dst, sends, recvs, to, me).start()

                @pl.when(to == me)
                def _():
                    own_sl = pl.ds(pl.multiple_of(me * cap, 8), cap)
                    dst[own_sl, :] = src[own_sl, :]

    def wait_group(src, dst, sends, recvs, group):
        for z in range(planes):
            for c in range(2):
                other = z * 8 + group * 2 + c

                @pl.when(other != me)
                def _():
                    part_copy(src, dst, sends, recvs, other, me).wait_send()
                    part_copy(src, dst, sends, recvs, me, other).wait_recv()

    def put_group(ref, group, rows):
        for z, start in enumerate(starts_of(group)):
            ref[pair_at(start), :] = rows[z * pair:(z + 1) * pair]

    def get_group(ref, group):
        return jnp.concatenate([ref[pair_at(start), :] for start in starts_of(group)], axis=0)

    def spread(ids, group):
        return ids + (ids // pair) * (8 * cap - pair) + group * pair

    def pick(i):
        group = group_of(i)
        rows = nn(hot_cols(col_of(send_row, starts_of(group)), n_grid), grid_lat[...]).astype(BF)
        put_group(outgoing, group, rows)
        send_group(outgoing, incoming, go_send, go_recv, group)
    loop(4, pick)

    loads[0].wait()
    loads[1].wait()

    def cells(i):
        sl = rows_at(i, t_grid)
        here = grid_lat[sl, :]
        saved, upd = mlp_fwd(nn(here, w_grid_up[...]), w_two[5], vec[5])
        grid_out[sl, :] = (here.astype(F32) + upd).astype(BF)
        d_top = d_grid[sl, :].astype(F32)
        d_pre, d_two5, d_vec = mlp_bwd(saved, w_two[5], vec[5], d_top)
        own[r_wgu:r_wgu + lat, :] += tn(here, d_pre)
        own[r_two5:r_two5 + lat, :] += d_two5
        add_vec(own, r_vec + 20, d_vec)
        d_lat[sl, :] = d_top + nt(d_pre, w_grid_up[...])
    loop(n_gt, cells)
    stores = [pltpu.make_async_copy(a, b, out_sem.at[k]) for k, (a, b) in enumerate([(grid_out, grid_out_h), (mesh_out, mesh_out_h), (d_grid_t, d_grid_t_h)])]
    stores[0].start()
    loads[2].wait()
    loads[3].wait()
    loads[4].wait()

    def nodes_in(i):
        sl = rows_at(i, t_mesh)
        _, emb = mlp_fwd(tn(mesh_t[:, sl], w_mesh_in[...]), w_two[1], vec[1])
        here = emb.astype(BF)
        mesh_lat[sl, :] = here
        d_mesh_lat[sl, :] = nn(here, w_mesh_up[0:lat, :])
    loop(n_nt, nodes_in)

    def edges_in(i):
        sl = rows_at(i, t_edge)
        _, emb = mlp_fwd(tn(edge_t[:, sl], w_edge_in[...]), w_two[2], vec[2])
        here = emb.astype(BF)
        edge_lat[sl, :] = here
        recv = nn(hot_cols(col_of(dst_row, tile_starts(i, t_edge)), n_mesh), mesh_lat[...]).astype(BF)
        recv_lat[sl, :] = recv
        act_s[sl, :] = nn(here, w_edge_up[0:lat, :]) + nn(recv, w_edge_up[2 * lat:3 * lat, :])
    loop(n_et, edges_in)


    def gather(i):
        group = group_of(i // n_et)
        tile = lax.rem(i, n_et)
        sl = rows_at(tile, t_edge)

        @pl.when(tile == 0)
        def _():
            wait_group(outgoing, incoming, go_send, go_recv, group)
        ids = spread(lax.broadcasted_iota(jnp.int32, (t_edge, 4 * pair), 1), group)
        rows = nn(one_hot(ids, col_of(src_row, tile_starts(tile, t_edge))), get_group(incoming, group))

        @pl.when(i < n_et)
        def _():
            nrm_s[sl, :] = rows

        @pl.when(i >= n_et)
        def _():
            nrm_s[sl, :] += rows
    loop(4 * n_et, gather)
    red[0].start(0)

    def edges_fwd(i):
        sl = rows_at(i, t_edge)
        sent = nrm_s[sl, :].astype(BF)
        send_lat[sl, :] = sent
        (act, _, _, normed, inv), upd = mlp_fwd(act_s[sl, :] + nn(sent, w_edge_up[lat:2 * lat, :]), w_two[3], vec[3])
        act_s[sl, :] = act
        nrm_s[sl, :] = normed
        inv_s[sl, :] = jnp.broadcast_to(inv, (t_edge, 128))
        edge_new[sl, :] = (edge_lat[sl, :].astype(F32) + upd).astype(BF)
    loop(n_et, edges_fwd, [(n_et // 2, red[0].step(1))])

    def nodes(i):
        sl = rows_at(i, t_mesh)
        agg = nn(hot_rows(dst_row[...], i * t_mesh, t_mesh), edge_new[...]).astype(BF)
        here = mesh_lat[sl, :]
        saved, upd = mlp_fwd(d_mesh_lat[sl, :] + nn(agg, w_mesh_up[lat:2 * lat, :]), w_two[4], vec[4])
        mesh_out[sl, :] = (here.astype(F32) + upd).astype(BF)
        d_top = d_mesh[sl, :].astype(F32)
        d_pre, d_two4, d_vec = mlp_bwd(saved, w_two[4], vec[4], d_top)
        d_pre4[sl, :] = d_pre
        own[r_wmu:r_wmu + lat, :] += tn(here, d_pre)
        own[r_wmu + lat:r_wmu + 2 * lat, :] += tn(agg, d_pre)
        own[r_two4:r_two4 + lat, :] += d_two4
        add_vec(own, r_vec + 16, d_vec)
        d_mesh_lat[sl, :] = d_top + nt(d_pre, w_mesh_up[0:lat, :])
    loop(n_nt, nodes, [(0, red[0].step(2)), (n_nt - 1, red[0].step(3))])
    stores[1].start()
    red[1].start(0)

    def edges_bwd(i):
        sl = rows_at(i, t_edge)
        picked = nn(hot_cols(col_of(dst_row, tile_starts(i, t_edge)), n_mesh), d_pre4[...]).astype(BF)
        d_new = nt(picked, w_mesh_up[lat:2 * lat, :])
        act = act_s[sl, :]
        sig = 0.5 * jnp.tanh(0.5 * act) + 0.5
        hidden = (act * sig).astype(BF)
        d_pre, d_two3, d_vec = mlp_bwd((act, sig, hidden, nrm_s[sl, :], inv_s[sl, 0:1]), w_two[3], vec[3], d_new)
        d_pre3[sl, :] = d_pre
        own[r_two3:r_two3 + lat, :] += d_two3
        add_vec(own, r_vec + 12, d_vec)
        d_edge_lat[sl, :] = d_new
    loop(n_et, edges_bwd, [(0, red[1].step(1)), (0, red[0].step(4)), (n_et // 2, red[1].step(2)), (n_et // 2, red[0].step(5)), (n_et - 1, red[1].step(3)), (n_et - 1, red[0].step(6))])

    def slots(i):
        group = group_of(i)
        ids = spread(lax.broadcasted_iota(jnp.int32, (4 * pair, n_edge), 0), group)
        d_slot = nn(one_hot(ids, src_row[...]), d_pre3[...]).astype(BF)
        put_group(d_incoming, group, nt(d_slot, w_edge_up[lat:2 * lat, :]).astype(BF))
        send_group(d_incoming, d_sent, back_send, back_recv, group)
    loop(4, slots)
    red[0].step(7)()

    def edges_grad(i):
        sl = rows_at(i, t_edge)
        d_pre = d_pre3[sl, :]
        own[r_weu:r_weu + lat, :] += tn(edge_lat[sl, :], d_pre)
        own[r_weu + lat:r_weu + 2 * lat, :] += tn(send_lat[sl, :], d_pre)
        own[r_weu + 2 * lat:r_weu + 3 * lat, :] += tn(recv_lat[sl, :], d_pre)
        d_edge_lat[sl, :] += nt(d_pre, w_edge_up[0:lat, :])
    loop(n_et, edges_grad)
    red[0].step(8)()
    red[2].start(0)

    def nodes_bwd(i):
        sl = rows_at(i, t_mesh)
        d_node = nn(hot_rows(dst_row[...], i * t_mesh, t_mesh), d_pre3[...]).astype(BF)
        d_top = d_mesh_lat[sl, :] + nt(d_node, w_edge_up[2 * lat:3 * lat, :])
        feat = mesh_t[:, sl]
        saved, _ = mlp_fwd(tn(feat, w_mesh_in[...]), w_two[1], vec[1])
        d_pre, d_two1, d_vec = mlp_bwd(saved, w_two[1], vec[1], d_top)
        own[r_two1:r_two1 + lat, :] += d_two1
        own[r_wmi:r_wmi + 3, :] += nn(feat, d_pre)
        add_vec(own, r_vec + 4, d_vec)
    loop(n_nt, nodes_bwd)

    def edges_in_bwd(i):
        sl = rows_at(i, t_edge)
        feat = edge_t[:, sl]
        saved, _ = mlp_fwd(tn(feat, w_edge_in[...]), w_two[2], vec[2])
        d_pre, d_two2, d_vec = mlp_bwd(saved, w_two[2], vec[2], d_edge_lat[sl, :])
        own[r_two2:r_two2 + lat, :] += d_two2
        own[r_wei:r_wei + 4, :] += nn(feat, d_pre)
        add_vec(own, r_vec + 8, d_vec)
    loop(n_et, edges_in_bwd)
    red[3].start(0)


    def scatter(i):
        group = group_of(i // n_gt)
        tile = lax.rem(i, n_gt)
        sl = rows_at(tile, t_grid)

        @pl.when(tile == 0)
        def _():
            wait_group(d_incoming, d_sent, back_send, back_recv, group)
        picks = jnp.concatenate([send_row[0:1, pl.ds(pl.multiple_of(start, 128), pair)] for start in starts_of(group)], axis=1)
        d_lat[sl, :] += nn(hot_rows(picks, tile * t_grid, t_grid), get_group(d_sent, group))
    loop(4 * n_gt, scatter, [(3 * n_gt - 1, red[1].step(4)), (3 * n_gt - 1, red[2].step(1)), (3 * n_gt - 1, red[3].step(1))])

    def grid_bwd(i):
        sl = rows_at(i, t_grid)
        d_top = d_lat[sl, :]
        feat = grid_t[:, sl]
        saved, _ = mlp_fwd(tn(feat, w_grid_in[...]), w_two[0], vec[0])
        d_pre, d_two0, d_vec = mlp_bwd(saved, w_two[0], vec[0], d_top)
        own[r_two0:r_two0 + lat, :] += d_two0
        own[r_wgi:r_wgi + n_feat, :] += nn(feat, d_pre)
        add_vec(own, r_vec, d_vec)
        d_grid_t[:, sl] = nt(w_grid_in[...], d_pre)
    loop(n_gt, grid_bwd, [(0, red[2].step(2)), (0, red[3].step(2)), (0, red[1].step(5)), (n_gt - 1, red[2].step(3)), (n_gt - 1, red[3].step(3)), (n_gt - 1, red[1].step(6))])
    red[4].start(0)
    red[5].start(0)

    stores[2].start()
    for g, k in ((4, 1), (5, 1), (1, 7), (4, 2), (5, 2), (2, 4), (3, 4), (1, 8), (4, 3), (5, 3), (2, 5), (3, 5), (4, 4), (5, 4), (2, 6), (3, 6),
                 (4, 5), (5, 5), (2, 7), (3, 7), (4, 6), (5, 6), (2, 8), (3, 8)):
        red[g].step(k)()
    puts = [(r_weu, 3 * lat, d_weu), (r_wmu, 2 * lat, d_wmu), (r_wgu, lat, d_wgu)]
    twos = [r_two0, r_two1, r_two2, r_two3, r_two4, r_two5]
    for row, n, ref in puts:
        ref[...] = out[row:row + n, :]
    for k in range(1, 6):
        d_two[k] = out[twos[k]:twos[k] + lat, :]
    for k in range(7, 9):
        red[4].step(k)()
        red[5].step(k)()
    d_two[0] = out[twos[0]:twos[0] + lat, :]
    d_wgi[...] = out[r_wgi:r_wgi + n_feat, :]
    d_wmi[...] = out[r_wmi:r_wmi + 3, :]
    d_wei[...] = out[r_wei:r_wei + 4, :]
    for k in range(6):
        d_vec_out[k] = out[r_vec + 4 * k:r_vec + 4 * k + 4, :]
    for copy in stores:
        copy.wait()


def finish_kernel(*refs):
    n = (len(refs) - 2) // 3
    srcs, dsts, held, (in_sem, out_sem) = refs[:n], refs[n:2 * n], refs[2 * n:3 * n], refs[3 * n:]
    big = 3
    takes = [pltpu.make_async_copy(srcs[k], held[k], in_sem.at[k]) for k in range(big)]
    gives = [pltpu.make_async_copy(held[k] if k < big else srcs[k], dsts[k], out_sem.at[k]) for k in range(n)]
    for copy in takes:
        copy.start()
    for copy in gives[big:]:
        copy.start()
    for take, give in zip(takes, gives):
        take.wait()
        give.start()
    for copy in gives:
        copy.wait()


def solution(mesh):
    parts = mesh.shape[AXIS]
    row_spec = P(AXIS, None)
    edge_spec = P(AXIS)
    rep_spec = P()
    in_specs = (row_spec, row_spec, row_spec, row_spec, edge_spec, edge_spec) + (rep_spec,) * 8 + (row_spec, row_spec)
    out_specs = (row_spec, row_spec, row_spec) + (rep_spec,) * 8

    def local_step(grid_in, mesh_static, edge_static, send_rows, edge_src, edge_dst, w_grid_in, w_mesh_in, w_edge_in, w_edge_up, w_mesh_up, w_grid_up, w_second, vectors, d_mesh_out, d_grid_out):
        lat = w_grid_up.shape[0]
        n_grid, n_feat = grid_in.shape
        n_mesh = mesh_static.shape[0]
        n_edge = edge_static.shape[0]
        n_slot = send_rows.size
        small = -(-n_feat // 8) * 8 + 8 + 8 + 24
        total = 11 * lat + -(-(lat + small) // 256) * 256
        near = pl.BlockSpec(memory_space=pltpu.VMEM)
        far = pl.BlockSpec(memory_space=pl.ANY)

        def sds(shape, dtype):
            return jax.ShapeDtypeStruct(shape, dtype)
        outs = [sds((n_mesh, lat), BF), sds((n_grid, lat), BF), sds((n_feat, n_grid), F32), sds(w_grid_in.shape, F32), sds(w_mesh_in.shape, F32), sds(w_edge_in.shape, F32),
                sds(w_edge_up.shape, F32), sds(w_mesh_up.shape, F32), sds(w_grid_up.shape, F32), sds(w_second.shape, F32), sds(vectors.shape, F32)]
        out_specs = [far] * 3 + [near] * 8
        V = pltpu.VMEM
        D = pltpu.SemaphoreType.DMA
        scratch = [V(w_edge_up.shape, BF), V(w_mesh_up.shape, BF), V(w_grid_up.shape, BF), V((n_mesh, lat), BF), V((n_grid, lat), BF),
                   V((n_mesh, lat), BF), V((n_grid, lat), BF), V((n_feat, n_grid), F32),
                   V((n_grid, lat), BF), V((n_slot, lat), BF), V((n_slot, lat), BF), V((n_grid, lat), F32), V((n_mesh, lat), BF),
                   V((n_edge, lat), BF), V((n_edge, lat), BF), V((n_edge, lat), BF), V((n_edge, lat), BF), V((n_edge, lat), F32), V((n_edge, lat), F32), V((n_edge, 128), F32),
                   V((n_mesh, lat), BF), V((n_mesh, lat), F32), V((n_edge, lat), F32), V((n_edge, lat), BF), V((n_slot, lat), BF), V((n_slot, lat), BF),
                   V((1, n_slot), jnp.int32), V((1, n_edge), jnp.int32), V((1, n_edge), jnp.int32),
                   V((total, lat), F32), V((total, lat), F32), V((total // 2, lat), F32), V((total // 4, lat), F32), V((total // 8, lat), F32), V((3, total // 32, lat), F32),
                   D((5,)), D((12,)), D((parts,)), D((parts,)), D((parts,)), D((parts,)), D((6, 12)), D((6, 12))]
        res = pl.pallas_call(
            functools.partial(step_kernel, parts),
            out_shape=outs,
            in_specs=[near] * 11 + [far] * 5,
            out_specs=out_specs,
            scratch_shapes=scratch,
            compiler_params=pltpu.CompilerParams(vmem_limit_bytes=STEP_LIMIT, collective_id=0, has_side_effects=True),
            name='step',
        )(grid_in.T, mesh_static.T, edge_static.T, send_rows, edge_src.reshape(-1, 128), edge_dst.reshape(-1, 128),
          w_grid_in, w_mesh_in, w_edge_in, w_second, vectors, w_edge_up, w_mesh_up, w_grid_up, d_mesh_out, d_grid_out)
        res = pl.pallas_call(
            finish_kernel,
            out_shape=outs,
            in_specs=[far] * len(outs),
            out_specs=[far] * len(outs),
            scratch_shapes=[V(o.shape, o.dtype) for o in outs] + [D((len(outs),)), D((len(outs),))],
            compiler_params=pltpu.CompilerParams(vmem_limit_bytes=VMEM_LIMIT),
            name='finish',
        )(*res)
        return (res[0], res[1], res[2].T) + tuple(res[3:])

    return jax.shard_map(local_step, mesh=mesh, in_specs=in_specs, out_specs=out_specs, check_vma=False)
```
